32 devices in a mesh: seq: 8 (over z, x), ctx: 4 (over y, core).
Axes of the slice: x: 2, y: 2, z: 4, core: 2. Of those that a mesh axis runs over, the one named last changes fastest.
Arguments:
- tokens: bfloat16 [8, 1024, 1024], P('seq', 'ctx'), may hold values from -6 to 6
- lengths: int32 [8], P('seq'), may hold values from 256 to 1024, as said below
- cotangent: bfloat16 [8, 1024, 1024], P('seq', 'ctx'), may hold values from -6 to 6
- ln1_gain: bfloat16 [1024], P(('seq', 'ctx')), may hold values from 0.5 to 1.5
- ln1_bias: bfloat16 [1024], P(('seq', 'ctx')), may hold values from -3 to 3
- qkv_weight: bfloat16 [1024, 3072], P(('seq', 'ctx')), may hold values from -0.1875 to 0.1875
- query_bias: bfloat16 [1024], P(('seq', 'ctx')), may hold values from -3 to 3
- value_bias: bfloat16 [1024], P(('seq', 'ctx')), may hold values from -3 to 3
- out_weight: bfloat16 [1024, 1024], P(('seq', 'ctx')), may hold values from -0.375 to 0.375
- out_bias: bfloat16 [1024], P(('seq', 'ctx')), may hold values from -3 to 3
- ln2_gain: bfloat16 [1024], P(('seq', 'ctx')), may hold values from 0.5 to 1.5
- ln2_bias: bfloat16 [1024], P(('seq', 'ctx')), may hold values from -3 to 3
- up_weight: bfloat16 [1024, 4096], P(('seq', 'ctx')), may hold values from -0.1875 to 0.1875
- up_bias: bfloat16 [4096], P(('seq', 'ctx')), may hold values from -3 to 3
- down_weight: bfloat16 [4096, 1024], P(('seq', 'ctx')), may hold values from -0.09375 to 0.09375
- down_bias: bfloat16 [1024], P(('seq', 'ctx')), may hold values from -3 to 3
Outputs:
- output: bfloat16 [8, 1024, 1024], P('seq', 'ctx')
- input_grad: float32 [8, 1024, 1024], P('seq', 'ctx')
- ln1_gain_grad: float32 [1024], P(('seq', 'ctx'))
- ln1_bias_grad: float32 [1024], P(('seq', 'ctx'))
- qkv_weight_grad: float32 [1024, 3072], P(('seq', 'ctx'))
- query_bias_grad: float32 [1024], P(('seq', 'ctx'))
- value_bias_grad: float32 [1024], P(('seq', 'ctx'))
- out_weight_grad: float32 [1024, 1024], P(('seq', 'ctx'))
- out_bias_grad: float32 [1024], P(('seq', 'ctx'))
- ln2_gain_grad: float32 [1024], P(('seq', 'ctx'))
- ln2_bias_grad: float32 [1024], P(('seq', 'ctx'))
- up_weight_grad: float32 [1024, 4096], P(('seq', 'ctx'))
- up_bias_grad: float32 [4096], P(('seq', 'ctx'))
- down_weight_grad: float32 [4096, 1024], P(('seq', 'ctx'))
- down_bias_grad: float32 [1024], P(('seq', 'ctx'))
- stats: float32 [8, 3], P('seq')
The draws below stay inside these ranges and needn't reach their ends.
Inputs may be any that keep to these rules, and one draw needn't show every extreme that they name: `lengths`: some sequence has length 1024 and another 1024 // 4 in every draw.
All inputs are finite; a program needn't handle non-finite values.
Results may differ from the reference program's by a relative error of at most 0.013.
Values may be sent and summed in bfloat16 or wider, within the bound.
A program may use at most 192 MiB of HBM per device.

```python
import jax
import jax.numpy as jnp
from jax import lax

D = 1024
FF = 4096
HEADS = 16
HEAD_DIM = 64
NSEQ = 8
SLOT = 1024


def draw_lengths(key, part):
    first_key, second_key, third_key = jax.random.split(key, 3)
    drawn_lengths = jax.random.randint(first_key, (NSEQ,), SLOT // 4, SLOT + 1)
    longest = jax.random.randint(second_key, (), 0, NSEQ)
    shortest = (longest + jax.random.randint(third_key, (), 1, NSEQ)) % NSEQ
    return drawn_lengths.at[longest].set(SLOT).at[shortest].set(SLOT // 4).astype(jnp.int32)


def strengthened(entries, rng, source, target, parts, factor):
    owner, partner = [(jnp.arange(entries.shape[position]) // (entries.shape[position] // parts)).reshape([-1 if axis == position else 1 for axis in range(entries.ndim)]) for position in (source, target)]
    chosen = jax.random.permutation(rng, parts)[partner]
    strong = (owner == chosen) | (owner == (partner + parts // 2) % parts)
    return jnp.where(strong, factor * entries, entries)


def block_scale(own_key, dims, pieces, low, largest):
    factor_of = 1.0
    for position, blocks in pieces:
        draws = jax.random.uniform(jax.random.fold_in(jax.random.fold_in(own_key, 6), position), (blocks,), jnp.float32, low / len(pieces), largest / len(pieces))
        factor_of = factor_of * jnp.repeat(jnp.exp(draws), dims[position] // blocks).reshape((-1,) + (1,) * (len(dims) - 1 - position))
    return factor_of


def scatter_about(rng, dims, width, reach, cuts=(), kind=jnp.bfloat16):
    values = jax.random.normal(rng, dims, jnp.float32) * width
    if len(cuts) > 0:
        values = block_scale(rng, dims, cuts, -0.22, 0.18) * values
    return jnp.clip(values, min=-reach, max=reach).astype(kind)


def bell_draw_with(own_key, shape, width, most, shards, heavy, kind=jnp.bfloat16):
    values = width * jax.random.normal(own_key, shape, jnp.float32)
    if shards:
        values = values * block_scale(own_key, shape, shards, -0.22, 0.18)
    return jnp.clip(strengthened(values, jax.random.fold_in(own_key, 3), *heavy), -most, most).astype(kind)


def setup_inputs(seed: int = 0) -> dict:
    key_list = jax.random.split(jax.random.key(seed), 17)
    return {
        "tokens": scatter_about(key_list[0], (NSEQ, SLOT, D), 1.0, 6.0, ((0, 8), (1, 4))),
        "lengths": draw_lengths(jax.random.fold_in(key_list[16], 71), 0),
        "cotangent": bell_draw_with(key_list[2], (NSEQ, SLOT, D), 1.0, 6.0, ((0, 8), (1, 4)), (0, 2, 8, 2.0)),
        "ln1_gain": jnp.clip(1.0 + 0.1 * jax.random.normal(key_list[3], (D,), jnp.float32), 0.5, 1.5).astype(jnp.bfloat16),
        "ln1_bias": scatter_about(key_list[4], (D,), 0.5, 3.0, ((0, 32),)),
        "qkv_weight": scatter_about(key_list[5], (D, 3 * D), D ** -0.5, 0.1875, ((0, 32),)),
        "query_bias": scatter_about(key_list[6], (D,), 0.5, 3.0, ((0, 32),)),
        "value_bias": scatter_about(key_list[7], (D,), 0.5, 3.0, ((0, 32),)),
        "out_weight": scatter_about(key_list[8], (D, D), (D // 4) ** -0.5, 0.375, ((0, 32),)),
        "out_bias": scatter_about(key_list[9], (D,), 0.5, 3.0, ((0, 32),)),
        "ln2_gain": jnp.clip(1.0 + 0.1 * jax.random.normal(key_list[10], (D,), jnp.float32), 0.5, 1.5).astype(jnp.bfloat16),
        "ln2_bias": scatter_about(key_list[11], (D,), 0.5, 3.0, ((0, 32),)),
        "up_weight": scatter_about(key_list[12], (D, FF), D ** -0.5, 0.1875, ((0, 32),)),
        "up_bias": scatter_about(key_list[13], (FF,), 0.5, 3.0, ((0, 32),)),
        "down_weight": scatter_about(key_list[14], (FF, D), FF ** -0.5, 0.09375, ((0, 32),)),
        "down_bias": scatter_about(key_list[15], (D,), 0.5, 3.0, ((0, 32),)),
    }


@jax.custom_vjp
def low(v):
    return lax.optimization_barrier(v.astype(jnp.bfloat16)).astype(jnp.float32)

@jax.custom_vjp
def low_back(v):
    return v

def low_keep(v):
    return (low(v), None)

def low_pass(kept, grad):
    return (grad,)

def back_keep(v):
    return (v, None)

def back_low(kept, grad):
    return (low(grad),)
low.defvjp(low_keep, low_pass)
low_back.defvjp(back_keep, back_low)
epsilon = 1e-05

def exact_dot(left, right):
    return jnp.dot(left, right, precision=lax.Precision.HIGHEST, preferred_element_type=jnp.float32)

def normalize(inputs, gain, shift):
    average = lax.optimization_barrier(jnp.mean(inputs, axis=-1, keepdims=True))
    centred = inputs - average
    variance = lax.optimization_barrier(jnp.mean(centred * centred, axis=-1, keepdims=True))
    return centred * lax.rsqrt(variance + epsilon) * gain + shift

def one_head(query_head, key_head, value_head, slope):
    positions = jnp.arange(query_head.shape[0], dtype=jnp.int32)
    raw = exact_dot(query_head, key_head.T) * HEAD_DIM ** (-0.5)
    offset = (positions[None, :] - positions[:, None]).astype(jnp.float32)
    scores = low_back(raw + slope * offset)
    allowed = positions[None, :] <= positions[:, None]
    probs = jax.nn.softmax(jnp.where(allowed, scores, -1e+30), axis=-1)
    return exact_dot(low(probs), value_head)

def sequence_forward(source, length, params):
    gain_one, shift_one, w_qkv, bias_query, bias_value, w_out, bias_out, gain_two, shift_two, w_up, bias_up, w_down, bias_down = params
    positions = jnp.arange(SLOT, dtype=jnp.int32)
    normed_one = low(normalize(source, gain_one, shift_one))
    mixed = exact_dot(normed_one, w_qkv)
    query = low_back(low(mixed[:, :D] + bias_query))
    keys = low_back(low(mixed[:, D:2 * D]))
    values = low_back(low(mixed[:, 2 * D:] + bias_value))
    slopes = jnp.exp2(-8.0 * (jnp.arange(HEADS, dtype=jnp.float32) + 1.0) / HEADS)

    def to_heads(array):
        return array.reshape(SLOT, HEADS, HEAD_DIM).transpose(1, 0, 2)
    attend = jax.checkpoint(one_head)

    def per_head(packed):
        return attend(packed[0], packed[1], packed[2], packed[3])
    head_out = lax.map(per_head, (to_heads(query), to_heads(keys), to_heads(values), slopes))
    attended = low_back(low(head_out.transpose(1, 0, 2).reshape(SLOT, D)))
    branch = low_back(exact_dot(attended, w_out) + bias_out)
    resid = source + branch
    normed_two = low(normalize(resid, gain_two, shift_two))
    pre_act = low_back(exact_dot(normed_two, w_up) + bias_up)
    activated = low(jax.nn.gelu(pre_act, approximate=True))
    ffn = low_back(exact_dot(activated, w_down) + bias_down)
    valid = (positions < length).astype(jnp.float32)[:, None]
    output = valid * (resid + ffn)
    squares = jnp.stack([jnp.sum(valid * branch * branch), jnp.sum(valid * resid * resid), jnp.sum(valid * ffn * ffn)])
    return (output, squares)

def reference(tokens, lengths, cotangent, ln1_gain, ln1_bias, qkv_weight, query_bias, value_bias, out_weight, out_bias, ln2_gain, ln2_bias, up_weight, up_bias, down_weight, down_bias):
    params = tuple((array.astype(jnp.float32) for array in (ln1_gain, ln1_bias, qkv_weight, query_bias, value_bias, out_weight, out_bias, ln2_gain, ln2_bias, up_weight, up_bias, down_weight, down_bias)))

    def per_sequence(carry, packed):
        source, length, grad_out = packed

        def forward(inputs, weights):
            return sequence_forward(inputs, length, weights)
        output, pullback, squares = jax.vjp(forward, source, params, has_aux=True)
        grad_source, grad_params = pullback(grad_out)
        carry = jax.tree.map(lambda left, right: left + right, carry, grad_params)
        stats = jnp.sqrt(squares / (length.astype(jnp.float32) * D))
        return (carry, (output.astype(jnp.bfloat16), grad_source, stats))
    zeros = jax.tree.map(jnp.zeros_like, params)
    grads, results = lax.scan(per_sequence, zeros, (tokens.astype(jnp.float32), lengths, cotangent.astype(jnp.float32)))
    outputs, input_grad, stats = results
    return (outputs, input_grad, grads[0], grads[1], grads[2], grads[3], grads[4], grads[5], grads[6], grads[7], grads[8], grads[9], grads[10], grads[11], grads[12], stats)
```

```python
import itertools

import jax
import jax.numpy as jnp
from jax import lax
from jax.experimental import pallas as pl
from jax.experimental.pallas import tpu as pltpu
from jax.sharding import PartitionSpec as P

MESH = pl.DeviceIdType.MESH
bf16, f32 = jnp.bfloat16, jnp.float32
LOG2E = 1.4426950408889634
D = 1024
R = 256
S = 1024
LIMIT = 66_000_000
NSEM = 200


def nn(a, b):
    return lax.dot_general(a, b, (((1,), (0,)), ((), ())), preferred_element_type=f32)


def nt(a, b):
    return lax.dot_general(a, b, (((1,), (1,)), ((), ())), preferred_element_type=f32)


def tn(a, b):
    return lax.dot_general(a, b, (((0,), (0,)), ((), ())), preferred_element_type=f32)


def mul(v, m):
    return pl.multiple_of(v, m)


def loop(n, body, start=0):
    def step(i, carry):
        body(i)
        return carry

    lax.fori_loop(start, n, step, 0)


def layer_stats(v):
    mean = jnp.sum(v, axis=-1, keepdims=True) * (1.0 / D)
    cen = v - mean
    var = jnp.sum(cen * cen, axis=-1, keepdims=True) * (1.0 / D)
    rstd = lax.rsqrt(var + 1e-5)
    return cen * rstd, rstd


def layer_back(g2, gain, z, rstd):
    g = g2 * gain
    m1 = jnp.sum(g, axis=-1, keepdims=True) * (1.0 / D)
    m2 = jnp.sum(g * z, axis=-1, keepdims=True) * (1.0 / D)
    return rstd * (g - m1 - z * m2)


def block_kernel(
    length_ref, tok, cot, small, qkv_in, out_in, up_in, down_in,
    o_out, o_grad, o_dqkv, o_dout, o_dup, o_ddown, o_small,
    wqkv, wout, wup, wdown, smc, smb, vec,
    n1, n2, gf, gb, act, gpre, qkv, vt, kt, attt, dot_, do_, dmix, linv,
    ptri, acck, accv,
    rs_s, rs_r, rs_own, rt_s, rt_r, rt_own, tmp, res,
    xs, xr_down, xr_up, xr_qkv, xr_out, own_a, own_b, own_out,
    zs, zso, zr_down, zr_up, zr_qkv, zr_out, fin_up, fin_qkv, fin_out,
    sg, sgx, sgs, sgz, sgf, sgc, gvec, gmat, stat,
    lsem, ssem, rsem,
):
    seq, ctx = lax.axis_index("seq"), lax.axis_index("ctx")
    z, x = seq // 2, seq % 2
    y, k = ctx // 2, ctx % 2
    ids = itertools.count()
    lids = itertools.count()

    mate = {"ctx": y * 2 + (k + 1) % 2}
    ypeer = {"ctx": ((y + 1) % 2) * 2 + k}
    xpeer = {"seq": z * 2 + (x + 1) % 2}

    def cpeer(d):
        return {"ctx": (ctx + d) % 4}

    def zpeer(d):
        return {"seq": ((z + d) % 4) * 2 + x}

    def take(n=1):
        first = next(ids)
        for _ in range(n - 1):
            next(ids)
        return first

    def rcopy(src, dst, dev, i):
        return pltpu.make_async_remote_copy(
            src_ref=src, dst_ref=dst, send_sem=ssem.at[i], recv_sem=rsem.at[i],
            device_id=dev, device_id_type=MESH)

    def wait_bytes(ref, sem):
        pltpu.make_async_copy(ref, ref, sem).wait()

    sends = []

    def sent(ref, i, cond=None):
        sends.append((ref, i, cond))

    def flush():
        for ref, i, cond in sends:
            if cond is None:
                wait_bytes(ref, ssem.at[i])
            else:
                @pl.when(cond)
                def _(ref=ref, i=i):
                    wait_bytes(ref, ssem.at[i])
        sends.clear()

    rows = lambda c: pl.ds(mul(c * R, R), R)
    srow = lambda s: pl.ds(mul(s * 128, 128), 128)

    barrier = pltpu.get_barrier_semaphore()
    for d in (1, 2, 3):
        pl.semaphore_signal(barrier, inc=1, device_id=cpeer(d), device_id_type=MESH)
        pl.semaphore_signal(barrier, inc=1, device_id=zpeer(d), device_id_type=MESH)
    pl.semaphore_signal(barrier, inc=1, device_id=xpeer, device_id_type=MESH)
    pl.semaphore_wait(barrier, 7)

    i_smc = take(4)
    for d in (1, 2, 3):
        rcopy(small, smc.at[d], cpeer(d), i_smc + d).start()
        sent(small, i_smc + d)
    own32 = pl.ds(mul(seq * 128 + ctx * 32, 32), 32)

    def qkv_pieces(c):
        for j in range(6):
            yield (pl.ds(mul((j // 2) * D + (c + 4 * (j % 2)) * 128, 128), 128),
                   pl.ds(j * 128, 128))

    i_qa = take(4)
    for d in (1, 2, 3):
        for a, b in qkv_pieces((ctx + d) % 4):
            rcopy(qkv_in.at[:, a], wqkv.at[own32, b], cpeer(d), i_qa + d).start()
        sent(wqkv.at[pl.ds(0, 32), :], i_qa + d)
    l_q = next(lids)
    for a, b in qkv_pieces(ctx):
        pltpu.make_async_copy(qkv_in.at[:, a], wqkv.at[own32, b], lsem.at[l_q]).start()

    for d in (1, 2, 3):
        rcopy(small, smc.at[d], cpeer(d), i_smc + d).wait_recv()
    rowid = lax.broadcasted_iota(jnp.int32, (16, 128), 0)
    smb[seq] = small[...] + jnp.where(rowid < 8, smc[1] + smc[2] + smc[3], 0.0)

    def gather_start(buf, block, zi, xi, src=None):
        for d in (1, 2, 3):
            own = block(seq) if src is None else src
            rcopy(own, block(seq), zpeer(d), zi + d).start()
            sent(own, zi + d)
        own = block(seq) if src is None else src
        rcopy(own, block(seq), xpeer, xi).start()
        sent(own, xi)

    def gather_forward(block, zi, xi, d):
        b = block(((z - d + 4) % 4) * 2 + x)
        rcopy(b, b, xpeer, zi + d).wait_recv()
        rcopy(b, b, xpeer, xi + d).start()
        sent(b, xi + d)

    def gather_finish(block, xi):
        for d in range(4):
            b = block(seq)
            rcopy(b, b, xpeer, xi + d).wait_recv()

    small_block = lambda s: smb.at[s]
    i_sz, i_sx = take(4), take(4)
    gather_start(smb, small_block, i_sz, i_sx)

    for d in (1, 2, 3):
        wait_bytes(wqkv.at[pl.ds(0, 32), :], rsem.at[i_qa + d])
    wait_bytes(wqkv.at[pl.ds(0, 32), :], lsem.at[l_q])
    qkv_block = lambda s: wqkv.at[srow(s), :]
    i_qz, i_qx = take(4), take(4)
    gather_start(wqkv, qkv_block, i_qz, i_qx)

    t = seq % 4
    out32 = pl.ds(mul((seq // 4) * 128 + ctx * 32, 32), 32)
    i_oa = take()
    l_o = next(lids)

    @pl.when(ctx != t)
    def _():
        rcopy(out_in, wout.at[out32, :], {"ctx": t}, i_oa).start()

    sent(out_in, i_oa, ctx != t)

    @pl.when(ctx == t)
    def _():
        pltpu.make_async_copy(out_in, wout.at[out32, :], lsem.at[l_o]).start()

    for d in (1, 2, 3):
        gather_forward(small_block, i_sz, i_sx, d)
    gather_finish(small_block, i_sx)
    for s in range(8):
        vec[:, s * 128 : (s + 1) * 128] = smb[s]

    length = length_ref[0]
    my = mul(ctx * R, R)

    def valid_rows(r0, n):
        pos = lax.broadcasted_iota(jnp.int32, (n, 1), 0) + (ctx * R + r0)
        return jnp.where(pos < length, 1.0, 0.0).astype(f32)

    def first(i):
        r0 = mul(i * 64, 64)
        zz, _ = layer_stats(tok[pl.ds(r0, 64), :].astype(f32))
        n1[pl.ds(mul(my + r0, 64), 64), :] = (zz * vec[0:1, :] + vec[1:2, :]).astype(bf16)
        g = cot[pl.ds(r0, 64), :].astype(f32) * valid_rows(r0, 64)
        gf[pl.ds(mul(my + r0, 64), 64), :] = g.astype(bf16)

    loop(4, first)

    CH = 2
    RC = R // CH

    def chunk(buf, c, ch):
        return buf.at[pl.ds(mul(c * R + ch * RC, RC), RC), :]

    def ag_start(buf, i, ch):
        own = chunk(buf, ctx, ch)
        rcopy(own, own, ypeer, i + CH + ch).start()
        rcopy(own, own, mate, i + ch).start()
        sent(own, i + CH + ch)
        sent(own, i + ch)

    def ag_forward(buf, i, ch):
        b = chunk(buf, ((y + 1) % 2) * 2 + k, ch)
        rcopy(b, b, mate, i + CH + ch).wait_recv()
        rcopy(b, b, mate, i + 2 * CH + ch).start()
        sent(buf.at[pl.ds(0, RC), :], i + 2 * CH + ch)

    def ag_wait(buf, i, which):
        for ch in range(CH):
            b = chunk(buf, ctx, ch)
            rcopy(b, b, mate, i + which * CH + ch).wait_recv()

    i_n1 = take(3 * CH)
    for ch in range(CH):
        ag_start(n1, i_n1, ch)

    i_ua = take(4)
    for d in (1, 2, 3):
        c2 = (ctx + d) % 4
        for s in range(8):
            rcopy(up_in.at[:, pl.ds(mul((s * 4 + c2) * 128, 128), 128)],
                  wup.at[own32, pl.ds(s * 128, 128)], cpeer(d), i_ua + d).start()
        sent(wup.at[pl.ds(0, 32), :], i_ua + d)
    l_u = next(lids)
    for s in range(8):
        pltpu.make_async_copy(up_in.at[:, pl.ds(mul((s * 4 + ctx) * 128, 128), 128)],
                              wup.at[own32, pl.ds(s * 128, 128)], lsem.at[l_u]).start()
    i_gf = take(3 * CH)
    for ch in range(CH):
        ag_start(gf, i_gf, ch)
    l_d = next(lids)
    down_block = lambda s: wdown.at[srow(s), :]
    pltpu.make_async_copy(down_in, down_block(seq), lsem.at[l_d]).start()

    i_oz, i_ox = take(4), take(4)
    out_block = lambda zz: wout.at[pl.ds(mul((zz // 2) * 128, 128), 128), :]

    @pl.when(ctx == t)
    def _():
        wait_bytes(wout.at[pl.ds(0, 96), :], rsem.at[i_oa])
        wait_bytes(wout.at[pl.ds(0, 32), :], lsem.at[l_o])
        for d in (1, 2, 3):
            rcopy(out_block(z), out_block(z), zpeer(d), i_oz + d).start()
        rcopy(out_block(z), out_block(z), xpeer, i_ox).start()

    for d in (1, 2, 3):
        sent(out_block(z), i_oz + d, ctx == t)
    sent(out_block(z), i_ox, ctx == t)

    for ch in range(CH):
        ag_forward(n1, i_n1, ch)

    for d in (1, 2, 3):
        wait_bytes(wup.at[pl.ds(0, 32), :], rsem.at[i_ua + d])
    wait_bytes(wup.at[pl.ds(0, 32), :], lsem.at[l_u])
    up_block = lambda s: wup.at[srow(s), :]
    i_uz, i_ux = take(4), take(4)
    gather_start(wup, up_block, i_uz, i_ux)
    i_dz, i_dx = take(4), take(4)
    gather_start(wdown, down_block, i_dz, i_dx, src=down_in)

    for d in (1, 2, 3):
        gather_forward(qkv_block, i_qz, i_qx, d)
    ag_wait(n1, i_n1, 0)
    gather_finish(qkv_block, i_qx)

    def project(it):
        blk = ((y + it // 2) % 2) * 2 + (k + it % 2) % 2

        @pl.when(it == 3)
        def _():
            ag_wait(n1, i_n1, 2)

        a = n1[rows(blk), :]
        for j in range(3):
            r = nn(a, wqkv[:, j * 256 : (j + 1) * 256])
            if j != 1:
                for i in range(2):
                    b = vec[2 + j // 2 : 3 + j // 2, pl.ds(mul((ctx + 4 * i) * 128, 128), 128)]
                    qkv[rows(blk), j * 256 + i * 128 : j * 256 + (i + 1) * 128] = (
                        r[:, i * 128 : (i + 1) * 128] + b).astype(bf16)
            else:
                qkv[rows(blk), 256:512] = r.astype(bf16)

    loop(4, project)
    for ch in range(CH):
        ag_forward(gf, i_gf, ch)

    mine = x == k
    for d in (1, 2, 3):
        zz = (z - d + 4) % 4

        @pl.when(jnp.logical_and(mine, zz % 2 == y))
        def _(d=d, zz=zz):
            rcopy(out_block(zz), out_block(zz), xpeer, i_oz + d).wait_recv()
            rcopy(out_block(zz), out_block(zz), xpeer, i_ox + d).start()

        sent(out_block(zz), i_ox + d, jnp.logical_and(mine, zz % 2 == y))

    def turn(i):
        c0 = pl.ds(mul(i * 128, 128), 128)
        vt[c0, :] = qkv[:, pl.ds(mul(512 + i * 128, 128), 128)].T
        kt[c0, :] = qkv[:, pl.ds(mul(256 + i * 128, 128), 128)].T

    loop(2, turn)

    lane = lax.broadcasted_iota(jnp.int32, (256, 128), 1)
    krow = lax.broadcasted_iota(jnp.int32, (256, 256), 0)
    qcol = lax.broadcasted_iota(jnp.int32, (256, 256), 1)

    def tri(kb, qb):
        return (qb * (qb + 1)) // 2 + kb

    def half(v, j):
        return jnp.where((lane // 64) == j, v, jnp.zeros_like(v))

    def pair_forward(i):
        for j in range(2):
            slope = jnp.exp2(jnp.full((1024, 128), -0.5, f32)
                             * (2 * ctx + 8 * i + j + 1).astype(f32)) * LOG2E
            b = slope * lax.broadcasted_iota(jnp.int32, (1024, 128), 0).astype(f32)
            for kb in range(4):
                own_b[j * 256 : (j + 1) * 256, kb * 128 : (kb + 1) * 128] = b[kb * 256 : (kb + 1) * 256]

        def queries(qb):
            q0 = pl.ds(mul(qb * 256, 256), 256)
            qblk = qkv[q0, pl.ds(mul(i * 128, 128), 128)]

            def scores(kb, best):
                k0 = pl.ds(mul(kb * 256, 256), 256)
                kblk = qkv[k0, pl.ds(mul(256 + i * 128, 128), 128)]
                new = []
                for j in range(2):
                    b = own_b[j * 256 : (j + 1) * 256, pl.ds(mul(kb * 128, 128), 128)]
                    sc = nt(half(kblk, j), qblk) * (0.125 * LOG2E) + jnp.concatenate([b, b], axis=1)
                    sc = jnp.where(krow + kb * 256 <= qcol + qb * 256, sc, -1e30)
                    own_a[j * 256 : (j + 1) * 256, k0] = sc
                    new.append(jnp.maximum(best[j], jnp.max(sc.reshape(32, 8, 256), axis=0)))
                return tuple(new)

            low = jnp.full((8, 256), -3e38, f32)
            best = lax.fori_loop(0, qb + 1, scores, (low, low))
            top = [jnp.max(b, axis=0, keepdims=True) for b in best]

            def weigh(kb, carry):
                k0 = pl.ds(mul(kb * 256, 256), 256)
                new = []
                for j in range(2):
                    total, acc = carry[2 * j], carry[2 * j + 1]
                    p = jnp.exp2(own_a[j * 256 : (j + 1) * 256, k0] - top[j])
                    total = total + jnp.sum(p.reshape(32, 8, 256), axis=0)
                    p = p.astype(bf16)
                    ptri[2 * i + j, tri(kb, qb)] = p
                    v = vt[pl.ds(mul(i * 128 + j * 64, 64), 64), k0]
                    new += [total, acc + nn(v, p)]
                return tuple(new)

            zero = (jnp.zeros((8, 256), f32), jnp.zeros((64, 256), f32))
            out = lax.fori_loop(0, qb + 1, weigh, zero + zero)
            for j in range(2):
                inv = 1.0 / jnp.sum(out[2 * j], axis=0, keepdims=True)
                linv[2 * i + j, :, q0] = jnp.broadcast_to(inv, (8, 256))
                attt[pl.ds(mul(i * 128 + j * 64, 64), 64), q0] = (out[2 * j + 1] * inv).astype(bf16)

        loop(4, queries)

    loop(2, pair_forward)

    def rs_run(partial, sb, rb, own, i):
        def step(tt):
            g, ch, sub = tt // 4, (tt // 2) % 2, tt % 2
            blk = ((y + 1 - g) % 2) * 2 + (k + 1 - sub) % 2
            partial(blk, ch, tmp)

            @pl.when(jnp.logical_and(g == 0, sub == 0))
            def _():
                sb[0, ch] = tmp[...].astype(bf16)
                rcopy(sb.at[0, ch], rb.at[0, ch], mate, i + ch).start()

            @pl.when(jnp.logical_and(g == 0, sub == 1))
            def _():
                rcopy(sb.at[0, ch], rb.at[0, ch], mate, i + ch).wait_recv()
                sb[1, ch] = (tmp[...] + rb[0, ch].astype(f32)).astype(bf16)
                rcopy(sb.at[1, ch], rb.at[1, ch], ypeer, i + CH + ch).start()

            @pl.when(jnp.logical_and(g == 1, sub == 0))
            def _():
                sb[2, ch] = tmp[...].astype(bf16)
                rcopy(sb.at[2, ch], rb.at[2, ch], mate, i + 2 * CH + ch).start()

            @pl.when(jnp.logical_and(g == 1, sub == 1))
            def _():
                own[ch] = tmp[...]

        loop(4 * CH, step)

    def rs_wait(sb, rb, i, ch):
        rcopy(sb.at[2, ch], rb.at[2, ch], mate, i + 2 * CH + ch).wait_recv()
        rcopy(sb.at[1, ch], rb.at[1, ch], mate, i + CH + ch).wait_recv()

    def rs_sum(rb, own, ch, r):
        return own[ch, r, :] + rb[2, ch, r, :].astype(f32) + rb[1, ch, r, :].astype(f32)

    def rs_sent(sb, i):
        for j in range(3):
            for ch in range(CH):
                wait_bytes(sb.at[j, ch], ssem.at[i + j * CH + ch])

    for d in range(4):
        zz = (z - d + 4) % 4

        @pl.when(jnp.logical_and(x != k, zz % 2 == y))
        def _(d=d):
            rcopy(out_block(z), out_block(z), xpeer, i_ox + d).wait_recv()

    def branch_part(blk, ch, dst):
        a = attt[:, pl.ds(mul(blk * R + ch * RC, RC), RC)]
        dst[...] = tn(a, wout[...])

    i_br = take(3 * CH)
    rs_run(branch_part, rs_s, rs_r, rs_own, i_br)

    for d in (1, 2, 3):
        gather_forward(up_block, i_uz, i_ux, d)

    i_n2 = take(3 * CH)
    stat[...] = jnp.zeros_like(stat)
    for ch in range(CH):
        rs_wait(rs_s, rs_r, i_br, ch)

        def second(q, ch=ch):
            r = pl.ds(mul(q * 32, 32), 32)
            r1 = pl.ds(mul(ch * RC + q * 32, 32), 32)
            branch = rs_sum(rs_r, rs_own, ch, r) + vec[4:5, :]
            resid = tok[r1, :].astype(f32) + branch
            res[r1, :] = resid
            zz, _ = layer_stats(resid)
            n2[pl.ds(mul(my + ch * RC + q * 32, 32), 32), :] = (
                zz * vec[5:6, :] + vec[6:7, :]).astype(bf16)
            v = valid_rows(ch * RC + q * 32, 32)
            stat[0:8, :] += jnp.sum((branch * branch * v).reshape(4, 8, D), axis=0)
            stat[8:16, :] += jnp.sum((resid * resid * v).reshape(4, 8, D), axis=0)

        loop(RC // 32, second)
        ag_start(n2, i_n2, ch)

    ag_wait(gf, i_gf, 0)
    ag_wait(gf, i_gf, 2)
    for d in (1, 2, 3):
        gather_forward(down_block, i_dz, i_dx, d)
    gather_finish(up_block, i_ux)

    def feed(it):
        blk = ((y + it // 2) % 2) * 2 + (k + it % 2) % 2

        @pl.when(it == 1)
        def _():
            ag_wait(n2, i_n2, 0)
            for ch in range(CH):
                ag_forward(n2, i_n2, ch)
            for d in range(4):
                rcopy(down_block(seq), down_block(seq), xpeer, i_dx + d).wait_recv()
            wait_bytes(down_in, lsem.at[l_d])

        @pl.when(it == 3)
        def _():
            ag_wait(n2, i_n2, 2)

        def cols(n):
            c0 = pl.ds(mul(n * 512, 512), 512)
            pre = nn(n2[rows(blk), :], wup[:, c0]) + vec[8:9, c0]
            sq = pre * pre
            th = jnp.tanh(0.7978845608028654 * pre * (1.0 + 0.044715 * sq))
            a1 = 0.5 * (1.0 + th)
            act[rows(blk), c0] = (pre * a1).astype(bf16)
            der = a1 + 0.5 * pre * (1.0 - th * th) * (
                0.7978845608028654 * (1.0 + 0.134145 * sq))
            gpre[rows(blk), c0] = der.astype(bf16)

        loop(2, cols)

    loop(4, feed)
    gvec[...] = jnp.zeros_like(gvec)

    def grad_feed(it):
        r = pl.ds(mul(it * R, R), R)

        def cols(n):
            c0 = pl.ds(mul(n * 512, 512), 512)
            ga = nt(gf[r, :], wdown[c0, :])
            g = (ga * gpre[r, c0].astype(f32)).astype(bf16)
            gpre[r, c0] = g
            gvec[2, :, c0] += jnp.sum(g.astype(f32).reshape(R // 8, 8, 512), axis=0)

        loop(2, cols)

    loop(4, grad_feed)

    rs_sent(rs_s, i_br)

    def gn2_part(blk, ch, dst):
        dst[...] = nt(gpre[pl.ds(mul(blk * R + ch * RC, RC), RC), :], wup[...])

    i_g2 = take(3 * CH)
    rs_run(gn2_part, rs_s, rs_r, rs_own, i_g2)

    def dw_half(a, b, n, xx, hh):
        c1 = pl.ds(mul(((2 * hh) * 2 + xx) * 128, 128), 128)
        c2 = pl.ds(mul(((2 * hh + 1) * 2 + xx) * 128, 128), 128)
        return tn(jnp.concatenate([a[:, c1], a[:, c2]], axis=1), b[:, 0:n])

    def dw_run(a, b, n, xr, own, i, before=None):
        def away(hh):
            xs[pl.ds(mul(hh * 256, 256), 256), 0:n] = dw_half(a, b, n, (x + 1) % 2, hh).astype(bf16)
            s0 = xs.at[pl.ds(mul(hh * 256, 256), 256), pl.ds(0, n)]
            rcopy(s0, xr.at[pl.ds(mul(hh * 256, 256), 256), :], xpeer, i + hh).start()

        loop(2, away)

        def keep(hh):
            own[pl.ds(mul(hh * 256, 256), 256), 0:n] = dw_half(a, b, n, x, hh)

        loop(2, keep)

    def dw_xsent(n, i):
        for hh in range(2):
            wait_bytes(xs.at[pl.ds(0, 256), pl.ds(0, n)], ssem.at[i + hh])

    def dw_z(n, xr, own, zr, fin, i, iz):
        for hh in range(2):
            wait_bytes(xr.at[pl.ds(0, 256), :], rsem.at[i + hh])
        for d in (1, 2, 3):
            blk = srow((z + d) % 4)
            zs[d - 1, :, 0:n] = (own[blk, 0:n] + xr[blk, :].astype(f32)).astype(bf16)
            rcopy(zs.at[d - 1, :, pl.ds(0, n)], zr.at[d - 1], zpeer(d), iz + d).start()
        blk = srow(z)
        fin[...] = own[blk, 0:n] + xr[blk, :].astype(f32)

    def dw_zsent(n, iz):
        for d in (1, 2, 3):
            wait_bytes(zs.at[d - 1, :, pl.ds(0, n)], ssem.at[iz + d])

    def dw_end(zr, fin, iz):
        for d in (1, 2, 3):
            wait_bytes(zr.at[d - 1], rsem.at[iz + d])
        fin[...] += (zr[0].astype(f32) + zr[1].astype(f32)) + zr[2].astype(f32)

    i_dwx, i_dwz = take(2), take(4)
    dw_run(act, gf, D, xr_down, own_a, i_dwx)

    i_gb = take(3 * CH)
    for ch in range(CH):
        rs_wait(rs_s, rs_r, i_g2, ch)

        def third(q, ch=ch):
            r = pl.ds(mul(q * 32, 32), 32)
            r1 = pl.ds(mul(ch * RC + q * 32, 32), 32)
            g2 = rs_sum(rs_r, rs_own, ch, r)
            zz, rstd = layer_stats(res[r1, :])
            gout = cot[r1, :].astype(f32) * valid_rows(ch * RC + q * 32, 32)
            gres = gout + layer_back(g2, vec[5:6, :], zz, rstd)
            o_grad[r1, :] = gres
            low = gres.astype(bf16)
            gb[pl.ds(mul(my + ch * RC + q * 32, 32), 32), :] = low
            fold = lambda v: jnp.sum(v.reshape(4, 8, D), axis=0)
            gvec[4] += fold(low.astype(f32))
            gvec[5] += fold(g2 * zz)
            gvec[6] += fold(g2)
            gvec[7] += fold(gout)

        loop(RC // 32, third)
        ag_start(gb, i_gb, ch)

    dw_xsent(D, i_dwx)
    i_uwx, i_uwz = take(2), take(4)
    dw_run(n2, gpre, D, xr_up, own_b, i_uwx)
    dw_z(D, xr_down, own_a, zr_down, o_ddown, i_dwx, i_dwz)
    for ch in range(CH):
        ag_forward(gb, i_gb, ch)

    def ffn_part(blk, ch, dst):
        dst[...] = nn(act[pl.ds(mul(blk * R + ch * RC, RC), RC), :], wdown[...])

    i_ff = take(3 * CH)
    rs_run(ffn_part, rt_s, rt_r, rt_own, i_ff)

    ag_wait(gb, i_gb, 0)
    ag_wait(gb, i_gb, 2)

    def att_grad(i):
        c0 = pl.ds(mul(i * 256, 256), 256)
        dot_[:, c0] = nt(wout[...], gb[c0, :]).astype(bf16)

    loop(4, att_grad)
    own_out[...] = nn(attt[...], gb[...])
    i_owx, i_owz = take(), take(4)

    dw_xsent(D, i_uwx)

    @pl.when(x != k)
    def _():
        xs[0:256, :] = own_out[...].astype(bf16)
        rcopy(xs.at[pl.ds(0, 256), :], xr_out, xpeer, i_owx).start()

    lane2 = lax.broadcasted_iota(jnp.int32, (1024, 128), 1)

    def pair_backward(i):
        p0 = pl.ds(mul(i * 128, 128), 128)
        for j in range(2):
            r0 = pl.ds(mul(i * 128 + j * 64, 64), 64)
            li = linv[2 * i + j, 0:1, :]
            dd = dot_[r0, :].astype(f32) * li
            delta = jnp.sum(dd * attt[r0, :].astype(f32), axis=0, keepdims=True)
            linv[2 * i + j, :, :] = jnp.broadcast_to(delta, (8, 1024))
            dot_[r0, :] = dd.astype(bf16)
        do_[...] = dot_[p0, :].T
        acck[...] = jnp.zeros_like(acck)
        accv[...] = jnp.zeros_like(accv)

        def queries(qb):
            q0 = pl.ds(mul(qb * 256, 256), 256)
            qblk = qkv[q0, p0]
            doblk = do_[q0, :]
            dt = dot_[p0, q0]

            def keys(kb, carry):
                k0 = pl.ds(mul(kb * 256, 256), 256)
                vblk = qkv[k0, pl.ds(mul(512 + i * 128, 128), 128)]
                new = []
                for j in range(2):
                    p = ptri[2 * i + j, tri(kb, qb)]
                    dp = nn(half(vblk, j), dt) - linv[2 * i + j, 0:1, q0]
                    ds = (p.astype(f32) * dp).astype(bf16)
                    accv[j, k0, :] += nn(p, doblk)
                    acck[j, k0, :] += nn(ds, qblk)
                    kk = kt[pl.ds(mul(i * 128 + j * 64, 64), 64), k0]
                    new.append(carry[j] + nn(kk, ds))
                return tuple(new)

            zero = jnp.zeros((64, 256), f32)
            dq = lax.fori_loop(0, qb + 1, keys, (zero, zero))
            dq = jnp.concatenate(dq, axis=0) * 0.125
            dmix[q0, pl.ds(mul(i * 128, 128), 128)] = dq.T.astype(bf16)

        loop(4, queries)
        dk = jnp.where(lane2 < 64, acck[0], acck[1]) * 0.125
        dv = jnp.where(lane2 < 64, accv[0], accv[1])
        dmix[:, pl.ds(mul(256 + i * 128, 128), 128)] = dk.astype(bf16)
        dmix[:, pl.ds(mul(512 + i * 128, 128), 128)] = dv.astype(bf16)

    loop(2, pair_backward)

    rs_sent(rs_s, i_g2)

    def gn1_part(blk, ch, dst):
        dst[...] = nt(dmix[pl.ds(mul(blk * R + ch * RC, RC), RC), :], wqkv[...])

    i_g1 = take(3 * CH)
    rs_run(gn1_part, rs_s, rs_r, rs_own, i_g1)
    dw_zsent(D, i_dwz)
    dw_z(D, xr_up, own_b, zr_up, fin_up, i_uwx, i_uwz)

    @pl.when(x != k)
    def _():
        wait_bytes(xs.at[pl.ds(0, 256), :], ssem.at[i_owx])

    i_qwx, i_qwz = take(2), take(4)
    dw_run(n1, dmix, 768, xr_qkv, own_a, i_qwx)

    for i in range(2):
        zi = y + 2 * i
        dz = (zi - z + 4) % 4

        @pl.when(x == k)
        def _(i=i, zi=zi, dz=dz):
            if i == 0:
                wait_bytes(xr_out, rsem.at[i_owx])
            half_rows = slice(i * 128, (i + 1) * 128)
            total = own_out[half_rows, :] + xr_out[half_rows, :].astype(f32)

            @pl.when(zi == z)
            def _():
                fin_out[...] = total

            @pl.when(zi != z)
            def _():
                zso[i] = total.astype(bf16)
                rcopy(zso.at[i], zr_out.at[dz - 1], {"seq": zi * 2 + x}, i_owz + dz).start()

        sent(zso.at[i], i_owz + dz, jnp.logical_and(x == k, zi != z))

    for ch in range(CH):
        rs_wait(rs_s, rs_r, i_g1, ch)

        def fourth(q, ch=ch):
            r = pl.ds(mul(q * 32, 32), 32)
            r1 = pl.ds(mul(ch * RC + q * 32, 32), 32)
            g1 = rs_sum(rs_r, rs_own, ch, r)
            zz, rstd = layer_stats(tok[r1, :].astype(f32))
            o_grad[r1, :] += layer_back(g1, vec[0:1, :], zz, rstd)
            fold = lambda v: jnp.sum(v.reshape(4, 8, D), axis=0)
            gvec[0] += fold(g1 * zz)
            gvec[1] += fold(g1)

        loop(RC // 32, fourth)

    gmat[...] = jnp.zeros_like(gmat)
    for r, v in ((0, 0), (1, 1), (4, 4), (5, 5), (6, 6), (7, 7), (8, 2)):
        gmat[r : r + 1, :] = jnp.sum(gvec[v], axis=0, keepdims=True)
    for j, r in ((0, 2), (2, 3)):
        v = dmix[:, j * 256 : (j + 1) * 256].astype(f32)
        v = jnp.sum(jnp.sum(v.reshape(128, 8, 256), axis=0), axis=0, keepdims=True)
        for i in range(2):
            gmat[r : r + 1, pl.ds(mul((ctx + 4 * i) * 128, 128), 128)] = v[:, i * 128 : (i + 1) * 128]
    for s in range(8):
        sg[s] = gmat[:, s * 128 : (s + 1) * 128]
    i_sgx, i_sgz, i_sgc = take(4), take(4), take(4)
    for j in range(4):
        src = sg.at[j * 2 + (x + 1) % 2]
        rcopy(src, sgx.at[j], xpeer, i_sgx + j).start()
        sent(src, i_sgx + j)

    dw_zsent(D, i_uwz)
    dw_z(768, xr_qkv, own_a, zr_qkv, fin_qkv, i_qwx, i_qwz)
    for j in range(4):
        rcopy(sg.at[j], sgx.at[j], xpeer, i_sgx + j).wait_recv()
    for d in (1, 2, 3):
        zz = (z + d) % 4
        sgs[d - 1] = sg[zz * 2 + x] + sgx[zz]
        rcopy(sgs.at[d - 1], sgz.at[d - 1], zpeer(d), i_sgz + d).start()
        sent(sgs.at[d - 1], i_sgz + d)

    dw_end(zr_down, o_ddown, i_dwz)
    dw_end(zr_up, fin_up, i_uwz)
    i_uf, i_qf, i_of = take(4), take(4), take(4)

    def up_piece(fin, c, s):
        return (fin.at[pl.ds(mul(c * 32, 32), 32), pl.ds(s * 128, 128)],
                o_dup.at[:, pl.ds(mul((s * 4 + ctx) * 128, 128), 128)])

    for d in (1, 2, 3):
        for s in range(8):
            a, b = up_piece(fin_up, (ctx + d) % 4, s)
            rcopy(a, b, cpeer(d), i_uf + d).start()
        sent(fin_up.at[pl.ds(0, 32), :], i_uf + d)
    mine32 = pl.ds(mul(ctx * 32, 32), 32)
    for s in range(8):
        o_dup[:, pl.ds(mul((s * 4 + ctx) * 128, 128), 128)] = fin_up[mine32, s * 128 : (s + 1) * 128]

    @pl.when(ctx == t)
    def _():
        for d in (1, 2, 3):
            wait_bytes(zr_out.at[d - 1], rsem.at[i_owz + d])
        fin_out[...] += (zr_out[0].astype(f32) + zr_out[1].astype(f32)) + zr_out[2].astype(f32)
        for d in (1, 2, 3):
            src = fin_out.at[pl.ds(mul(((ctx + d) % 4) * 32, 32), 32), :]
            rcopy(src, o_dout, cpeer(d), i_of + d).start()
        o_dout[...] = fin_out[mine32, :]

    for d in (1, 2, 3):
        sent(fin_out.at[pl.ds(0, 32), :], i_of + d, ctx == t)

    for ch in range(CH):
        rs_wait(rt_s, rt_r, i_ff, ch)

        def last(q, ch=ch):
            r = pl.ds(mul(q * 32, 32), 32)
            r1 = pl.ds(mul(ch * RC + q * 32, 32), 32)
            ffn = rs_sum(rt_r, rt_own, ch, r) + vec[7:8, :]
            v = valid_rows(ch * RC + q * 32, 32)
            o_out[r1, :] = (v * (res[r1, :] + ffn)).astype(bf16)
            stat[16:24, :] += jnp.sum((ffn * ffn * v).reshape(4, 8, D), axis=0)

        loop(RC // 32, last)

    for d in (1, 2, 3):
        wait_bytes(sgz.at[d - 1], rsem.at[i_sgz + d])
    sgf[...] = sg[seq] + sgx[z] + (sgz[0] + sgz[1] + sgz[2])
    for j in range(3):
        v = jnp.sum(stat[j * 8 : (j + 1) * 8, :], axis=0, keepdims=True)
        sgf[9 + j : 10 + j, :] = jnp.broadcast_to(jnp.sum(v, axis=1, keepdims=True), (1, 128))
    for d in (1, 2, 3):
        rcopy(sgf, sgc.at[d], cpeer(d), i_sgc + d).start()
        sent(sgf, i_sgc + d)

    dw_end(zr_qkv, fin_qkv, i_qwz)
    for d in (1, 2, 3):
        c2 = (ctx + d) % 4
        for a, b in qkv_pieces(ctx):
            rcopy(fin_qkv.at[pl.ds(mul(c2 * 32, 32), 32), b], o_dqkv.at[:, a], cpeer(d), i_qf + d).start()
        sent(fin_qkv.at[pl.ds(0, 32), :], i_qf + d)
    for a, b in qkv_pieces(ctx):
        o_dqkv[:, a] = fin_qkv[mine32, b]

    for d in (1, 2, 3):
        wait_bytes(sgc.at[d], rsem.at[i_sgc + d])
    o_small[...] = sgf[...] + jnp.where(rowid != 8, sgc[1] + sgc[2] + sgc[3], 0.0)

    @pl.when(ctx != t)
    def _():
        wait_bytes(o_dout, rsem.at[i_of + (ctx - t + 4) % 4])

    for d in (1, 2, 3):
        wait_bytes(fin_up.at[pl.ds(0, 32), :], rsem.at[i_uf + d])
        wait_bytes(fin_qkv.at[pl.ds(0, 32), :], rsem.at[i_qf + d])
    dw_zsent(768, i_qwz)
    dw_xsent(768, i_qwx)
    rs_sent(rs_s, i_g1)
    rs_sent(rt_s, i_ff)
    flush()
    assert next(ids) <= NSEM, next(ids)


def fast(mesh):
    def scratch():
        v = lambda dt, *shape: pltpu.VMEM(shape, dt)
        return [
            v(bf16, D, 768), v(bf16, 256, D), v(bf16, D, D), v(bf16, D, D),
            v(f32, 4, 16, 128), v(f32, 8, 16, 128), v(f32, 16, D),
            v(bf16, S, D), v(bf16, S, D), v(bf16, S, D), v(bf16, S, D), v(bf16, S, D), v(bf16, S, D),
            v(bf16, S, 768), v(bf16, 256, S), v(bf16, 256, S), v(bf16, 256, S),
            v(bf16, 256, S), v(bf16, S, 128), v(bf16, S, 768), v(f32, 4, 8, S),
            v(bf16, 4, 10, 256, 256), v(f32, 2, S, 128), v(f32, 2, S, 128),
            v(bf16, 3, 2, 128, D), v(bf16, 3, 2, 128, D), v(f32, 2, 128, D),
            v(bf16, 3, 2, 128, D), v(bf16, 3, 2, 128, D), v(f32, 2, 128, D),
            v(f32, 128, D), v(f32, R, D),
            v(bf16, 512, D), v(bf16, 512, D), v(bf16, 512, D), v(bf16, 512, 768), v(bf16, 256, D),
            v(f32, 512, D), v(f32, 512, D), v(f32, 256, D),
            v(bf16, 3, 128, D), v(bf16, 2, 128, D),
            v(bf16, 3, 128, D), v(bf16, 3, 128, D), v(bf16, 3, 128, 768), v(bf16, 3, 128, D),
            v(f32, 128, D), v(f32, 128, 768), v(f32, 128, D),
            v(f32, 8, 16, 128), v(f32, 4, 16, 128), v(f32, 3, 16, 128), v(f32, 3, 16, 128),
            v(f32, 16, 128), v(f32, 4, 16, 128), v(f32, 8, 8, D), v(f32, 16, D), v(f32, 24, D),
            pltpu.SemaphoreType.DMA((8,)),
            pltpu.SemaphoreType.DMA((NSEM,)),
            pltpu.SemaphoreType.DMA((NSEM,)),
        ]

    def on_device(tokens, lengths, cotangent, g1, b1, wq, qb, vb, wo, ob, g2, b2, wu, ub, wd, db):
        ctx = lax.axis_index("ctx")
        vectors = jnp.stack([g1, b1, qb, vb, ob, g2, b2, db]).astype(f32)
        place = (jnp.arange(128) // 32) == ctx
        small = jnp.concatenate([
            jnp.where(place[None], jnp.tile(vectors, (1, 4)), 0.0),
            ub.astype(f32)[None], jnp.zeros((7, 128), f32)])
        vm = pl.BlockSpec(memory_space=pltpu.VMEM)
        sds = jax.ShapeDtypeStruct
        out, grad, dqkv, dout, dup, ddown, sums = pl.pallas_call(
            block_kernel,
            out_shape=(sds((R, D), bf16), sds((R, D), f32), sds((32, 3 * D), f32), sds((32, D), f32),
                       sds((32, 4 * D), f32), sds((128, D), f32), sds((16, 128), f32)),
            in_specs=[pl.BlockSpec(memory_space=pltpu.SMEM)] + [vm] * 7,
            out_specs=tuple([vm] * 7),
            scratch_shapes=scratch(),
            compiler_params=pltpu.CompilerParams(
                collective_id=0, has_side_effects=True, vmem_limit_bytes=LIMIT),
            name="block",
        )(lengths, tokens[0], cotangent[0], small, wq, wo, wu, wd)
        mine = lax.dynamic_slice(sums, (0, ctx * 32), (8, 32))
        stats = jnp.sqrt(sums[9:12, 0] / (lengths[0].astype(f32) * D))[None]
        return (out[None], grad[None], mine[0], mine[1], dqkv, mine[2], mine[3], dout, mine[4],
                mine[5], mine[6], dup, sums[8], ddown, mine[7], stats)

    return on_device


HEADS = 16


epsilon = 1e-05


def normalize(inputs, gain, shift):
    average = jnp.mean(inputs, axis=-1, keepdims=True)
    centred = inputs - average
    variance = jnp.mean(centred * centred, axis=-1, keepdims=True)
    return centred * lax.rsqrt(variance + epsilon) * gain + shift


def gelu_tanh(inputs):
    return jax.nn.gelu(inputs, approximate=True)


def inner_rows(left, right):
    return lax.dot_general(
        left, right, (((0,), (0,)), ((), ())), preferred_element_type=jnp.float32
    )


def outer_cols(left, right):
    return lax.dot_general(
        left, right, (((1,), (1,)), ((), ())), preferred_element_type=jnp.float32
    )


def alibi_scores(query_block, key_block, query_pos, key_pos, slope_block):
    raw = jnp.einsum("qhd,khd->hqk", query_block, key_block, preferred_element_type=jnp.float32)
    offset = (key_pos[None, :] - query_pos[:, None]).astype(jnp.float32)
    scores = raw * query_block.shape[-1] ** (-0.5) + slope_block[:, None, None] * offset[None]
    allowed = key_pos[None, :] <= query_pos[:, None]
    return (scores, allowed)


def score_grads(
    query_block,
    key_block,
    value_block,
    grad_block,
    query_pos,
    key_pos,
    slope_block,
    log_block,
    delta_block,
):
    scores, allowed = alibi_scores(query_block, key_block, query_pos, key_pos, slope_block)
    probs = jnp.where(allowed[None], jnp.exp(scores - log_block[..., None]), 0.0)
    grad_probs = jnp.einsum(
        "qhd,khd->hqk", grad_block, value_block, preferred_element_type=jnp.float32
    )
    delta_block = jnp.sum(probs * grad_probs, axis=-1)
    grad_scores = (probs * (grad_probs - delta_block[..., None])).astype(jnp.bfloat16)
    return (probs, grad_scores, delta_block)


def on_device(
    tokens,
    lengths,
    cotangent,
    ln1_gain,
    ln1_bias,
    qkv_weight,
    query_bias,
    value_bias,
    out_weight,
    out_bias,
    ln2_gain,
    ln2_bias,
    up_weight,
    up_bias,
    down_weight,
    down_bias,
):
    shards = (
        ln1_gain,
        ln1_bias,
        qkv_weight,
        query_bias,
        value_bias,
        out_weight,
        out_bias,
        ln2_gain,
        ln2_bias,
        up_weight,
        up_bias,
        down_weight,
        down_bias,
    )
    row_count = tokens.shape[1]
    model_width = tokens.shape[2]
    head_count = HEADS
    head_width = model_width // head_count
    per_block = 2
    block_count = head_count // per_block
    slot_rows = row_count * lax.axis_size("ctx")
    positions = lax.axis_index("ctx") * row_count + jnp.arange(row_count, dtype=jnp.int32)
    length = lengths[0]
    valid_rows = (positions < length).astype(jnp.float32)[:, None]
    slopes = jnp.exp2(-8.0 * (jnp.arange(head_count, dtype=jnp.float32) + 1.0) / head_count)
    key_positions = jnp.arange(slot_rows, dtype=jnp.int32)
    scale = head_width ** (-0.5)
    full_weights = (
        lax.all_gather(shards[0], ("seq", "ctx"), axis=0, tiled=True),
        lax.all_gather(shards[1], ("seq", "ctx"), axis=0, tiled=True),
        lax.all_gather(shards[2], ("seq", "ctx"), axis=0, tiled=True),
        lax.all_gather(shards[3], ("seq", "ctx"), axis=0, tiled=True),
        lax.all_gather(shards[4], ("seq", "ctx"), axis=0, tiled=True),
        lax.all_gather(shards[5], ("seq", "ctx"), axis=0, tiled=True),
        lax.all_gather(shards[6], ("seq", "ctx"), axis=0, tiled=True),
        lax.all_gather(shards[7], ("seq", "ctx"), axis=0, tiled=True),
        lax.all_gather(shards[8], ("seq", "ctx"), axis=0, tiled=True),
        lax.all_gather(shards[9], ("seq", "ctx"), axis=0, tiled=True),
        lax.all_gather(shards[10], ("seq", "ctx"), axis=0, tiled=True),
        lax.all_gather(shards[11], ("seq", "ctx"), axis=0, tiled=True),
        lax.all_gather(shards[12], ("seq", "ctx"), axis=0, tiled=True),
    )
    (
        gain_one,
        shift_one,
        w_qkv,
        bias_query,
        bias_value,
        w_out,
        bias_out,
        gain_two,
        shift_two,
        w_up,
        bias_up,
        w_down,
        bias_down,
    ) = full_weights

    def pick(array, index):
        return lax.dynamic_slice_in_dim(array, index * per_block, per_block, 1)

    def pick_slopes(index):
        return lax.dynamic_slice_in_dim(slopes, index * per_block, per_block, 0)

    def to_blocks(array):
        return array.transpose(1, 0, 2, 3).reshape(array.shape[1], model_width)

    source = tokens[0].astype(jnp.float32)
    normed_one, back_one = jax.vjp(normalize, source, gain_one, shift_one)
    normed_low = normed_one.astype(jnp.bfloat16)
    mixed = jnp.dot(normed_low, w_qkv, preferred_element_type=jnp.float32)
    query = (mixed[:, :model_width] + bias_query).astype(jnp.bfloat16)
    keys = mixed[:, model_width : 2 * model_width].astype(jnp.bfloat16)
    values = (mixed[:, 2 * model_width :] + bias_value).astype(jnp.bfloat16)
    all_keys, all_values = (
        lax.all_gather(keys, "ctx", axis=0, tiled=True),
        lax.all_gather(values, "ctx", axis=0, tiled=True),
    )
    query_heads = query.reshape(row_count, head_count, head_width)
    key_heads = all_keys.reshape(slot_rows, head_count, head_width)
    value_heads = all_values.reshape(slot_rows, head_count, head_width)

    def forward_block(index):
        scores, allowed = alibi_scores(
            pick(query_heads, index),
            pick(key_heads, index),
            positions,
            key_positions,
            pick_slopes(index),
        )
        masked = jnp.where(allowed[None], scores, -1e30)
        highest = jnp.max(masked, axis=-1)
        total = jnp.sum(jnp.exp(masked - highest[..., None]), axis=-1)
        log_total = highest + jnp.log(total)
        probs = jnp.where(allowed[None], jnp.exp(scores - log_total[..., None]), 0.0)
        block_out = jnp.einsum(
            "hqk,khd->qhd",
            probs.astype(jnp.bfloat16),
            pick(value_heads, index),
            preferred_element_type=jnp.float32,
        )
        return (block_out, log_total)

    head_out, log_totals = lax.map(forward_block, jnp.arange(block_count))
    attended = to_blocks(head_out).astype(jnp.bfloat16)
    branch = jnp.dot(attended, w_out, preferred_element_type=jnp.float32) + bias_out
    resid = source + branch
    normed_two, back_two = jax.vjp(normalize, resid, gain_two, shift_two)
    normed_two_low = normed_two.astype(jnp.bfloat16)
    pre_act = jnp.dot(normed_two_low, w_up, preferred_element_type=jnp.float32) + bias_up
    activated, back_act = jax.vjp(gelu_tanh, pre_act)
    activated_low = activated.astype(jnp.bfloat16)
    ffn = jnp.dot(activated_low, w_down, preferred_element_type=jnp.float32) + bias_down
    output = (valid_rows * (resid + ffn)).astype(jnp.bfloat16)[None]
    squares = jnp.stack(
        [
            jnp.sum(valid_rows * branch * branch),
            jnp.sum(valid_rows * resid * resid),
            jnp.sum(valid_rows * ffn * ffn),
        ]
    )
    totals = lax.psum(squares, "ctx")
    stats = jnp.sqrt(totals / (length.astype(jnp.float32) * model_width))[None]
    w_qkv, w_out, w_up, w_down = (
        lax.all_gather(qkv_weight, ("seq", "ctx"), axis=0, tiled=True),
        lax.all_gather(out_weight, ("seq", "ctx"), axis=0, tiled=True),
        lax.all_gather(up_weight, ("seq", "ctx"), axis=0, tiled=True),
        lax.all_gather(down_weight, ("seq", "ctx"), axis=0, tiled=True),
    )
    grad_out = cotangent[0].astype(jnp.float32) * valid_rows
    grad_ffn = grad_out.astype(jnp.bfloat16)
    grad_down_w = inner_rows(activated_low, grad_ffn)
    grad_down_b = jnp.sum(grad_ffn.astype(jnp.float32), axis=0)
    grad_activated = outer_cols(grad_ffn, w_down)
    (grad_pre,) = back_act(grad_activated)
    grad_pre_low = grad_pre.astype(jnp.bfloat16)
    grad_up_w = inner_rows(normed_two_low, grad_pre_low)
    grad_up_b = jnp.sum(grad_pre_low.astype(jnp.float32), axis=0)
    grad_normed_two = outer_cols(grad_pre_low, w_up)
    grad_resid_norm, grad_gain_two, grad_shift_two = back_two(grad_normed_two)
    grad_resid = grad_out + grad_resid_norm
    grad_branch = grad_resid.astype(jnp.bfloat16)
    grad_out_w = inner_rows(attended, grad_branch)
    grad_out_b = jnp.sum(grad_branch.astype(jnp.float32), axis=0)
    grad_attended = outer_cols(grad_branch, w_out).astype(jnp.bfloat16)
    grad_heads = grad_attended.reshape(row_count, head_count, head_width)

    def backward_block(index):
        query_block = pick(query_heads, index)
        key_block = pick(key_heads, index)
        grad_block = pick(grad_heads, index)
        probs, grad_scores, delta_block = score_grads(
            query_block,
            key_block,
            pick(value_heads, index),
            grad_block,
            positions,
            key_positions,
            pick_slopes(index),
            log_totals[index],
            None,
        )
        grad_query_block = (
            jnp.einsum("hqk,khd->qhd", grad_scores, key_block, preferred_element_type=jnp.float32)
            * scale
        )
        grad_key_block = (
            jnp.einsum("hqk,qhd->khd", grad_scores, query_block, preferred_element_type=jnp.float32)
            * scale
        )
        grad_value_block = jnp.einsum(
            "hqk,qhd->khd",
            probs.astype(jnp.bfloat16),
            grad_block,
            preferred_element_type=jnp.float32,
        )
        return (grad_query_block, grad_key_block, grad_value_block)

    query_parts, key_parts, value_parts = lax.map(backward_block, jnp.arange(block_count))
    grad_query_all = to_blocks(query_parts)
    own_keys, own_values = (
        lax.psum_scatter(
            to_blocks(key_parts).astype(jnp.bfloat16), "ctx", scatter_dimension=0, tiled=True
        ).astype(jnp.float32),
        lax.psum_scatter(
            to_blocks(value_parts).astype(jnp.bfloat16), "ctx", scatter_dimension=0, tiled=True
        ).astype(jnp.float32),
    )
    grad_query_low = grad_query_all.astype(jnp.bfloat16)
    grad_key_low = own_keys.astype(jnp.bfloat16)
    grad_value_low = own_values.astype(jnp.bfloat16)
    grad_mixed = jnp.concatenate([grad_query_low, grad_key_low, grad_value_low], axis=1)
    grad_qkv_w = inner_rows(normed_low, grad_mixed)
    grad_query_bias = jnp.sum(grad_query_low.astype(jnp.float32), axis=0)
    grad_value_bias = jnp.sum(grad_value_low.astype(jnp.float32), axis=0)
    grad_normed_one = outer_cols(grad_mixed, w_qkv)
    grad_source_norm, grad_gain_one, grad_shift_one = back_one(grad_normed_one)
    grad_tokens = (grad_resid + grad_source_norm)[None]
    summed = (
        lax.psum_scatter(
            grad_gain_one.astype(jnp.float32), ("seq", "ctx"), scatter_dimension=0, tiled=True
        ),
        lax.psum_scatter(
            grad_shift_one.astype(jnp.float32), ("seq", "ctx"), scatter_dimension=0, tiled=True
        ),
        lax.psum_scatter(grad_qkv_w, ("seq", "ctx"), scatter_dimension=0, tiled=True),
        lax.psum_scatter(grad_query_bias, ("seq", "ctx"), scatter_dimension=0, tiled=True),
        lax.psum_scatter(grad_value_bias, ("seq", "ctx"), scatter_dimension=0, tiled=True),
        lax.psum_scatter(grad_out_w, ("seq", "ctx"), scatter_dimension=0, tiled=True),
        lax.psum_scatter(grad_out_b, ("seq", "ctx"), scatter_dimension=0, tiled=True),
        lax.psum_scatter(
            grad_gain_two.astype(jnp.float32), ("seq", "ctx"), scatter_dimension=0, tiled=True
        ),
        lax.psum_scatter(
            grad_shift_two.astype(jnp.float32), ("seq", "ctx"), scatter_dimension=0, tiled=True
        ),
        lax.psum_scatter(grad_up_w, ("seq", "ctx"), scatter_dimension=0, tiled=True),
        lax.psum_scatter(grad_up_b, ("seq", "ctx"), scatter_dimension=0, tiled=True),
        lax.psum_scatter(grad_down_w, ("seq", "ctx"), scatter_dimension=0, tiled=True),
        lax.psum_scatter(grad_down_b, ("seq", "ctx"), scatter_dimension=0, tiled=True),
    )
    return (output, grad_tokens) + tuple(summed) + (stats,)


def solution(mesh):
    small_slice = mesh.shape["seq"] == 8 and mesh.shape["ctx"] == 4
    placed = (
        P("seq", "ctx", None),
        P("seq"),
        P("seq", "ctx", None),
        P(("seq", "ctx")),
        P(("seq", "ctx")),
        P(("seq", "ctx"), None),
        P(("seq", "ctx")),
        P(("seq", "ctx")),
        P(("seq", "ctx"), None),
        P(("seq", "ctx")),
        P(("seq", "ctx")),
        P(("seq", "ctx")),
        P(("seq", "ctx"), None),
        P(("seq", "ctx")),
        P(("seq", "ctx"), None),
        P(("seq", "ctx")),
    )
    return jax.shard_map(
        fast(mesh) if small_slice else on_device,
        mesh=mesh,
        in_specs=placed,
        out_specs=(
            P("seq", "ctx", None),
            P("seq", "ctx", None),
            P(("seq", "ctx")),
            P(("seq", "ctx")),
            P(("seq", "ctx"), None),
            P(("seq", "ctx")),
            P(("seq", "ctx")),
            P(("seq", "ctx"), None),
            P(("seq", "ctx")),
            P(("seq", "ctx")),
            P(("seq", "ctx")),
            P(("seq", "ctx"), None),
            P(("seq", "ctx")),
            P(("seq", "ctx"), None),
            P(("seq", "ctx")),
            P("seq", None),
        ),
        check_vma=False,
    )
```

```python
import itertools

import jax
import jax.numpy as jnp
from jax import lax
from jax.experimental import pallas as pl
from jax.experimental.pallas import tpu as pltpu
from jax.sharding import PartitionSpec as P

MESH = pl.DeviceIdType.MESH
bf16, f32 = jnp.bfloat16, jnp.float32
LOG2E = 1.4426950408889634
D = 1024
R = 256
S = 1024
LIMIT = 66_000_000
NSEM = 260
ORDER = (2, 3, 1)


def nn(a, b):
    return lax.dot_general(a, b, (((1,), (0,)), ((), ())), preferred_element_type=f32)


def nt(a, b):
    return lax.dot_general(a, b, (((1,), (1,)), ((), ())), preferred_element_type=f32)


def tn(a, b):
    return lax.dot_general(a, b, (((0,), (0,)), ((), ())), preferred_element_type=f32)


def mul(v, m):
    return pl.multiple_of(v, m)


def loop(n, body, start=0):
    def step(i, carry):
        body(i)
        return carry

    lax.fori_loop(start, n, step, 0)


def layer_stats(v):
    mean = jnp.sum(v, axis=-1, keepdims=True) * (1.0 / D)
    cen = v - mean
    var = jnp.sum(cen * cen, axis=-1, keepdims=True) * (1.0 / D)
    rstd = lax.rsqrt(var + 1e-5)
    return cen * rstd, rstd


def layer_back(g2, gain, z, rstd):
    g = g2 * gain
    m1 = jnp.sum(g, axis=-1, keepdims=True) * (1.0 / D)
    m2 = jnp.sum(g * z, axis=-1, keepdims=True) * (1.0 / D)
    return rstd * (g - m1 - z * m2)


def block_kernel(
    length_ref, tok, cot, small, qkv_in, out_in, up_in, down_in,
    o_out, o_grad, o_dqkv, o_dout, o_dup, o_ddown, o_small,
    wqkv, wout, wup, wdown, smc, smb, vec,
    n1, n2, gf, gb, act, gpre, qkv, vt, kt, attt, dot_, do_, dmix, linv,
    ptri, acck, accv,
    rs_s, rs_r, rs_own, rt_s, rt_r, rt_own, tmp, res,
    xs_down, xs_up, xr_down, xr_up, xr_qkv, xr_out, own_a, own_b, own_out,
    zr_down, zr_up, zr_qkv, zr_out, fin_up, fin_qkv, fin_out,
    sg, sgx, sgs, sgz, sgf, sgc, gvec, gmat, stat, qbias,
    lsem, ssem, rsem,
):
    seq, ctx = lax.axis_index("seq"), lax.axis_index("ctx")
    z, x = seq // 2, seq % 2
    y, k = ctx // 2, ctx % 2
    ids = itertools.count()
    lids = itertools.count()

    mate = {"ctx": y * 2 + (k + 1) % 2}
    ypeer = {"ctx": ((y + 1) % 2) * 2 + k}
    xpeer = {"seq": z * 2 + (x + 1) % 2}

    def cpeer(d):
        return {"ctx": (ctx + d) % 4}

    def zpeer(d):
        return {"seq": ((z + d) % 4) * 2 + x}

    def take(n=1):
        first = next(ids)
        for _ in range(n - 1):
            next(ids)
        return first

    def rcopy(src, dst, dev, i):
        return pltpu.make_async_remote_copy(
            src_ref=src, dst_ref=dst, send_sem=ssem.at[i], recv_sem=rsem.at[i],
            device_id=dev, device_id_type=MESH)

    def wait_bytes(ref, sem):
        pltpu.make_async_copy(ref, ref, sem).wait()

    sends = []

    def sent(ref, i, cond=None):
        sends.append((ref, i, cond))

    def flush():
        for ref, i, cond in sends:
            if cond is None:
                wait_bytes(ref, ssem.at[i])
            else:
                @pl.when(cond)
                def _(ref=ref, i=i):
                    wait_bytes(ref, ssem.at[i])
        sends.clear()

    rows = lambda c: pl.ds(mul(c * R, R), R)
    srow = lambda s: pl.ds(s * 128 if isinstance(s, int) else mul(s * 128, 128), 128)

    barrier = pltpu.get_barrier_semaphore()
    for d in (1, 2, 3):
        pl.semaphore_signal(barrier, inc=1, device_id=cpeer(d), device_id_type=MESH)
        pl.semaphore_signal(barrier, inc=1, device_id=zpeer(d), device_id_type=MESH)
    pl.semaphore_signal(barrier, inc=1, device_id=xpeer, device_id_type=MESH)
    pl.semaphore_wait(barrier, 7)

    i_smc = take(4)
    for d in (1, 2, 3):
        rcopy(small, smc.at[d], cpeer(d), i_smc + d).start()
        sent(small, i_smc + d)
    own32 = pl.ds(mul(seq * 128 + ctx * 32, 32), 32)

    def qkv_pieces(c):
        for j in range(6):
            yield (pl.ds(mul((j % 3) * D + (c + 4 * (j // 3)) * 128, 128), 128),
                   pl.ds(j * 128, 128))

    i_qa = take(4)
    for d in (1, 2, 3):
        for a, b in qkv_pieces((ctx + d) % 4):
            rcopy(qkv_in.at[:, a], wqkv.at[own32, b], cpeer(d), i_qa + d).start()
        sent(wqkv.at[pl.ds(0, 32), :], i_qa + d)
    l_q = next(lids)
    for a, b in qkv_pieces(ctx):
        pltpu.make_async_copy(qkv_in.at[:, a], wqkv.at[own32, b], lsem.at[l_q]).start()

    t = seq % 4
    out32 = pl.ds(mul((seq // 4) * 128 + ctx * 32, 32), 32)
    i_oa = take()
    l_o = next(lids)

    @pl.when(ctx != t)
    def _():
        rcopy(out_in, wout.at[out32, :], {"ctx": t}, i_oa).start()

    sent(out_in, i_oa, ctx != t)

    @pl.when(ctx == t)
    def _():
        pltpu.make_async_copy(out_in, wout.at[out32, :], lsem.at[l_o]).start()

    i_ua = take(4)
    for d in (1, 2, 3):
        c2 = (ctx + d) % 4
        for s in range(8):
            rcopy(up_in.at[:, pl.ds(mul((s * 4 + c2) * 128, 128), 128)],
                  wup.at[own32, pl.ds(s * 128, 128)], cpeer(d), i_ua + d).start()
        sent(wup.at[pl.ds(0, 32), :], i_ua + d)
    l_u = next(lids)
    for s in range(8):
        pltpu.make_async_copy(up_in.at[:, pl.ds(mul((s * 4 + ctx) * 128, 128), 128)],
                              wup.at[own32, pl.ds(s * 128, 128)], lsem.at[l_u]).start()

    for d in (1, 2, 3):
        rcopy(small, smc.at[d], cpeer(d), i_smc + d).wait_recv()
    rowid = lax.broadcasted_iota(jnp.int32, (16, 128), 0)
    smb[seq] = small[...] + jnp.where(rowid < 8, smc[1] + smc[2] + smc[3], 0.0)

    def gather_z(block, zi, src=None):
        own = block(seq) if src is None else src
        for d in ORDER:
            rcopy(own, block(seq), zpeer(d), zi + d).start()
            sent(own, zi + d)

    def gather_x(block, xi, src=None):
        own = block(seq) if src is None else src
        rcopy(own, block(seq), xpeer, xi).start()
        sent(own, xi)

    def gather_forward(block, zi, xi, d):
        b = block(((z - d + 4) % 4) * 2 + x)
        rcopy(b, b, xpeer, zi + d).wait_recv()
        rcopy(b, b, xpeer, xi + d).start()
        sent(block(0), xi + d)

    def gather_finish(block, xi):
        for d in range(4):
            b = block(seq)
            rcopy(b, b, xpeer, xi + d).wait_recv()

    def relay_start(block, i, src=None):
        own = block(seq) if src is None else src
        for cond, step, first in ((z < 3, 1, i), (z > 0, -1, i + 4)):
            @pl.when(cond)
            def _(step=step, first=first):
                rcopy(own, block(seq), {"seq": (z + step) * 2 + x}, first + 1).start()

            sent(own, first + 1, cond)

    def relay_x(block, i, src=None):
        own = block(seq) if src is None else src
        rcopy(own, block(seq), xpeer, i + 8 + z).start()
        sent(own, i + 8 + z)

    def relay_step(block, i, j):
        for has, on, step, first in ((z >= j, z < 3, 1, i), (z + j <= 3, z > 0, -1, i + 4)):
            zz = z - j * step

            @pl.when(has)
            def _(on=on, step=step, first=first, zz=zz):
                b = block(zz * 2 + x)
                rcopy(b, b, xpeer, first + j).wait_recv()
                if j < 3:
                    @pl.when(on)
                    def _():
                        rcopy(b, b, {"seq": (z + step) * 2 + x}, first + j + 1).start()
                rcopy(b, b, xpeer, i + 8 + zz).start()

            if j < 3:
                sent(block(0), first + j + 1, jnp.logical_and(has, on))

    def relay_finish(block, i):
        for zz in range(4):
            rcopy(block(0), block(0), xpeer, i + 8 + zz).wait_recv()

    def relay_sent(block, i):
        for j in (1, 2, 3):
            for has, zz in ((z >= j, z - j), (z + j <= 3, z + j)):
                @pl.when(has)
                def _(zz=zz):
                    wait_bytes(block(0), ssem.at[i + 8 + zz])

    small_block = lambda s: smb.at[s]
    i_sz, i_sx = take(4), take(4)
    gather_z(small_block, i_sz)
    gather_x(small_block, i_sx)

    for d in (1, 2, 3):
        wait_bytes(wqkv.at[pl.ds(0, 32), :], rsem.at[i_qa + d])
    wait_bytes(wqkv.at[pl.ds(0, 32), :], lsem.at[l_q])
    qkv_block = lambda s: wqkv.at[srow(s), :]
    i_qr = take(12)
    relay_start(qkv_block, i_qr)
    for d in ORDER:
        gather_forward(small_block, i_sz, i_sx, d)
    relay_x(qkv_block, i_qr)
    l_d = next(lids)
    down_block = lambda s: wdown.at[srow(s), :]
    i_dr = take(12)
    relay_x(down_block, i_dr, src=down_in)
    pltpu.make_async_copy(down_in, down_block(seq), lsem.at[l_d]).start()

    gather_finish(small_block, i_sx)
    for s in range(8):
        vec[:, s * 128 : (s + 1) * 128] = smb[s]

    length = length_ref[0]
    my = mul(ctx * R, R)

    def valid_rows(r0, n):
        pos = lax.broadcasted_iota(jnp.int32, (n, 1), 0) + (ctx * R + r0)
        return jnp.where(pos < length, 1.0, 0.0).astype(f32)

    CH = 2
    RC = R // CH

    def chunk(buf, c, ch):
        return buf.at[pl.ds(mul(c * R + ch * RC, RC), RC), :]

    def ag_start(buf, i, ch):
        own = chunk(buf, ctx, ch)
        rcopy(own, own, ypeer, i + CH + ch).start()
        rcopy(own, own, mate, i + ch).start()
        if buf is not gf and buf is not n2:
            sent(own, i + CH + ch)
            sent(own, i + ch)

    def ag_forward(buf, i, ch):
        b = chunk(buf, ((y + 1) % 2) * 2 + k, ch)
        rcopy(b, b, mate, i + CH + ch).wait_recv()
        rcopy(b, b, mate, i + 2 * CH + ch).start()
        if buf is not gf and buf is not n2:
            sent(buf.at[pl.ds(0, RC), :], i + 2 * CH + ch)

    def ag_wait(buf, i, which):
        for ch in range(CH):
            b = chunk(buf, ctx, ch)
            rcopy(b, b, mate, i + which * CH + ch).wait_recv()

    i_n1 = take(3 * CH)
    for ch in range(CH):
        def first(q, ch=ch):
            r0 = mul(ch * RC + q * 32, 32)
            zz, _ = layer_stats(tok[pl.ds(r0, 32), :].astype(f32))
            n1[pl.ds(mul(my + r0, 32), 32), :] = (zz * vec[0:1, :] + vec[1:2, :]).astype(bf16)

        loop(RC // 32, first)
        ag_start(n1, i_n1, ch)


    def mask_rows(q):
        r0 = mul(q * 32, 32)
        g = cot[pl.ds(r0, 32), :].astype(f32) * valid_rows(r0, 32)
        gf[pl.ds(mul(my + r0, 32), 32), :] = g.astype(bf16)

    loop(R // 32, mask_rows)
    i_gf = take(3 * CH)
    for ch in range(CH):
        ag_start(gf, i_gf, ch)
    for j in range(6):
        if j % 3 == 1:
            qbias[:, j * 128 : (j + 1) * 128] = jnp.zeros((8, 128), f32)
        else:
            r = 2 + j % 3 // 2
            b = vec[r : r + 1, pl.ds(mul((ctx + 4 * (j // 3)) * 128, 128), 128)]
            qbias[:, j * 128 : (j + 1) * 128] = jnp.broadcast_to(b, (8, 128))
    relay_step(qkv_block, i_qr, 1)
    relay_step(qkv_block, i_qr, 2)
    ag_forward(n1, i_n1, 0)
    relay_step(qkv_block, i_qr, 3)
    i_oz, i_ox = take(4), take(4)
    out_block = lambda zz: wout.at[pl.ds(mul((zz // 2) * 128, 128), 128), :]

    @pl.when(ctx == t)
    def _():
        wait_bytes(wout.at[pl.ds(0, 96), :], rsem.at[i_oa])
        wait_bytes(wout.at[pl.ds(0, 32), :], lsem.at[l_o])
        for d in (1, 2, 3):
            rcopy(out_block(z), out_block(z), zpeer(d), i_oz + d).start()
        rcopy(out_block(z), out_block(z), xpeer, i_ox).start()

    for d in (1, 2, 3):
        sent(out_block(z), i_oz + d, ctx == t)
    sent(out_block(z), i_ox, ctx == t)

    for d in (1, 2, 3):
        wait_bytes(wup.at[pl.ds(0, 32), :], rsem.at[i_ua + d])
    wait_bytes(wup.at[pl.ds(0, 32), :], lsem.at[l_u])
    up_block = lambda s: wup.at[srow(s), :]
    i_ur = take(12)
    relay_start(up_block, i_ur)
    ag_forward(n1, i_n1, 1)

    ag_wait(n1, i_n1, 0)
    relay_finish(qkv_block, i_qr)
    relay_x(up_block, i_ur)

    def project(it):
        blk = ((y + it // 2) % 2) * 2 + (k + it % 2) % 2

        @pl.when(it == 3)
        def _():
            ag_wait(n1, i_n1, 2)

        qkv[rows(blk), :] = (nn(n1[rows(blk), :], wqkv[...]) + qbias[0:1, :]).astype(bf16)

    loop(4, project)
    mine = x == k
    for d in (1, 2, 3):
        zz = (z - d + 4) % 4

        @pl.when(jnp.logical_and(mine, zz % 2 == y))
        def _(d=d, zz=zz):
            rcopy(out_block(zz), out_block(zz), xpeer, i_oz + d).wait_recv()
            rcopy(out_block(zz), out_block(zz), xpeer, i_ox + d).start()

        sent(out_block(zz), i_ox + d, jnp.logical_and(mine, zz % 2 == y))

    relay_step(up_block, i_ur, 1)
    relay_start(down_block, i_dr, src=down_in)

    def turn(i):
        c0 = pl.ds(mul(i * 128, 128), 128)
        vt[c0, :] = qkv[:, pl.ds(mul(i * 384 + 256, 128), 128)].T
        kt[c0, :] = qkv[:, pl.ds(mul(i * 384 + 128, 128), 128)].T

    loop(2, turn)

    lane = lax.broadcasted_iota(jnp.int32, (256, 128), 1)
    krow = lax.broadcasted_iota(jnp.int32, (256, 256), 0)
    qcol = lax.broadcasted_iota(jnp.int32, (256, 256), 1)

    def tri(kb, qb):
        return (qb * (qb + 1)) // 2 + kb

    def half(v, j):
        return jnp.where((lane // 64) == j, v, jnp.zeros_like(v))

    def pair_forward(i):
        for j in range(2):
            slope = jnp.exp2(jnp.full((1024, 128), -0.5, f32)
                             * (2 * ctx + 8 * i + j + 1).astype(f32)) * LOG2E
            b = slope * lax.broadcasted_iota(jnp.int32, (1024, 128), 0).astype(f32)
            for kb in range(4):
                own_b[j * 256 : (j + 1) * 256, kb * 128 : (kb + 1) * 128] = b[kb * 256 : (kb + 1) * 256]

        def queries(qb):
            q0 = pl.ds(mul(qb * 256, 256), 256)
            qblk = qkv[q0, pl.ds(mul(i * 384, 128), 128)]

            def scores(kb, best):
                k0 = pl.ds(mul(kb * 256, 256), 256)
                kblk = qkv[k0, pl.ds(mul(i * 384 + 128, 128), 128)]
                new = []
                for j in range(2):
                    b = own_b[j * 256 : (j + 1) * 256, pl.ds(mul(kb * 128, 128), 128)]
                    sc = nt(half(kblk, j), qblk) * (0.125 * LOG2E) + jnp.concatenate([b, b], axis=1)
                    sc = jnp.where(krow + kb * 256 <= qcol + qb * 256, sc, -1e30)
                    own_a[j * 256 : (j + 1) * 256, k0] = sc
                    new.append(jnp.maximum(best[j], jnp.max(sc.reshape(32, 8, 256), axis=0)))
                return tuple(new)

            low = jnp.full((8, 256), -3e38, f32)
            best = lax.fori_loop(0, qb + 1, scores, (low, low))
            top = [jnp.max(b, axis=0, keepdims=True) for b in best]

            def weigh(kb, carry):
                k0 = pl.ds(mul(kb * 256, 256), 256)
                new = []
                for j in range(2):
                    total, acc = carry[2 * j], carry[2 * j + 1]
                    p = jnp.exp2(own_a[j * 256 : (j + 1) * 256, k0] - top[j])
                    total = total + jnp.sum(p.reshape(32, 8, 256), axis=0)
                    p = p.astype(bf16)
                    ptri[2 * i + j, tri(kb, qb)] = p
                    v = vt[pl.ds(mul(i * 128 + j * 64, 64), 64), k0]
                    new += [total, acc + nn(v, p)]
                return tuple(new)

            zero = (jnp.zeros((8, 256), f32), jnp.zeros((64, 256), f32))
            out = lax.fori_loop(0, qb + 1, weigh, zero + zero)
            for j in range(2):
                inv = 1.0 / jnp.sum(out[2 * j], axis=0, keepdims=True)
                linv[2 * i + j, :, q0] = jnp.broadcast_to(inv, (8, 256))
                attt[pl.ds(mul(i * 128 + j * 64, 64), 64), q0] = (out[2 * j + 1] * inv).astype(bf16)

        loop(4, queries)

    pair_forward(0)
    for ch in range(CH):
        ag_forward(gf, i_gf, ch)
    pair_forward(1)

    relay_step(up_block, i_ur, 2)
    def rs_run(partial, sb, rb, own, i):
        def step(tt):
            g, ch, sub = tt // 4, tt % 2, (tt // 2) % 2
            blk = ((y + 1 - g) % 2) * 2 + (k + 1 - sub) % 2
            partial(blk, ch, tmp)

            @pl.when(jnp.logical_and(g == 0, sub == 0))
            def _():
                sb[0, ch] = tmp[...].astype(bf16)
                rcopy(sb.at[0, ch], rb.at[0, ch], mate, i + ch).start()

            @pl.when(jnp.logical_and(g == 0, sub == 1))
            def _():
                rcopy(sb.at[0, ch], rb.at[0, ch], mate, i + ch).wait_recv()
                sb[1, ch] = (tmp[...] + rb[0, ch].astype(f32)).astype(bf16)
                rcopy(sb.at[1, ch], rb.at[1, ch], ypeer, i + CH + ch).start()

            @pl.when(jnp.logical_and(g == 1, sub == 0))
            def _():
                sb[2, ch] = tmp[...].astype(bf16)
                rcopy(sb.at[2, ch], rb.at[2, ch], mate, i + 2 * CH + ch).start()

            @pl.when(jnp.logical_and(g == 1, sub == 1))
            def _():
                own[ch] = tmp[...]

        loop(4 * CH, step)

    def rs_wait(sb, rb, i, ch):
        rcopy(sb.at[2, ch], rb.at[2, ch], mate, i + 2 * CH + ch).wait_recv()
        rcopy(sb.at[1, ch], rb.at[1, ch], mate, i + CH + ch).wait_recv()

    def rs_sum(rb, own, ch, r):
        return own[ch, r, :] + rb[2, ch, r, :].astype(f32) + rb[1, ch, r, :].astype(f32)

    def rs_sent(sb, i):
        for j in range(3):
            for ch in range(CH):
                wait_bytes(sb.at[j, ch], ssem.at[i + j * CH + ch])

    for d in range(4):
        zz = (z - d + 4) % 4

        @pl.when(jnp.logical_and(x != k, zz % 2 == y))
        def _(d=d):
            rcopy(out_block(z), out_block(z), xpeer, i_ox + d).wait_recv()

    def branch_part(blk, ch, dst):
        a = attt[:, pl.ds(mul(blk * R + ch * RC, RC), RC)]
        dst[...] = tn(a, wout[...])

    i_br = take(3 * CH)
    rs_run(branch_part, rs_s, rs_r, rs_own, i_br)
    relay_step(up_block, i_ur, 3)
    relay_step(down_block, i_dr, 1)

    i_n2 = take(3 * CH)
    stat[...] = jnp.zeros_like(stat)
    for ch in range(CH):
        rs_wait(rs_s, rs_r, i_br, ch)

        def second(q, ch=ch):
            r = pl.ds(mul(q * 32, 32), 32)
            r1 = pl.ds(mul(ch * RC + q * 32, 32), 32)
            branch = rs_sum(rs_r, rs_own, ch, r) + vec[4:5, :]
            resid = tok[r1, :].astype(f32) + branch
            res[r1, :] = resid
            zz, _ = layer_stats(resid)
            n2[pl.ds(mul(my + ch * RC + q * 32, 32), 32), :] = (
                zz * vec[5:6, :] + vec[6:7, :]).astype(bf16)
            v = valid_rows(ch * RC + q * 32, 32)
            stat[0:8, :] += jnp.sum((branch * branch * v).reshape(4, 8, D), axis=0)
            stat[8:16, :] += jnp.sum((resid * resid * v).reshape(4, 8, D), axis=0)

        loop(RC // 32, second)
        ag_start(n2, i_n2, ch)

    relay_step(down_block, i_dr, 2)
    relay_finish(up_block, i_ur)

    def feed(it):
        blk = ((y + it // 2) % 2) * 2 + (k + it % 2) % 2

        @pl.when(it == 1)
        def _():
            ag_wait(n2, i_n2, 0)
            ag_forward(n2, i_n2, 0)
            relay_step(down_block, i_dr, 3)

        @pl.when(it == 2)
        def _():
            ag_forward(n2, i_n2, 1)

        @pl.when(it == 3)
        def _():
            ag_wait(n2, i_n2, 2)

        def cols(n):
            c0 = pl.ds(mul(n * 512, 512), 512)
            pre = nn(n2[rows(blk), :], wup[:, c0]) + vec[8:9, c0]
            sq = pre * pre
            th = jnp.tanh(0.7978845608028654 * pre * (1.0 + 0.044715 * sq))
            a1 = 0.5 * (1.0 + th)
            act[rows(blk), c0] = (pre * a1).astype(bf16)
            der = a1 + 0.5 * pre * (1.0 - th * th) * (
                0.7978845608028654 * (1.0 + 0.134145 * sq))
            gpre[rows(blk), c0] = der.astype(bf16)

        loop(2, cols)

    loop(4, feed)

    def dw_half(a, b, c0, n, xx, hh):
        c1 = pl.ds(mul(((2 * hh) * 2 + xx) * 128, 128), 128)
        c2 = pl.ds(mul(((2 * hh + 1) * 2 + xx) * 128, 128), 128)
        return tn(jnp.concatenate([a[:, c1], a[:, c2]], axis=1), b[:, c0 : c0 + n])

    def dw_away(a, b, c0, n, xb, xr, i):
        def away(hh):
            r = pl.ds(mul(hh * 256, 256), 256)
            xb[r, c0 : c0 + n] = dw_half(a, b, c0, n, (x + 1) % 2, hh).astype(bf16)
            rcopy(xb.at[r, pl.ds(c0, n)], xr.at[r, pl.ds(c0, n)], xpeer, i + hh).start()
            sent(xb.at[pl.ds(0, 256), pl.ds(c0, n)], i + hh)

        for hh in range(2):
            away(hh)

    def dw_keep(a, b, c0, n, own):
        def keep(hh):
            own[pl.ds(mul(hh * 256, 256), 256), c0 : c0 + n] = dw_half(a, b, c0, n, x, hh)

        loop(2, keep)

    def dw_z(hh, c0, n, xr, own, zb, zo, zr, fin, i, iz):
        wait_bytes(xr.at[pl.ds(0, 256), pl.ds(c0, n)], rsem.at[i + hh])
        c = slice(c0, c0 + n)
        for zz in (2 * hh, 2 * hh + 1):
            r = slice(zz * 128, zz * 128 + 128)
            ro = slice(zo + zz * 128, zo + zz * 128 + 128)
            dz = (zz - z + 4) % 4

            @pl.when(zz == z)
            def _(r=r):
                fin[:, c] = own[r, c] + xr[r, c].astype(f32)

            @pl.when(zz != z)
            def _(r=r, ro=ro, zz=zz, dz=dz):
                zb[ro, c] = (own[r, c] + xr[r, c].astype(f32)).astype(bf16)
                rcopy(zb.at[ro, c], zr.at[dz - 1, :, c], {"seq": zz * 2 + x}, iz + dz).start()

            sent(zb.at[ro, c], iz + dz, zz != z)

    def dw_end(c0, n, zr, fin, iz):
        c = slice(c0, c0 + n)
        for d in (1, 2, 3):
            wait_bytes(zr.at[d - 1, :, c], rsem.at[iz + d])
        fin[:, c] += (zr[0, :, c].astype(f32) + zr[1, :, c].astype(f32)) + zr[2, :, c].astype(f32)

    ag_wait(gf, i_gf, 0)
    ag_wait(gf, i_gf, 2)
    i_dwx, i_dwz = take(2), take(4)
    dw_away(act, gf, 0, D, xs_down, xr_down, i_dwx)
    dw_keep(act, gf, 0, D, own_a)
    relay_finish(down_block, i_dr)
    wait_bytes(down_in, lsem.at[l_d])
    gvec[...] = jnp.zeros_like(gvec)

    def grad_feed(it):
        r = pl.ds(mul(it * R, R), R)

        def cols(n):
            c0 = pl.ds(mul(n * 512, 512), 512)
            ga = nt(gf[r, :], wdown[c0, :])
            g = (ga * gpre[r, c0].astype(f32)).astype(bf16)
            gpre[r, c0] = g
            gvec[2, :, c0] += jnp.sum(g.astype(f32).reshape(R // 8, 8, 512), axis=0)

        loop(2, cols)

    loop(4, grad_feed)

    rs_sent(rs_s, i_br)

    def gn2_part(blk, ch, dst):
        dst[...] = nt(gpre[pl.ds(mul(blk * R + ch * RC, RC), RC), :], wup[...])

    i_g2 = take(3 * CH)
    rs_run(gn2_part, rs_s, rs_r, rs_own, i_g2)

    def down_z(hh):
        dw_z(hh, 0, D, xr_down, own_a, gpre, 0, zr_down, o_ddown, i_dwx, i_dwz)

    def up_z(hh):
        dw_z(hh, 0, D, xr_up, own_b, gpre, 512, zr_up, fin_up, i_uwx, i_uwz)

    i_uwx, i_uwz = take(2), take(4)
    dw_away(n2, gpre, 0, D, xs_up, xr_up, i_uwx)
    dw_keep(n2, gpre, 0, D, own_b)
    down_z(0)

    i_gb = take(3 * CH)
    for ch in range(CH):
        rs_wait(rs_s, rs_r, i_g2, ch)

        def third(q, ch=ch):
            r = pl.ds(mul(q * 32, 32), 32)
            r1 = pl.ds(mul(ch * RC + q * 32, 32), 32)
            g2 = rs_sum(rs_r, rs_own, ch, r)
            zz, rstd = layer_stats(res[r1, :])
            gout = cot[r1, :].astype(f32) * valid_rows(ch * RC + q * 32, 32)
            gres = gout + layer_back(g2, vec[5:6, :], zz, rstd)
            o_grad[r1, :] = gres
            low = gres.astype(bf16)
            gb[pl.ds(mul(my + ch * RC + q * 32, 32), 32), :] = low
            fold = lambda v: jnp.sum(v.reshape(4, 8, D), axis=0)
            gvec[4] += fold(low.astype(f32))
            gvec[5] += fold(g2 * zz)
            gvec[6] += fold(g2)
            gvec[7] += fold(gout)

        loop(RC // 32, third)
        ag_start(gb, i_gb, ch)

    down_z(1)
    ag_forward(gb, i_gb, 0)

    def ffn_part(blk, ch, dst):
        dst[...] = nn(act[pl.ds(mul(blk * R + ch * RC, RC), RC), :], wdown[...])

    i_ff = take(3 * CH)
    rs_run(ffn_part, rt_s, rt_r, rt_own, i_ff)
    ag_forward(gb, i_gb, 1)

    ag_wait(gb, i_gb, 0)
    ag_wait(gb, i_gb, 2)

    def att_grad(i):
        c0 = pl.ds(mul(i * 256, 256), 256)
        dot_[:, c0] = nt(wout[...], gb[c0, :]).astype(bf16)

    loop(4, att_grad)
    own_out[...] = nn(attt[...], gb[...])
    i_owx, i_owz = take(), take(4)
    for j in range(3 * CH):
        wait_bytes(gf.at[pl.ds(0, RC), :], ssem.at[i_gf + j])
        wait_bytes(n2.at[pl.ds(0, RC), :], ssem.at[i_n2 + j])
    xs_out = gf.at[pl.ds(512, 256), :]

    @pl.when(x != k)
    def _():
        gf[512:768, :] = own_out[...].astype(bf16)
        rcopy(xs_out, xr_out, xpeer, i_owx).start()

    sent(xs_out, i_owx, x != k)

    lane2 = lax.broadcasted_iota(jnp.int32, (1024, 128), 1)

    def pair_backward(i):
        p0 = pl.ds(mul(i * 128, 128), 128)
        for j in range(2):
            r0 = pl.ds(mul(i * 128 + j * 64, 64), 64)
            li = linv[2 * i + j, 0:1, :]
            dd = dot_[r0, :].astype(f32) * li
            delta = jnp.sum(dd * attt[r0, :].astype(f32), axis=0, keepdims=True)
            linv[2 * i + j, :, :] = jnp.broadcast_to(delta, (8, 1024))
            dot_[r0, :] = dd.astype(bf16)
        do_[...] = dot_[p0, :].T
        acck[...] = jnp.zeros_like(acck)
        accv[...] = jnp.zeros_like(accv)

        def queries(qb):
            q0 = pl.ds(mul(qb * 256, 256), 256)
            qblk = qkv[q0, pl.ds(mul(i * 384, 128), 128)]
            doblk = do_[q0, :]
            dt = dot_[p0, q0]

            def keys(kb, carry):
                k0 = pl.ds(mul(kb * 256, 256), 256)
                vblk = qkv[k0, pl.ds(mul(i * 384 + 256, 128), 128)]
                new = []
                for j in range(2):
                    p = ptri[2 * i + j, tri(kb, qb)]
                    dp = nn(half(vblk, j), dt) - linv[2 * i + j, 0:1, q0]
                    ds = (p.astype(f32) * dp).astype(bf16)
                    accv[j, k0, :] += nn(p, doblk)
                    acck[j, k0, :] += nn(ds, qblk)
                    kk = kt[pl.ds(mul(i * 128 + j * 64, 64), 64), k0]
                    new.append(carry[j] + nn(kk, ds))
                return tuple(new)

            zero = jnp.zeros((64, 256), f32)
            dq = lax.fori_loop(0, qb + 1, keys, (zero, zero))
            dq = jnp.concatenate(dq, axis=0) * 0.125
            dmix[q0, pl.ds(mul(i * 384, 128), 128)] = dq.T.astype(bf16)

        loop(4, queries)
        dk = jnp.where(lane2 < 64, acck[0], acck[1]) * 0.125
        dv = jnp.where(lane2 < 64, accv[0], accv[1])
        dmix[:, pl.ds(mul(i * 384 + 128, 128), 128)] = dk.astype(bf16)
        dmix[:, pl.ds(mul(i * 384 + 256, 128), 128)] = dv.astype(bf16)

    up_z(0)
    pair_backward(0)
    i_qwx, i_qwz = (take(2), take(2)), (take(4), take(4))
    dw_away(n1, dmix, 0, 384, gf, xr_qkv, i_qwx[0])
    pair_backward(1)

    rs_sent(rs_s, i_g2)

    def gn1_part(blk, ch, dst):
        dst[...] = nt(dmix[pl.ds(mul(blk * R + ch * RC, RC), RC), :], wqkv[...])

    i_g1 = take(3 * CH)
    up_z(1)
    rs_run(gn1_part, rs_s, rs_r, rs_own, i_g1)
    dw_away(n1, dmix, 384, 384, gf, xr_qkv, i_qwx[1])
    dw_keep(n1, dmix, 0, 768, own_a)

    for i in range(2):
        zi = y + 2 * i
        dz = (zi - z + 4) % 4

        @pl.when(x == k)
        def _(i=i, zi=zi, dz=dz):
            if i == 0:
                wait_bytes(xr_out, rsem.at[i_owx])
            half_rows = slice(i * 128, (i + 1) * 128)
            total = own_out[half_rows, :] + xr_out[half_rows, :].astype(f32)

            @pl.when(zi == z)
            def _():
                fin_out[...] = total

            @pl.when(zi != z)
            def _():
                n2[512 + i * 128 : 640 + i * 128, :] = total.astype(bf16)
                rcopy(n2.at[pl.ds(512 + i * 128, 128), :], zr_out.at[dz - 1], {"seq": zi * 2 + x}, i_owz + dz).start()

        sent(n2.at[pl.ds(512, 128), :], i_owz + dz, jnp.logical_and(x == k, zi != z))

    for ch in range(CH):
        rs_wait(rs_s, rs_r, i_g1, ch)

        def fourth(q, ch=ch):
            r = pl.ds(mul(q * 32, 32), 32)
            r1 = pl.ds(mul(ch * RC + q * 32, 32), 32)
            g1 = rs_sum(rs_r, rs_own, ch, r)
            zz, rstd = layer_stats(tok[r1, :].astype(f32))
            o_grad[r1, :] += layer_back(g1, vec[0:1, :], zz, rstd)
            fold = lambda v: jnp.sum(v.reshape(4, 8, D), axis=0)
            gvec[0] += fold(g1 * zz)
            gvec[1] += fold(g1)

        loop(RC // 32, fourth)

    gmat[...] = jnp.zeros_like(gmat)
    for r, v in ((0, 0), (1, 1), (4, 4), (5, 5), (6, 6), (7, 7), (8, 2)):
        gmat[r : r + 1, :] = jnp.sum(gvec[v], axis=0, keepdims=True)
    for r, p in ((2, 0), (3, 256)):
        for i in range(2):
            v = dmix[:, i * 384 + p : i * 384 + p + 128].astype(f32)
            v = jnp.sum(jnp.sum(v.reshape(128, 8, 128), axis=0), axis=0, keepdims=True)
            gmat[r : r + 1, pl.ds(mul((ctx + 4 * i) * 128, 128), 128)] = v
    for s in range(8):
        sg[s] = gmat[:, s * 128 : (s + 1) * 128]
    i_sgx, i_sgz, i_sgc = take(4), take(4), take(4)
    for j in range(4):
        src = sg.at[j * 2 + (x + 1) % 2]
        rcopy(src, sgx.at[j], xpeer, i_sgx + j).start()
        sent(src, i_sgx + j)

    for h in range(2):
        for hh in range(2):
            dw_z(hh, h * 384, 384, xr_qkv, own_a, n2, 0, zr_qkv, fin_qkv, i_qwx[h], i_qwz[h])
    for j in range(4):
        rcopy(sg.at[j], sgx.at[j], xpeer, i_sgx + j).wait_recv()
    for d in (1, 2, 3):
        zz = (z + d) % 4
        sgs[d - 1] = sg[zz * 2 + x] + sgx[zz]
        rcopy(sgs.at[d - 1], sgz.at[d - 1], zpeer(d), i_sgz + d).start()
        sent(sgs.at[d - 1], i_sgz + d)

    dw_end(0, D, zr_down, o_ddown, i_dwz)
    dw_end(0, D, zr_up, fin_up, i_uwz)
    i_uf, i_qf, i_of = take(4), take(4), take(4)

    def up_piece(fin, c, s):
        return (fin.at[pl.ds(mul(c * 32, 32), 32), pl.ds(s * 128, 128)],
                o_dup.at[:, pl.ds(mul((s * 4 + ctx) * 128, 128), 128)])

    for d in (1, 2, 3):
        for s in range(8):
            a, b = up_piece(fin_up, (ctx + d) % 4, s)
            rcopy(a, b, cpeer(d), i_uf + d).start()
        sent(fin_up.at[pl.ds(0, 32), :], i_uf + d)
    mine32 = pl.ds(mul(ctx * 32, 32), 32)
    for s in range(8):
        o_dup[:, pl.ds(mul((s * 4 + ctx) * 128, 128), 128)] = fin_up[mine32, s * 128 : (s + 1) * 128]

    @pl.when(ctx == t)
    def _():
        for d in (1, 2, 3):
            wait_bytes(zr_out.at[d - 1], rsem.at[i_owz + d])
        fin_out[...] += (zr_out[0].astype(f32) + zr_out[1].astype(f32)) + zr_out[2].astype(f32)
        for d in (1, 2, 3):
            src = fin_out.at[pl.ds(mul(((ctx + d) % 4) * 32, 32), 32), :]
            rcopy(src, o_dout, cpeer(d), i_of + d).start()
        o_dout[...] = fin_out[mine32, :]

    for d in (1, 2, 3):
        sent(fin_out.at[pl.ds(0, 32), :], i_of + d, ctx == t)

    for ch in range(CH):
        rs_wait(rt_s, rt_r, i_ff, ch)

        def last(q, ch=ch):
            r = pl.ds(mul(q * 32, 32), 32)
            r1 = pl.ds(mul(ch * RC + q * 32, 32), 32)
            ffn = rs_sum(rt_r, rt_own, ch, r) + vec[7:8, :]
            v = valid_rows(ch * RC + q * 32, 32)
            o_out[r1, :] = (v * (res[r1, :] + ffn)).astype(bf16)
            stat[16:24, :] += jnp.sum((ffn * ffn * v).reshape(4, 8, D), axis=0)

        loop(RC // 32, last)

    for d in (1, 2, 3):
        wait_bytes(sgz.at[d - 1], rsem.at[i_sgz + d])
    sgf[...] = sg[seq] + sgx[z] + (sgz[0] + sgz[1] + sgz[2])
    for j in range(3):
        v = jnp.sum(stat[j * 8 : (j + 1) * 8, :], axis=0, keepdims=True)
        sgf[9 + j : 10 + j, :] = jnp.broadcast_to(jnp.sum(v, axis=1, keepdims=True), (1, 128))
    for d in (1, 2, 3):
        rcopy(sgf, sgc.at[d], cpeer(d), i_sgc + d).start()
        sent(sgf, i_sgc + d)

    for h in range(2):
        dw_end(h * 384, 384, zr_qkv, fin_qkv, i_qwz[h])
    for d in (1, 2, 3):
        c2 = (ctx + d) % 4
        for a, b in qkv_pieces(ctx):
            rcopy(fin_qkv.at[pl.ds(mul(c2 * 32, 32), 32), b], o_dqkv.at[:, a], cpeer(d), i_qf + d).start()
        sent(fin_qkv.at[pl.ds(0, 32), :], i_qf + d)
    for a, b in qkv_pieces(ctx):
        o_dqkv[:, a] = fin_qkv[mine32, b]

    for d in (1, 2, 3):
        wait_bytes(sgc.at[d], rsem.at[i_sgc + d])
    o_small[...] = sgf[...] + jnp.where(rowid != 8, sgc[1] + sgc[2] + sgc[3], 0.0)

    @pl.when(ctx != t)
    def _():
        wait_bytes(o_dout, rsem.at[i_of + (ctx - t + 4) % 4])

    for d in (1, 2, 3):
        wait_bytes(fin_up.at[pl.ds(0, 32), :], rsem.at[i_uf + d])
        wait_bytes(fin_qkv.at[pl.ds(0, 32), :], rsem.at[i_qf + d])
    rs_sent(rs_s, i_g1)
    rs_sent(rt_s, i_ff)
    for block, i in ((qkv_block, i_qr), (up_block, i_ur), (down_block, i_dr)):
        relay_sent(block, i)
    flush()
    assert next(ids) <= NSEM, next(ids)


def fast(mesh):
    def scratch():
        v = lambda dt, *shape: pltpu.VMEM(shape, dt)
        return [
            v(bf16, D, 768), v(bf16, 256, D), v(bf16, D, D), v(bf16, D, D),
            v(f32, 4, 16, 128), v(f32, 8, 16, 128), v(f32, 16, D),
            v(bf16, S, D), v(bf16, S, D), v(bf16, S, D), v(bf16, S, D), v(bf16, S, D), v(bf16, S, D),
            v(bf16, S, 768), v(bf16, 256, S), v(bf16, 256, S), v(bf16, 256, S),
            v(bf16, 256, S), v(bf16, S, 128), v(bf16, S, 768), v(f32, 4, 8, S),
            v(bf16, 4, 10, 256, 256), v(f32, 2, S, 128), v(f32, 2, S, 128),
            v(bf16, 3, 2, 128, D), v(bf16, 3, 2, 128, D), v(f32, 2, 128, D),
            v(bf16, 3, 2, 128, D), v(bf16, 3, 2, 128, D), v(f32, 2, 128, D),
            v(f32, 128, D), v(f32, R, D),
            v(bf16, 512, D), v(bf16, 512, D), v(bf16, 512, D), v(bf16, 512, D), v(bf16, 512, 768), v(bf16, 256, D),
            v(f32, 512, D), v(f32, 512, D), v(f32, 256, D),
            v(bf16, 3, 128, D), v(bf16, 3, 128, D), v(bf16, 3, 128, 768), v(bf16, 3, 128, D),
            v(f32, 128, D), v(f32, 128, 768), v(f32, 128, D),
            v(f32, 8, 16, 128), v(f32, 4, 16, 128), v(f32, 3, 16, 128), v(f32, 3, 16, 128),
            v(f32, 16, 128), v(f32, 4, 16, 128), v(f32, 8, 8, D), v(f32, 16, D), v(f32, 24, D), v(f32, 8, 768),
            pltpu.SemaphoreType.DMA((8,)),
            pltpu.SemaphoreType.DMA((NSEM,)),
            pltpu.SemaphoreType.DMA((NSEM,)),
        ]

    def on_device(tokens, lengths, cotangent, g1, b1, wq, qb, vb, wo, ob, g2, b2, wu, ub, wd, db):
        ctx = lax.axis_index("ctx")
        vectors = jnp.stack([g1, b1, qb, vb, ob, g2, b2, db]).astype(f32)
        place = (jnp.arange(128) // 32) == ctx
        small = jnp.concatenate([
            jnp.where(place[None], jnp.tile(vectors, (1, 4)), 0.0),
            ub.astype(f32)[None], jnp.zeros((7, 128), f32)])
        vm = pl.BlockSpec(memory_space=pltpu.VMEM)
        sds = jax.ShapeDtypeStruct
        out, grad, dqkv, dout, dup, ddown, sums = pl.pallas_call(
            block_kernel,
            out_shape=(sds((R, D), bf16), sds((R, D), f32), sds((32, 3 * D), f32), sds((32, D), f32),
                       sds((32, 4 * D), f32), sds((128, D), f32), sds((16, 128), f32)),
            in_specs=[pl.BlockSpec(memory_space=pltpu.SMEM)] + [vm] * 7,
            out_specs=tuple([vm] * 7),
            scratch_shapes=scratch(),
            compiler_params=pltpu.CompilerParams(
                collective_id=0, has_side_effects=True, vmem_limit_bytes=LIMIT),
            name="block",
        )(lengths, tokens[0], cotangent[0], small, wq, wo, wu, wd)
        mine = lax.dynamic_slice(sums, (0, ctx * 32), (8, 32))
        stats = jnp.sqrt(sums[9:12, 0] / (lengths[0].astype(f32) * D))[None]
        return (out[None], grad[None], mine[0], mine[1], dqkv, mine[2], mine[3], dout, mine[4],
                mine[5], mine[6], dup, sums[8], ddown, mine[7], stats)

    return on_device


HEADS = 16


epsilon = 1e-05


def normalize(inputs, gain, shift):
    average = jnp.mean(inputs, axis=-1, keepdims=True)
    centred = inputs - average
    variance = jnp.mean(centred * centred, axis=-1, keepdims=True)
    return centred * lax.rsqrt(variance + epsilon) * gain + shift


def gelu_tanh(inputs):
    return jax.nn.gelu(inputs, approximate=True)


def inner_rows(left, right):
    return lax.dot_general(
        left, right, (((0,), (0,)), ((), ())), preferred_element_type=jnp.float32
    )


def outer_cols(left, right):
    return lax.dot_general(
        left, right, (((1,), (1,)), ((), ())), preferred_element_type=jnp.float32
    )


def alibi_scores(query_block, key_block, query_pos, key_pos, slope_block):
    raw = jnp.einsum("qhd,khd->hqk", query_block, key_block, preferred_element_type=jnp.float32)
    offset = (key_pos[None, :] - query_pos[:, None]).astype(jnp.float32)
    scores = raw * query_block.shape[-1] ** (-0.5) + slope_block[:, None, None] * offset[None]
    allowed = key_pos[None, :] <= query_pos[:, None]
    return (scores, allowed)


def score_grads(
    query_block,
    key_block,
    value_block,
    grad_block,
    query_pos,
    key_pos,
    slope_block,
    log_block,
    delta_block,
):
    scores, allowed = alibi_scores(query_block, key_block, query_pos, key_pos, slope_block)
    probs = jnp.where(allowed[None], jnp.exp(scores - log_block[..., None]), 0.0)
    grad_probs = jnp.einsum(
        "qhd,khd->hqk", grad_block, value_block, preferred_element_type=jnp.float32
    )
    delta_block = jnp.sum(probs * grad_probs, axis=-1)
    grad_scores = (probs * (grad_probs - delta_block[..., None])).astype(jnp.bfloat16)
    return (probs, grad_scores, delta_block)


def on_device(
    tokens,
    lengths,
    cotangent,
    ln1_gain,
    ln1_bias,
    qkv_weight,
    query_bias,
    value_bias,
    out_weight,
    out_bias,
    ln2_gain,
    ln2_bias,
    up_weight,
    up_bias,
    down_weight,
    down_bias,
):
    shards = (
        ln1_gain,
        ln1_bias,
        qkv_weight,
        query_bias,
        value_bias,
        out_weight,
        out_bias,
        ln2_gain,
        ln2_bias,
        up_weight,
        up_bias,
        down_weight,
        down_bias,
    )
    row_count = tokens.shape[1]
    model_width = tokens.shape[2]
    head_count = HEADS
    head_width = model_width // head_count
    per_block = 2
    block_count = head_count // per_block
    slot_rows = row_count * lax.axis_size("ctx")
    positions = lax.axis_index("ctx") * row_count + jnp.arange(row_count, dtype=jnp.int32)
    length = lengths[0]
    valid_rows = (positions < length).astype(jnp.float32)[:, None]
    slopes = jnp.exp2(-8.0 * (jnp.arange(head_count, dtype=jnp.float32) + 1.0) / head_count)
    key_positions = jnp.arange(slot_rows, dtype=jnp.int32)
    scale = head_width ** (-0.5)
    full_weights = (
        lax.all_gather(shards[0], ("seq", "ctx"), axis=0, tiled=True),
        lax.all_gather(shards[1], ("seq", "ctx"), axis=0, tiled=True),
        lax.all_gather(shards[2], ("seq", "ctx"), axis=0, tiled=True),
        lax.all_gather(shards[3], ("seq", "ctx"), axis=0, tiled=True),
        lax.all_gather(shards[4], ("seq", "ctx"), axis=0, tiled=True),
        lax.all_gather(shards[5], ("seq", "ctx"), axis=0, tiled=True),
        lax.all_gather(shards[6], ("seq", "ctx"), axis=0, tiled=True),
        lax.all_gather(shards[7], ("seq", "ctx"), axis=0, tiled=True),
        lax.all_gather(shards[8], ("seq", "ctx"), axis=0, tiled=True),
        lax.all_gather(shards[9], ("seq", "ctx"), axis=0, tiled=True),
        lax.all_gather(shards[10], ("seq", "ctx"), axis=0, tiled=True),
        lax.all_gather(shards[11], ("seq", "ctx"), axis=0, tiled=True),
        lax.all_gather(shards[12], ("seq", "ctx"), axis=0, tiled=True),
    )
    (
        gain_one,
        shift_one,
        w_qkv,
        bias_query,
        bias_value,
        w_out,
        bias_out,
        gain_two,
        shift_two,
        w_up,
        bias_up,
        w_down,
        bias_down,
    ) = full_weights

    def pick(array, index):
        return lax.dynamic_slice_in_dim(array, index * per_block, per_block, 1)

    def pick_slopes(index):
        return lax.dynamic_slice_in_dim(slopes, index * per_block, per_block, 0)

    def to_blocks(array):
        return array.transpose(1, 0, 2, 3).reshape(array.shape[1], model_width)

    source = tokens[0].astype(jnp.float32)
    normed_one, back_one = jax.vjp(normalize, source, gain_one, shift_one)
    normed_low = normed_one.astype(jnp.bfloat16)
    mixed = jnp.dot(normed_low, w_qkv, preferred_element_type=jnp.float32)
    query = (mixed[:, :model_width] + bias_query).astype(jnp.bfloat16)
    keys = mixed[:, model_width : 2 * model_width].astype(jnp.bfloat16)
    values = (mixed[:, 2 * model_width :] + bias_value).astype(jnp.bfloat16)
    all_keys, all_values = (
        lax.all_gather(keys, "ctx", axis=0, tiled=True),
        lax.all_gather(values, "ctx", axis=0, tiled=True),
    )
    query_heads = query.reshape(row_count, head_count, head_width)
    key_heads = all_keys.reshape(slot_rows, head_count, head_width)
    value_heads = all_values.reshape(slot_rows, head_count, head_width)

    def forward_block(index):
        scores, allowed = alibi_scores(
            pick(query_heads, index),
            pick(key_heads, index),
            positions,
            key_positions,
            pick_slopes(index),
        )
        masked = jnp.where(allowed[None], scores, -1e30)
        highest = jnp.max(masked, axis=-1)
        total = jnp.sum(jnp.exp(masked - highest[..., None]), axis=-1)
        log_total = highest + jnp.log(total)
        probs = jnp.where(allowed[None], jnp.exp(scores - log_total[..., None]), 0.0)
        block_out = jnp.einsum(
            "hqk,khd->qhd",
            probs.astype(jnp.bfloat16),
            pick(value_heads, index),
            preferred_element_type=jnp.float32,
        )
        return (block_out, log_total)

    head_out, log_totals = lax.map(forward_block, jnp.arange(block_count))
    attended = to_blocks(head_out).astype(jnp.bfloat16)
    branch = jnp.dot(attended, w_out, preferred_element_type=jnp.float32) + bias_out
    resid = source + branch
    normed_two, back_two = jax.vjp(normalize, resid, gain_two, shift_two)
    normed_two_low = normed_two.astype(jnp.bfloat16)
    pre_act = jnp.dot(normed_two_low, w_up, preferred_element_type=jnp.float32) + bias_up
    activated, back_act = jax.vjp(gelu_tanh, pre_act)
    activated_low = activated.astype(jnp.bfloat16)
    ffn = jnp.dot(activated_low, w_down, preferred_element_type=jnp.float32) + bias_down
    output = (valid_rows * (resid + ffn)).astype(jnp.bfloat16)[None]
    squares = jnp.stack(
        [
            jnp.sum(valid_rows * branch * branch),
            jnp.sum(valid_rows * resid * resid),
            jnp.sum(valid_rows * ffn * ffn),
        ]
    )
    totals = lax.psum(squares, "ctx")
    stats = jnp.sqrt(totals / (length.astype(jnp.float32) * model_width))[None]
    w_qkv, w_out, w_up, w_down = (
        lax.all_gather(qkv_weight, ("seq", "ctx"), axis=0, tiled=True),
        lax.all_gather(out_weight, ("seq", "ctx"), axis=0, tiled=True),
        lax.all_gather(up_weight, ("seq", "ctx"), axis=0, tiled=True),
        lax.all_gather(down_weight, ("seq", "ctx"), axis=0, tiled=True),
    )
    grad_out = cotangent[0].astype(jnp.float32) * valid_rows
    grad_ffn = grad_out.astype(jnp.bfloat16)
    grad_down_w = inner_rows(activated_low, grad_ffn)
    grad_down_b = jnp.sum(grad_ffn.astype(jnp.float32), axis=0)
    grad_activated = outer_cols(grad_ffn, w_down)
    (grad_pre,) = back_act(grad_activated)
    grad_pre_low = grad_pre.astype(jnp.bfloat16)
    grad_up_w = inner_rows(normed_two_low, grad_pre_low)
    grad_up_b = jnp.sum(grad_pre_low.astype(jnp.float32), axis=0)
    grad_normed_two = outer_cols(grad_pre_low, w_up)
    grad_resid_norm, grad_gain_two, grad_shift_two = back_two(grad_normed_two)
    grad_resid = grad_out + grad_resid_norm
    grad_branch = grad_resid.astype(jnp.bfloat16)
    grad_out_w = inner_rows(attended, grad_branch)
    grad_out_b = jnp.sum(grad_branch.astype(jnp.float32), axis=0)
    grad_attended = outer_cols(grad_branch, w_out).astype(jnp.bfloat16)
    grad_heads = grad_attended.reshape(row_count, head_count, head_width)

    def backward_block(index):
        query_block = pick(query_heads, index)
        key_block = pick(key_heads, index)
        grad_block = pick(grad_heads, index)
        probs, grad_scores, delta_block = score_grads(
            query_block,
            key_block,
            pick(value_heads, index),
            grad_block,
            positions,
            key_positions,
            pick_slopes(index),
            log_totals[index],
            None,
        )
        grad_query_block = (
            jnp.einsum("hqk,khd->qhd", grad_scores, key_block, preferred_element_type=jnp.float32)
            * scale
        )
        grad_key_block = (
            jnp.einsum("hqk,qhd->khd", grad_scores, query_block, preferred_element_type=jnp.float32)
            * scale
        )
        grad_value_block = jnp.einsum(
            "hqk,qhd->khd",
            probs.astype(jnp.bfloat16),
            grad_block,
            preferred_element_type=jnp.float32,
        )
        return (grad_query_block, grad_key_block, grad_value_block)

    query_parts, key_parts, value_parts = lax.map(backward_block, jnp.arange(block_count))
    grad_query_all = to_blocks(query_parts)
    own_keys, own_values = (
        lax.psum_scatter(
            to_blocks(key_parts).astype(jnp.bfloat16), "ctx", scatter_dimension=0, tiled=True
        ).astype(jnp.float32),
        lax.psum_scatter(
            to_blocks(value_parts).astype(jnp.bfloat16), "ctx", scatter_dimension=0, tiled=True
        ).astype(jnp.float32),
    )
    grad_query_low = grad_query_all.astype(jnp.bfloat16)
    grad_key_low = own_keys.astype(jnp.bfloat16)
    grad_value_low = own_values.astype(jnp.bfloat16)
    grad_mixed = jnp.concatenate([grad_query_low, grad_key_low, grad_value_low], axis=1)
    grad_qkv_w = inner_rows(normed_low, grad_mixed)
    grad_query_bias = jnp.sum(grad_query_low.astype(jnp.float32), axis=0)
    grad_value_bias = jnp.sum(grad_value_low.astype(jnp.float32), axis=0)
    grad_normed_one = outer_cols(grad_mixed, w_qkv)
    grad_source_norm, grad_gain_one, grad_shift_one = back_one(grad_normed_one)
    grad_tokens = (grad_resid + grad_source_norm)[None]
    summed = (
        lax.psum_scatter(
            grad_gain_one.astype(jnp.float32), ("seq", "ctx"), scatter_dimension=0, tiled=True
        ),
        lax.psum_scatter(
            grad_shift_one.astype(jnp.float32), ("seq", "ctx"), scatter_dimension=0, tiled=True
        ),
        lax.psum_scatter(grad_qkv_w, ("seq", "ctx"), scatter_dimension=0, tiled=True),
        lax.psum_scatter(grad_query_bias, ("seq", "ctx"), scatter_dimension=0, tiled=True),
        lax.psum_scatter(grad_value_bias, ("seq", "ctx"), scatter_dimension=0, tiled=True),
        lax.psum_scatter(grad_out_w, ("seq", "ctx"), scatter_dimension=0, tiled=True),
        lax.psum_scatter(grad_out_b, ("seq", "ctx"), scatter_dimension=0, tiled=True),
        lax.psum_scatter(
            grad_gain_two.astype(jnp.float32), ("seq", "ctx"), scatter_dimension=0, tiled=True
        ),
        lax.psum_scatter(
            grad_shift_two.astype(jnp.float32), ("seq", "ctx"), scatter_dimension=0, tiled=True
        ),
        lax.psum_scatter(grad_up_w, ("seq", "ctx"), scatter_dimension=0, tiled=True),
        lax.psum_scatter(grad_up_b, ("seq", "ctx"), scatter_dimension=0, tiled=True),
        lax.psum_scatter(grad_down_w, ("seq", "ctx"), scatter_dimension=0, tiled=True),
        lax.psum_scatter(grad_down_b, ("seq", "ctx"), scatter_dimension=0, tiled=True),
    )
    return (output, grad_tokens) + tuple(summed) + (stats,)


def solution(mesh):
    small_slice = mesh.shape["seq"] == 8 and mesh.shape["ctx"] == 4
    placed = (
        P("seq", "ctx", None),
        P("seq"),
        P("seq", "ctx", None),
        P(("seq", "ctx")),
        P(("seq", "ctx")),
        P(("seq", "ctx"), None),
        P(("seq", "ctx")),
        P(("seq", "ctx")),
        P(("seq", "ctx"), None),
        P(("seq", "ctx")),
        P(("seq", "ctx")),
        P(("seq", "ctx")),
        P(("seq", "ctx"), None),
        P(("seq", "ctx")),
        P(("seq", "ctx"), None),
        P(("seq", "ctx")),
    )
    return jax.shard_map(
        fast(mesh) if small_slice else on_device,
        mesh=mesh,
        in_specs=placed,
        out_specs=(
            P("seq", "ctx", None),
            P("seq", "ctx", None),
            P(("seq", "ctx")),
            P(("seq", "ctx")),
            P(("seq", "ctx"), None),
            P(("seq", "ctx")),
            P(("seq", "ctx")),
            P(("seq", "ctx"), None),
            P(("seq", "ctx")),
            P(("seq", "ctx")),
            P(("seq", "ctx")),
            P(("seq", "ctx"), None),
            P(("seq", "ctx")),
            P(("seq", "ctx"), None),
            P(("seq", "ctx")),
            P("seq", None),
        ),
        check_vma=False,
    )
```

```python
import itertools

import jax
import jax.numpy as jnp
from jax import lax
from jax.experimental import pallas as pl
from jax.experimental.pallas import tpu as pltpu
from jax.sharding import PartitionSpec as P

MESH = pl.DeviceIdType.MESH
bf16, f32 = jnp.bfloat16, jnp.float32
LOG2E = 1.4426950408889634
D = 1024
R = 256
S = 1024
LIMIT = 66_000_000
NSEM = 260
ORDER = (2, 3, 1)


def nn(a, b):
    return lax.dot_general(a, b, (((1,), (0,)), ((), ())), preferred_element_type=f32)


def nt(a, b):
    return lax.dot_general(a, b, (((1,), (1,)), ((), ())), preferred_element_type=f32)


def tn(a, b):
    return lax.dot_general(a, b, (((0,), (0,)), ((), ())), preferred_element_type=f32)


def mul(v, m):
    return pl.multiple_of(v, m)


def loop(n, body, start=0):
    def step(i, carry):
        body(i)
        return carry

    lax.fori_loop(start, n, step, 0)


def layer_stats(v):
    mean = jnp.sum(v, axis=-1, keepdims=True) * (1.0 / D)
    cen = v - mean
    var = jnp.sum(cen * cen, axis=-1, keepdims=True) * (1.0 / D)
    rstd = lax.rsqrt(var + 1e-5)
    return cen * rstd, rstd


def layer_back(g2, gain, z, rstd):
    g = g2 * gain
    m1 = jnp.sum(g, axis=-1, keepdims=True) * (1.0 / D)
    m2 = jnp.sum(g * z, axis=-1, keepdims=True) * (1.0 / D)
    return rstd * (g - m1 - z * m2)


def block_kernel(
    length_ref, tok, cot, small, qkv_in, out_in, up_in, down_in,
    o_out, o_grad, o_dqkv, o_dout, o_dup, o_ddown, o_small,
    wqkv, wout, wup, wdown, smc, smb, vec,
    n1, n2, gf, gb, act, gpre, qkv, vt, kt, attt, dot_, do_, dmix, linv,
    ptri, acck, accv,
    rs_s, rs_r, rs_own, rt_s, rt_r, rt_own, tmp, res,
    xs_down, xs_up, xr_down, xr_up, xr_qkv, xr_out, own_a, own_b, own_out,
    zr_down, zr_up, zr_qkv, zr_out, fin_up, fin_qkv, fin_out,
    st_out, st_grad, fin_down, sg, sgx, sgs, sgz, sgf, sgc, gvec, gmat, stat, qbias,
    lsem, ssem, rsem,
):
    seq, ctx = lax.axis_index("seq"), lax.axis_index("ctx")
    z, x = seq // 2, seq % 2
    y, k = ctx // 2, ctx % 2
    ids = itertools.count()
    lids = itertools.count()

    mate = {"ctx": y * 2 + (k + 1) % 2}
    ypeer = {"ctx": ((y + 1) % 2) * 2 + k}
    xpeer = {"seq": z * 2 + (x + 1) % 2}

    def cpeer(d):
        return {"ctx": (ctx + d) % 4}

    def zpeer(d):
        return {"seq": ((z + d) % 4) * 2 + x}

    def take(n=1):
        first = next(ids)
        for _ in range(n - 1):
            next(ids)
        return first

    def rcopy(src, dst, dev, i):
        return pltpu.make_async_remote_copy(
            src_ref=src, dst_ref=dst, send_sem=ssem.at[i], recv_sem=rsem.at[i],
            device_id=dev, device_id_type=MESH)

    def wait_bytes(ref, sem):
        pltpu.make_async_copy(ref, ref, sem).wait()

    sends = []

    def sent(ref, i, cond=None):
        sends.append((ref, i, cond))

    def flush():
        for ref, i, cond in sends:
            if cond is None:
                wait_bytes(ref, ssem.at[i])
            else:
                @pl.when(cond)
                def _(ref=ref, i=i):
                    wait_bytes(ref, ssem.at[i])
        sends.clear()

    rows = lambda c: pl.ds(mul(c * R, R), R)
    srow = lambda s: pl.ds(s * 128 if isinstance(s, int) else mul(s * 128, 128), 128)

    barrier = pltpu.get_barrier_semaphore()
    for d in (1, 2, 3):
        pl.semaphore_signal(barrier, inc=1, device_id=cpeer(d), device_id_type=MESH)
        pl.semaphore_signal(barrier, inc=1, device_id=zpeer(d), device_id_type=MESH)
    pl.semaphore_signal(barrier, inc=1, device_id=xpeer, device_id_type=MESH)
    pl.semaphore_wait(barrier, 7)

    i_smc = take(4)
    for d in (1, 2, 3):
        rcopy(small, smc.at[d], cpeer(d), i_smc + d).start()
        sent(small, i_smc + d)
    own32 = pl.ds(mul(seq * 128 + ctx * 32, 32), 32)

    def qkv_pieces(c):
        for j in range(6):
            yield (pl.ds(mul((j % 3) * D + (c + 4 * (j // 3)) * 128, 128), 128),
                   pl.ds(j * 128, 128))

    i_qa = take(4)
    for d in (1, 2, 3):
        for a, b in qkv_pieces((ctx + d) % 4):
            rcopy(qkv_in.at[:, a], wqkv.at[own32, b], cpeer(d), i_qa + d).start()
        sent(wqkv.at[pl.ds(0, 32), :], i_qa + d)
    l_q = next(lids)
    for a, b in qkv_pieces(ctx):
        pltpu.make_async_copy(qkv_in.at[:, a], wqkv.at[own32, b], lsem.at[l_q]).start()

    t = seq % 4
    out32 = pl.ds(mul((seq // 4) * 128 + ctx * 32, 32), 32)
    i_oa = take()
    l_o = next(lids)

    @pl.when(ctx != t)
    def _():
        rcopy(out_in, wout.at[out32, :], {"ctx": t}, i_oa).start()

    sent(out_in, i_oa, ctx != t)

    @pl.when(ctx == t)
    def _():
        pltpu.make_async_copy(out_in, wout.at[out32, :], lsem.at[l_o]).start()

    i_ua = take(4)
    for d in (1, 2, 3):
        c2 = (ctx + d) % 4
        for s in range(8):
            rcopy(up_in.at[:, pl.ds(mul((s * 4 + c2) * 128, 128), 128)],
                  wup.at[own32, pl.ds(s * 128, 128)], cpeer(d), i_ua + d).start()
        sent(wup.at[pl.ds(0, 32), :], i_ua + d)
    l_u = next(lids)
    for s in range(8):
        pltpu.make_async_copy(up_in.at[:, pl.ds(mul((s * 4 + ctx) * 128, 128), 128)],
                              wup.at[own32, pl.ds(s * 128, 128)], lsem.at[l_u]).start()

    for d in (1, 2, 3):
        rcopy(small, smc.at[d], cpeer(d), i_smc + d).wait_recv()
    rowid = lax.broadcasted_iota(jnp.int32, (16, 128), 0)
    smb[seq] = small[...] + jnp.where(rowid < 8, smc[1] + smc[2] + smc[3], 0.0)

    def gather_z(block, zi, src=None):
        own = block(seq) if src is None else src
        for d in ORDER:
            rcopy(own, block(seq), zpeer(d), zi + d).start()
            sent(own, zi + d)

    def gather_x(block, xi, src=None):
        own = block(seq) if src is None else src
        rcopy(own, block(seq), xpeer, xi).start()
        sent(own, xi)

    def gather_forward(block, zi, xi, d):
        b = block(((z - d + 4) % 4) * 2 + x)
        rcopy(b, b, xpeer, zi + d).wait_recv()
        rcopy(b, b, xpeer, xi + d).start()
        sent(block(0), xi + d)

    def gather_finish(block, xi):
        for d in range(4):
            b = block(seq)
            rcopy(b, b, xpeer, xi + d).wait_recv()

    def relay_start(block, i, src=None):
        own = block(seq) if src is None else src
        for cond, step, first in ((z < 3, 1, i), (z > 0, -1, i + 4)):
            @pl.when(cond)
            def _(step=step, first=first):
                rcopy(own, block(seq), {"seq": (z + step) * 2 + x}, first + 1).start()

            sent(own, first + 1, cond)

    def relay_x(block, i, src=None):
        own = block(seq) if src is None else src
        rcopy(own, block(seq), xpeer, i + 8 + z).start()
        sent(own, i + 8 + z)

    def relay_step(block, i, j):
        for has, on, step, first in ((z >= j, z < 3, 1, i), (z + j <= 3, z > 0, -1, i + 4)):
            zz = z - j * step

            @pl.when(has)
            def _(on=on, step=step, first=first, zz=zz):
                b = block(zz * 2 + x)
                rcopy(b, b, xpeer, first + j).wait_recv()
                if j < 3:
                    @pl.when(on)
                    def _():
                        rcopy(b, b, {"seq": (z + step) * 2 + x}, first + j + 1).start()
                rcopy(b, b, xpeer, i + 8 + zz).start()

            if j < 3:
                sent(block(0), first + j + 1, jnp.logical_and(has, on))

    def relay_finish(block, i):
        for zz in range(4):
            rcopy(block(0), block(0), xpeer, i + 8 + zz).wait_recv()

    def relay_sent(block, i):
        for j in (1, 2, 3):
            for has, zz in ((z >= j, z - j), (z + j <= 3, z + j)):
                @pl.when(has)
                def _(zz=zz):
                    wait_bytes(block(0), ssem.at[i + 8 + zz])

    small_block = lambda s: smb.at[s]
    i_sz, i_sx = take(4), take(4)
    gather_z(small_block, i_sz)
    gather_x(small_block, i_sx)

    for d in (1, 2, 3):
        wait_bytes(wqkv.at[pl.ds(0, 32), :], rsem.at[i_qa + d])
    wait_bytes(wqkv.at[pl.ds(0, 32), :], lsem.at[l_q])
    qkv_block = lambda s: wqkv.at[srow(s), :]
    i_qr = take(12)
    relay_start(qkv_block, i_qr)
    for d in ORDER:
        gather_forward(small_block, i_sz, i_sx, d)
    relay_x(qkv_block, i_qr)
    l_d = next(lids)
    down_block = lambda s: wdown.at[srow(s), :]
    i_dr = take(12)
    relay_x(down_block, i_dr, src=down_in)
    pltpu.make_async_copy(down_in, down_block(seq), lsem.at[l_d]).start()

    gather_finish(small_block, i_sx)
    for s in range(8):
        vec[:, s * 128 : (s + 1) * 128] = smb[s]

    length = length_ref[0]
    my = mul(ctx * R, R)

    def valid_rows(r0, n):
        pos = lax.broadcasted_iota(jnp.int32, (n, 1), 0) + (ctx * R + r0)
        return jnp.where(pos < length, 1.0, 0.0).astype(f32)

    CH = 2
    RC = R // CH

    def chunk(buf, c, ch):
        return buf.at[pl.ds(mul(c * R + ch * RC, RC), RC), :]

    def ag_start(buf, i, ch):
        own = chunk(buf, ctx, ch)
        rcopy(own, own, ypeer, i + CH + ch).start()
        rcopy(own, own, mate, i + ch).start()
        if buf is not gf and buf is not n2:
            sent(own, i + CH + ch)
            sent(own, i + ch)

    def ag_forward(buf, i, ch):
        b = chunk(buf, ((y + 1) % 2) * 2 + k, ch)
        rcopy(b, b, mate, i + CH + ch).wait_recv()
        rcopy(b, b, mate, i + 2 * CH + ch).start()
        if buf is not gf and buf is not n2:
            sent(buf.at[pl.ds(0, RC), :], i + 2 * CH + ch)

    def ag_wait(buf, i, which):
        for ch in range(CH):
            b = chunk(buf, ctx, ch)
            rcopy(b, b, mate, i + which * CH + ch).wait_recv()

    i_n1 = take(3 * CH)
    for ch in range(CH):
        def first(q, ch=ch):
            r0 = mul(ch * RC + q * 32, 32)
            zz, _ = layer_stats(tok[pl.ds(r0, 32), :].astype(f32))
            n1[pl.ds(mul(my + r0, 32), 32), :] = (zz * vec[0:1, :] + vec[1:2, :]).astype(bf16)

        loop(RC // 32, first)
        ag_start(n1, i_n1, ch)


    def mask_rows(q):
        r0 = mul(q * 32, 32)
        g = cot[pl.ds(r0, 32), :].astype(f32) * valid_rows(r0, 32)
        gf[pl.ds(mul(my + r0, 32), 32), :] = g.astype(bf16)

    loop(R // 32, mask_rows)
    i_gf = take(3 * CH)
    for ch in range(CH):
        ag_start(gf, i_gf, ch)
    for j in range(6):
        if j % 3 == 1:
            qbias[:, j * 128 : (j + 1) * 128] = jnp.zeros((8, 128), f32)
        else:
            r = 2 + j % 3 // 2
            b = vec[r : r + 1, pl.ds(mul((ctx + 4 * (j // 3)) * 128, 128), 128)]
            qbias[:, j * 128 : (j + 1) * 128] = jnp.broadcast_to(b, (8, 128))
    relay_step(qkv_block, i_qr, 1)
    relay_step(qkv_block, i_qr, 2)
    i_oz, i_ox = take(4), take(4)
    out_block = lambda zz: wout.at[pl.ds(mul((zz // 2) * 128, 128), 128), :]

    @pl.when(ctx == t)
    def _():
        wait_bytes(wout.at[pl.ds(0, 96), :], rsem.at[i_oa])
        wait_bytes(wout.at[pl.ds(0, 32), :], lsem.at[l_o])
        for d in (1, 2, 3):
            rcopy(out_block(z), out_block(z), zpeer(d), i_oz + d).start()
        rcopy(out_block(z), out_block(z), xpeer, i_ox).start()

    for d in (1, 2, 3):
        sent(out_block(z), i_oz + d, ctx == t)
    sent(out_block(z), i_ox, ctx == t)

    ag_forward(n1, i_n1, 0)
    relay_step(qkv_block, i_qr, 3)
    for d in (1, 2, 3):
        wait_bytes(wup.at[pl.ds(0, 32), :], rsem.at[i_ua + d])
    wait_bytes(wup.at[pl.ds(0, 32), :], lsem.at[l_u])
    up_block = lambda s: wup.at[srow(s), :]
    i_ur = take(12)
    relay_start(up_block, i_ur)
    ag_forward(n1, i_n1, 1)

    ag_wait(n1, i_n1, 0)
    relay_finish(qkv_block, i_qr)
    mine = x == k
    for d in (1, 2, 3):
        zz = (z - d + 4) % 4

        @pl.when(jnp.logical_and(mine, zz % 2 == y))
        def _(d=d, zz=zz):
            rcopy(out_block(zz), out_block(zz), xpeer, i_oz + d).wait_recv()
            rcopy(out_block(zz), out_block(zz), xpeer, i_ox + d).start()

        sent(out_block(zz), i_ox + d, jnp.logical_and(mine, zz % 2 == y))
    relay_x(up_block, i_ur)

    def project(it):
        blk = ((y + it // 2) % 2) * 2 + (k + it % 2) % 2

        @pl.when(it == 3)
        def _():
            ag_wait(n1, i_n1, 2)

        qkv[rows(blk), :] = (nn(n1[rows(blk), :], wqkv[...]) + qbias[0:1, :]).astype(bf16)

    loop(4, project)
    relay_step(up_block, i_ur, 1)
    relay_start(down_block, i_dr, src=down_in)

    def turn(i):
        c0 = pl.ds(mul(i * 128, 128), 128)
        vt[c0, :] = qkv[:, pl.ds(mul(i * 384 + 256, 128), 128)].T
        kt[c0, :] = qkv[:, pl.ds(mul(i * 384 + 128, 128), 128)].T

    loop(2, turn)

    lane = lax.broadcasted_iota(jnp.int32, (256, 128), 1)
    krow = lax.broadcasted_iota(jnp.int32, (256, 256), 0)
    qcol = lax.broadcasted_iota(jnp.int32, (256, 256), 1)

    def tri(kb, qb):
        return (qb * (qb + 1)) // 2 + kb

    def half(v, j):
        return jnp.where((lane // 64) == j, v, jnp.zeros_like(v))

    def pair_forward(i):
        for j in range(2):
            slope = jnp.exp2(jnp.full((1024, 128), -0.5, f32)
                             * (2 * ctx + 8 * i + j + 1).astype(f32)) * LOG2E
            b = slope * lax.broadcasted_iota(jnp.int32, (1024, 128), 0).astype(f32)
            for kb in range(4):
                own_b[j * 256 : (j + 1) * 256, kb * 128 : (kb + 1) * 128] = b[kb * 256 : (kb + 1) * 256]

        def queries(qb):
            q0 = pl.ds(mul(qb * 256, 256), 256)
            qblk = qkv[q0, pl.ds(mul(i * 384, 128), 128)]

            def scores(kb, best):
                k0 = pl.ds(mul(kb * 256, 256), 256)
                kblk = qkv[k0, pl.ds(mul(i * 384 + 128, 128), 128)]
                new = []
                for j in range(2):
                    b = own_b[j * 256 : (j + 1) * 256, pl.ds(mul(kb * 128, 128), 128)]
                    sc = nt(half(kblk, j), qblk) * (0.125 * LOG2E) + jnp.concatenate([b, b], axis=1)
                    sc = jnp.where(krow + kb * 256 <= qcol + qb * 256, sc, -1e30)
                    own_a[j * 256 : (j + 1) * 256, k0] = sc
                    new.append(jnp.maximum(best[j], jnp.max(sc.reshape(32, 8, 256), axis=0)))
                return tuple(new)

            low = jnp.full((8, 256), -3e38, f32)
            best = lax.fori_loop(0, qb + 1, scores, (low, low))
            top = [jnp.max(b, axis=0, keepdims=True) for b in best]

            def weigh(kb, carry):
                k0 = pl.ds(mul(kb * 256, 256), 256)
                new = []
                for j in range(2):
                    total, acc = carry[2 * j], carry[2 * j + 1]
                    p = jnp.exp2(own_a[j * 256 : (j + 1) * 256, k0] - top[j])
                    total = total + jnp.sum(p.reshape(32, 8, 256), axis=0)
                    p = p.astype(bf16)
                    ptri[2 * i + j, tri(kb, qb)] = p
                    v = vt[pl.ds(mul(i * 128 + j * 64, 64), 64), k0]
                    new += [total, acc + nn(v, p)]
                return tuple(new)

            zero = (jnp.zeros((8, 256), f32), jnp.zeros((64, 256), f32))
            out = lax.fori_loop(0, qb + 1, weigh, zero + zero)
            for j in range(2):
                inv = 1.0 / jnp.sum(out[2 * j], axis=0, keepdims=True)
                linv[2 * i + j, :, q0] = jnp.broadcast_to(inv, (8, 256))
                attt[pl.ds(mul(i * 128 + j * 64, 64), 64), q0] = (out[2 * j + 1] * inv).astype(bf16)

        loop(4, queries)

    pair_forward(0)
    for ch in range(CH):
        ag_forward(gf, i_gf, ch)
    pair_forward(1)

    relay_step(up_block, i_ur, 2)
    def rs_run(partial, sb, rb, own, i):
        def step(tt):
            g, ch, sub = tt // 4, tt % 2, (tt // 2) % 2
            blk = ((y + 1 - g) % 2) * 2 + (k + 1 - sub) % 2
            partial(blk, ch, tmp)

            @pl.when(jnp.logical_and(g == 0, sub == 0))
            def _():
                sb[0, ch] = tmp[...].astype(bf16)
                rcopy(sb.at[0, ch], rb.at[0, ch], mate, i + ch).start()

            @pl.when(jnp.logical_and(g == 0, sub == 1))
            def _():
                rcopy(sb.at[0, ch], rb.at[0, ch], mate, i + ch).wait_recv()
                sb[1, ch] = (tmp[...] + rb[0, ch].astype(f32)).astype(bf16)
                rcopy(sb.at[1, ch], rb.at[1, ch], ypeer, i + CH + ch).start()

            @pl.when(jnp.logical_and(g == 1, sub == 0))
            def _():
                sb[2, ch] = tmp[...].astype(bf16)
                rcopy(sb.at[2, ch], rb.at[2, ch], mate, i + 2 * CH + ch).start()

            @pl.when(jnp.logical_and(g == 1, sub == 1))
            def _():
                own[ch] = tmp[...]

        loop(4 * CH, step)

    def rs_wait(sb, rb, i, ch):
        rcopy(sb.at[2, ch], rb.at[2, ch], mate, i + 2 * CH + ch).wait_recv()
        rcopy(sb.at[1, ch], rb.at[1, ch], mate, i + CH + ch).wait_recv()

    def rs_sum(rb, own, ch, r):
        return own[ch, r, :] + rb[2, ch, r, :].astype(f32) + rb[1, ch, r, :].astype(f32)

    def rs_sent(sb, i):
        for j in range(3):
            for ch in range(CH):
                wait_bytes(sb.at[j, ch], ssem.at[i + j * CH + ch])

    for d in range(4):
        zz = (z - d + 4) % 4

        @pl.when(jnp.logical_and(x != k, zz % 2 == y))
        def _(d=d):
            rcopy(out_block(z), out_block(z), xpeer, i_ox + d).wait_recv()

    def branch_part(blk, ch, dst):
        a = attt[:, pl.ds(mul(blk * R + ch * RC, RC), RC)]
        dst[...] = tn(a, wout[...])

    i_br = take(3 * CH)
    rs_run(branch_part, rs_s, rs_r, rs_own, i_br)
    relay_step(up_block, i_ur, 3)
    relay_step(down_block, i_dr, 1)

    i_n2 = take(3 * CH)
    stat[...] = jnp.zeros_like(stat)
    for ch in range(CH):
        rs_wait(rs_s, rs_r, i_br, ch)

        def second(q, ch=ch):
            r = pl.ds(mul(q * 32, 32), 32)
            r1 = pl.ds(mul(ch * RC + q * 32, 32), 32)
            branch = rs_sum(rs_r, rs_own, ch, r) + vec[4:5, :]
            resid = tok[r1, :].astype(f32) + branch
            res[r1, :] = resid
            zz, _ = layer_stats(resid)
            n2[pl.ds(mul(my + ch * RC + q * 32, 32), 32), :] = (
                zz * vec[5:6, :] + vec[6:7, :]).astype(bf16)
            v = valid_rows(ch * RC + q * 32, 32)
            stat[0:8, :] += jnp.sum((branch * branch * v).reshape(4, 8, D), axis=0)
            stat[8:16, :] += jnp.sum((resid * resid * v).reshape(4, 8, D), axis=0)

        loop(RC // 32, second)
        ag_start(n2, i_n2, ch)

    relay_step(down_block, i_dr, 2)
    relay_finish(up_block, i_ur)

    def feed(it):
        blk = ((y + it // 2) % 2) * 2 + (k + it % 2) % 2

        @pl.when(it == 1)
        def _():
            ag_wait(n2, i_n2, 0)
            ag_forward(n2, i_n2, 0)
            relay_step(down_block, i_dr, 3)

        @pl.when(it == 2)
        def _():
            ag_forward(n2, i_n2, 1)

        @pl.when(it == 3)
        def _():
            ag_wait(n2, i_n2, 2)

        def cols(n):
            c0 = pl.ds(mul(n * 512, 512), 512)
            pre = nn(n2[rows(blk), :], wup[:, c0]) + vec[8:9, c0]
            sq = pre * pre
            th = jnp.tanh(0.7978845608028654 * pre * (1.0 + 0.044715 * sq))
            a1 = 0.5 * (1.0 + th)
            act[rows(blk), c0] = (pre * a1).astype(bf16)
            der = a1 + 0.5 * pre * (1.0 - th * th) * (
                0.7978845608028654 * (1.0 + 0.134145 * sq))
            gpre[rows(blk), c0] = der.astype(bf16)

        loop(2, cols)

    loop(4, feed)

    def dw_half(a, b, c0, n, xx, hh):
        c1 = pl.ds(mul((hh * 2 + xx) * 128, 128), 128)
        c2 = pl.ds(mul(((3 - hh) * 2 + xx) * 128, 128), 128)
        return tn(jnp.concatenate([a[:, c1], a[:, c2]], axis=1), b[:, c0 : c0 + n])

    def dw_away(a, b, c0, n, xb, xr, i):
        def away(hh):
            r = pl.ds(mul(hh * 256, 256), 256)
            xb[r, c0 : c0 + n] = dw_half(a, b, c0, n, (x + 1) % 2, hh).astype(bf16)
            rcopy(xb.at[r, pl.ds(c0, n)], xr.at[r, pl.ds(c0, n)], xpeer, i + hh).start()
            sent(xb.at[pl.ds(0, 256), pl.ds(c0, n)], i + hh)

        for hh in range(2):
            away(hh)

    def dw_keep(a, b, c0, n, own):
        def keep(hh):
            own[pl.ds(mul(hh * 256, 256), 256), c0 : c0 + n] = dw_half(a, b, c0, n, x, hh)

        loop(2, keep)

    def dw_z(hh, c0, n, xr, own, zb, zo, zr, fin, i, iz):
        wait_bytes(xr.at[pl.ds(0, 256), pl.ds(c0, n)], rsem.at[i + hh])
        c = slice(c0, c0 + n)
        for sub, zz in enumerate((hh, 3 - hh)):
            r = slice(hh * 256 + sub * 128, hh * 256 + sub * 128 + 128)
            ro = slice(zo + zz * 128, zo + zz * 128 + 128)
            dz = (zz - z + 4) % 4

            @pl.when(zz == z)
            def _(r=r):
                fin[:, c] = own[r, c] + xr[r, c].astype(f32)

            @pl.when(zz != z)
            def _(r=r, ro=ro, zz=zz, dz=dz):
                zb[ro, c] = (own[r, c] + xr[r, c].astype(f32)).astype(bf16)
                rcopy(zb.at[ro, c], zr.at[dz - 1, :, c], {"seq": zz * 2 + x}, iz + dz).start()

            sent(zb.at[ro, c], iz + dz, zz != z)

    def dw_end(c0, n, zr, fin, iz):
        c = slice(c0, c0 + n)
        for d in (1, 2, 3):
            wait_bytes(zr.at[d - 1, :, c], rsem.at[iz + d])
        fin[:, c] += (zr[0, :, c].astype(f32) + zr[1, :, c].astype(f32)) + zr[2, :, c].astype(f32)

    ag_wait(gf, i_gf, 0)
    ag_wait(gf, i_gf, 2)
    i_dwx, i_dwz = take(2), take(4)
    dw_away(act, gf, 0, D, xs_down, xr_down, i_dwx)
    dw_keep(act, gf, 0, D, own_a)
    relay_finish(down_block, i_dr)
    wait_bytes(down_in, lsem.at[l_d])
    gvec[...] = jnp.zeros_like(gvec)

    def grad_feed(it):
        r = pl.ds(mul(it * R, R), R)

        def cols(n):
            c0 = pl.ds(mul(n * 512, 512), 512)
            ga = nt(gf[r, :], wdown[c0, :])
            g = (ga * gpre[r, c0].astype(f32)).astype(bf16)
            gpre[r, c0] = g
            gvec[2, :, c0] += jnp.sum(g.astype(f32).reshape(R // 8, 8, 512), axis=0)

        loop(2, cols)

    loop(4, grad_feed)

    rs_sent(rs_s, i_br)

    def gn2_part(blk, ch, dst):
        dst[...] = nt(gpre[pl.ds(mul(blk * R + ch * RC, RC), RC), :], wup[...])

    i_g2 = take(3 * CH)
    rs_run(gn2_part, rs_s, rs_r, rs_own, i_g2)

    def down_z(hh):
        dw_z(hh, 0, D, xr_down, own_a, gpre, 0, zr_down, fin_down, i_dwx, i_dwz)

    def up_z(hh):
        dw_z(hh, 0, D, xr_up, own_b, gpre, 512, zr_up, fin_up, i_uwx, i_uwz)

    i_uwx, i_uwz = take(2), take(4)
    dw_away(n2, gpre, 0, D, xs_up, xr_up, i_uwx)
    dw_keep(n2, gpre, 0, D, own_b)
    down_z(0)

    i_gb = take(3 * CH)
    for ch in range(CH):
        rs_wait(rs_s, rs_r, i_g2, ch)

        def third(q, ch=ch):
            r = pl.ds(mul(q * 32, 32), 32)
            r1 = pl.ds(mul(ch * RC + q * 32, 32), 32)
            g2 = rs_sum(rs_r, rs_own, ch, r)
            zz, rstd = layer_stats(res[r1, :])
            gout = cot[r1, :].astype(f32) * valid_rows(ch * RC + q * 32, 32)
            gres = gout + layer_back(g2, vec[5:6, :], zz, rstd)
            st_grad[r1, :] = gres
            low = gres.astype(bf16)
            gb[pl.ds(mul(my + ch * RC + q * 32, 32), 32), :] = low
            fold = lambda v: jnp.sum(v.reshape(4, 8, D), axis=0)
            gvec[4] += fold(low.astype(f32))
            gvec[5] += fold(g2 * zz)
            gvec[6] += fold(g2)
            gvec[7] += fold(gout)

        loop(RC // 32, third)
        ag_start(gb, i_gb, ch)

    down_z(1)
    ag_forward(gb, i_gb, 0)

    def ffn_part(blk, ch, dst):
        dst[...] = nn(act[pl.ds(mul(blk * R + ch * RC, RC), RC), :], wdown[...])

    i_ff = take(3 * CH)
    rs_run(ffn_part, rt_s, rt_r, rt_own, i_ff)
    ag_forward(gb, i_gb, 1)

    ag_wait(gb, i_gb, 0)
    ag_wait(gb, i_gb, 2)

    def att_grad(i):
        c0 = pl.ds(mul(i * 256, 256), 256)
        dot_[:, c0] = nt(wout[...], gb[c0, :]).astype(bf16)

    loop(4, att_grad)
    own_out[...] = nn(attt[...], gb[...])
    i_owx, i_owz = take(), take(4)
    for j in range(3 * CH):
        wait_bytes(gf.at[pl.ds(0, RC), :], ssem.at[i_gf + j])
        wait_bytes(n2.at[pl.ds(0, RC), :], ssem.at[i_n2 + j])
    xs_out = gf.at[pl.ds(512, 256), :]

    @pl.when(x != k)
    def _():
        gf[512:768, :] = own_out[...].astype(bf16)
        rcopy(xs_out, xr_out, xpeer, i_owx).start()

    sent(xs_out, i_owx, x != k)

    lane2 = lax.broadcasted_iota(jnp.int32, (1024, 128), 1)

    def pair_backward(i):
        p0 = pl.ds(mul(i * 128, 128), 128)
        for j in range(2):
            r0 = pl.ds(mul(i * 128 + j * 64, 64), 64)
            li = linv[2 * i + j, 0:1, :]
            dd = dot_[r0, :].astype(f32) * li
            delta = jnp.sum(dd * attt[r0, :].astype(f32), axis=0, keepdims=True)
            linv[2 * i + j, :, :] = jnp.broadcast_to(delta, (8, 1024))
            dot_[r0, :] = dd.astype(bf16)
        do_[...] = dot_[p0, :].T
        acck[...] = jnp.zeros_like(acck)
        accv[...] = jnp.zeros_like(accv)

        def queries(qb):
            q0 = pl.ds(mul(qb * 256, 256), 256)
            qblk = qkv[q0, pl.ds(mul(i * 384, 128), 128)]
            doblk = do_[q0, :]
            dt = dot_[p0, q0]

            def keys(kb, carry):
                k0 = pl.ds(mul(kb * 256, 256), 256)
                vblk = qkv[k0, pl.ds(mul(i * 384 + 256, 128), 128)]
                new = []
                for j in range(2):
                    p = ptri[2 * i + j, tri(kb, qb)]
                    dp = nn(half(vblk, j), dt) - linv[2 * i + j, 0:1, q0]
                    ds = (p.astype(f32) * dp).astype(bf16)
                    accv[j, k0, :] += nn(p, doblk)
                    acck[j, k0, :] += nn(ds, qblk)
                    kk = kt[pl.ds(mul(i * 128 + j * 64, 64), 64), k0]
                    new.append(carry[j] + nn(kk, ds))
                return tuple(new)

            zero = jnp.zeros((64, 256), f32)
            dq = lax.fori_loop(0, qb + 1, keys, (zero, zero))
            dq = jnp.concatenate(dq, axis=0) * 0.125
            dmix[q0, pl.ds(mul(i * 384, 128), 128)] = dq.T.astype(bf16)

        loop(4, queries)
        dk = jnp.where(lane2 < 64, acck[0], acck[1]) * 0.125
        dv = jnp.where(lane2 < 64, accv[0], accv[1])
        dmix[:, pl.ds(mul(i * 384 + 128, 128), 128)] = dk.astype(bf16)
        dmix[:, pl.ds(mul(i * 384 + 256, 128), 128)] = dv.astype(bf16)

    up_z(0)
    pair_backward(0)
    i_qwx, i_qwz = (take(2), take(2)), (take(4), take(4))
    dw_away(n1, dmix, 0, 384, gf, xr_qkv, i_qwx[0])
    pair_backward(1)

    rs_sent(rs_s, i_g2)

    def gn1_part(blk, ch, dst):
        dst[...] = nt(dmix[pl.ds(mul(blk * R + ch * RC, RC), RC), :], wqkv[...])

    i_g1 = take(3 * CH)
    up_z(1)
    rs_run(gn1_part, rs_s, rs_r, rs_own, i_g1)
    dw_away(n1, dmix, 384, 384, gf, xr_qkv, i_qwx[1])
    dw_keep(n1, dmix, 0, 768, own_a)

    def qkv_z(h):
        for hh in range(2):
            dw_z(hh, h * 384, 384, xr_qkv, own_a, n2, 0, zr_qkv, fin_qkv, i_qwx[h], i_qwz[h])

    for i in range(2):
        zi = y + 2 * i
        dz = (zi - z + 4) % 4

        @pl.when(x == k)
        def _(i=i, zi=zi, dz=dz):
            if i == 0:
                wait_bytes(xr_out, rsem.at[i_owx])
            half_rows = slice(i * 128, (i + 1) * 128)
            total = own_out[half_rows, :] + xr_out[half_rows, :].astype(f32)

            @pl.when(zi == z)
            def _():
                fin_out[...] = total

            @pl.when(zi != z)
            def _():
                n2[512 + i * 128 : 640 + i * 128, :] = total.astype(bf16)
                rcopy(n2.at[pl.ds(512 + i * 128, 128), :], zr_out.at[dz - 1], {"seq": zi * 2 + x}, i_owz + dz).start()

        sent(n2.at[pl.ds(512, 128), :], i_owz + dz, jnp.logical_and(x == k, zi != z))

    qkv_z(0)
    for ch in range(CH):
        rs_wait(rs_s, rs_r, i_g1, ch)

        def fourth(q, ch=ch):
            r = pl.ds(mul(q * 32, 32), 32)
            r1 = pl.ds(mul(ch * RC + q * 32, 32), 32)
            g1 = rs_sum(rs_r, rs_own, ch, r)
            zz, rstd = layer_stats(tok[r1, :].astype(f32))
            st_grad[r1, :] += layer_back(g1, vec[0:1, :], zz, rstd)
            fold = lambda v: jnp.sum(v.reshape(4, 8, D), axis=0)
            gvec[0] += fold(g1 * zz)
            gvec[1] += fold(g1)

        loop(RC // 32, fourth)
    l_g = next(lids)
    pltpu.make_async_copy(st_grad, o_grad, lsem.at[l_g]).start()

    gmat[...] = jnp.zeros_like(gmat)
    for r, v in ((0, 0), (1, 1), (4, 4), (5, 5), (6, 6), (7, 7), (8, 2)):
        gmat[r : r + 1, :] = jnp.sum(gvec[v], axis=0, keepdims=True)
    for r, p in ((2, 0), (3, 256)):
        for i in range(2):
            v = dmix[:, i * 384 + p : i * 384 + p + 128].astype(f32)
            v = jnp.sum(jnp.sum(v.reshape(128, 8, 128), axis=0), axis=0, keepdims=True)
            gmat[r : r + 1, pl.ds(mul((ctx + 4 * i) * 128, 128), 128)] = v
    for s in range(8):
        sg[s] = gmat[:, s * 128 : (s + 1) * 128]
    i_sgx, i_sgz, i_sgc = take(4), take(4), take(4)
    for j in range(4):
        src = sg.at[j * 2 + (x + 1) % 2]
        rcopy(src, sgx.at[j], xpeer, i_sgx + j).start()
        sent(src, i_sgx + j)

    qkv_z(1)
    for j in range(4):
        rcopy(sg.at[j], sgx.at[j], xpeer, i_sgx + j).wait_recv()
    for d in (1, 2, 3):
        zz = (z + d) % 4
        sgs[d - 1] = sg[zz * 2 + x] + sgx[zz]
        rcopy(sgs.at[d - 1], sgz.at[d - 1], zpeer(d), i_sgz + d).start()
        sent(sgs.at[d - 1], i_sgz + d)

    dw_end(0, D, zr_down, fin_down, i_dwz)
    l_dd = next(lids)
    pltpu.make_async_copy(fin_down, o_ddown, lsem.at[l_dd]).start()
    dw_end(0, D, zr_up, fin_up, i_uwz)
    i_uf, i_qf, i_of = take(4), (take(4), take(4)), take(4)

    def up_piece(fin, c, s):
        return (fin.at[pl.ds(mul(c * 32, 32), 32), pl.ds(s * 128, 128)],
                o_dup.at[:, pl.ds(mul((s * 4 + ctx) * 128, 128), 128)])

    for d in (1, 2, 3):
        for s in range(8):
            a, b = up_piece(fin_up, (ctx + d) % 4, s)
            rcopy(a, b, cpeer(d), i_uf + d).start()
        sent(fin_up.at[pl.ds(0, 32), :], i_uf + d)
    mine32 = pl.ds(mul(ctx * 32, 32), 32)
    l_up = next(lids)
    for s in range(8):
        a, b = up_piece(fin_up, ctx, s)
        pltpu.make_async_copy(a, b, lsem.at[l_up]).start()

    l_do = next(lids)

    @pl.when(ctx == t)
    def _():
        for d in (1, 2, 3):
            wait_bytes(zr_out.at[d - 1], rsem.at[i_owz + d])
        fin_out[...] += (zr_out[0].astype(f32) + zr_out[1].astype(f32)) + zr_out[2].astype(f32)
        for d in (1, 2, 3):
            src = fin_out.at[pl.ds(mul(((ctx + d) % 4) * 32, 32), 32), :]
            rcopy(src, o_dout, cpeer(d), i_of + d).start()
        pltpu.make_async_copy(fin_out.at[mine32, :], o_dout, lsem.at[l_do]).start()

    for d in (1, 2, 3):
        sent(fin_out.at[pl.ds(0, 32), :], i_of + d, ctx == t)

    for ch in range(CH):
        rs_wait(rt_s, rt_r, i_ff, ch)

        def last(q, ch=ch):
            r = pl.ds(mul(q * 32, 32), 32)
            r1 = pl.ds(mul(ch * RC + q * 32, 32), 32)
            ffn = rs_sum(rt_r, rt_own, ch, r) + vec[7:8, :]
            v = valid_rows(ch * RC + q * 32, 32)
            st_out[r1, :] = (v * (res[r1, :] + ffn)).astype(bf16)
            stat[16:24, :] += jnp.sum((ffn * ffn * v).reshape(4, 8, D), axis=0)

        loop(RC // 32, last)
    l_t = next(lids)
    pltpu.make_async_copy(st_out, o_out, lsem.at[l_t]).start()

    for d in (1, 2, 3):
        wait_bytes(sgz.at[d - 1], rsem.at[i_sgz + d])
    sgf[...] = sg[seq] + sgx[z] + (sgz[0] + sgz[1] + sgz[2])
    for j in range(3):
        v = jnp.sum(stat[j * 8 : (j + 1) * 8, :], axis=0, keepdims=True)
        sgf[9 + j : 10 + j, :] = jnp.broadcast_to(jnp.sum(v, axis=1, keepdims=True), (1, 128))
    for d in (1, 2, 3):
        rcopy(sgf, sgc.at[d], cpeer(d), i_sgc + d).start()
        sent(sgf, i_sgc + d)

    l_dq = []
    for h in range(2):
        dw_end(h * 384, 384, zr_qkv, fin_qkv, i_qwz[h])
        pieces = list(qkv_pieces(ctx))[3 * h : 3 * h + 3]
        for d in (1, 2, 3):
            c2 = (ctx + d) % 4
            for a, b in pieces:
                rcopy(fin_qkv.at[pl.ds(mul(c2 * 32, 32), 32), b], o_dqkv.at[:, a], cpeer(d), i_qf[h] + d).start()
            sent(fin_qkv.at[pl.ds(0, 32), pl.ds(0, 384)], i_qf[h] + d)
        l_dq.append(next(lids))
        for a, b in pieces:
            pltpu.make_async_copy(fin_qkv.at[mine32, b], o_dqkv.at[:, a], lsem.at[l_dq[h]]).start()

    for d in (1, 2, 3):
        wait_bytes(sgc.at[d], rsem.at[i_sgc + d])
    o_small[...] = sgf[...] + jnp.where(rowid != 8, sgc[1] + sgc[2] + sgc[3], 0.0)

    @pl.when(ctx != t)
    def _():
        wait_bytes(fin_out.at[pl.ds(0, 32), :], rsem.at[i_of + (ctx - t + 4) % 4])

    @pl.when(ctx == t)
    def _():
        wait_bytes(fin_out.at[pl.ds(0, 32), :], lsem.at[l_do])

    for d in (1, 2, 3):
        wait_bytes(fin_up.at[pl.ds(0, 32), :], rsem.at[i_uf + d])
        for h in range(2):
            wait_bytes(fin_qkv.at[pl.ds(0, 32), pl.ds(0, 384)], rsem.at[i_qf[h] + d])
    rs_sent(rs_s, i_g1)
    rs_sent(rt_s, i_ff)
    for block, i in ((qkv_block, i_qr), (up_block, i_ur), (down_block, i_dr)):
        relay_sent(block, i)
    flush()
    for ref, i in ((st_grad, l_g), (st_out, l_t), (fin_down, l_dd), (fin_up.at[pl.ds(0, 32), :], l_up),
                   (fin_qkv.at[pl.ds(0, 32), pl.ds(0, 384)], l_dq[0]),
                   (fin_qkv.at[pl.ds(0, 32), pl.ds(0, 384)], l_dq[1])):
        wait_bytes(ref, lsem.at[i])
    assert next(ids) <= NSEM, next(ids)


def finish_kernel(length_ref, sums, *refs):
    big, outs, vecs = refs[:6], refs[6:12], refs[12:20]
    o_ub, o_stats = refs[20:22]
    stage, s_in, s_out = refs[22:28], refs[28], refs[29]
    for i in range(6):
        pltpu.make_async_copy(big[i], stage[i], s_in.at[i]).start()
    ctx = lax.axis_index("ctx")
    mine = sums[0:8, 0:32]
    for c in range(1, 4):
        mine = jnp.where(ctx == c, sums[0:8, c * 32 : (c + 1) * 32], mine)
    for r in range(8):
        vecs[r][...] = mine[r, :]
    o_ub[...] = sums[8, :]
    lane = lax.broadcasted_iota(jnp.int32, (1, 128), 1)
    v = jnp.where(lane == 0, sums[9:10, :], jnp.where(lane == 1, sums[10:11, :], sums[11:12, :]))
    o_stats[...] = jnp.sqrt(v / (length_ref[0].astype(f32) * D))[:, 0:3]
    for i in range(6):
        pltpu.make_async_copy(big[i], stage[i], s_in.at[i]).wait()
        pltpu.make_async_copy(stage[i], outs[i], s_out.at[i]).start()
    for i in range(6):
        pltpu.make_async_copy(stage[i], outs[i], s_out.at[i]).wait()


def fast(mesh):
    def scratch():
        v = lambda dt, *shape: pltpu.VMEM(shape, dt)
        return [
            v(bf16, D, 768), v(bf16, 256, D), v(bf16, D, D), v(bf16, D, D),
            v(f32, 4, 16, 128), v(f32, 8, 16, 128), v(f32, 16, D),
            v(bf16, S, D), v(bf16, S, D), v(bf16, S, D), v(bf16, S, D), v(bf16, S, D), v(bf16, S, D),
            v(bf16, S, 768), v(bf16, 256, S), v(bf16, 256, S), v(bf16, 256, S),
            v(bf16, 256, S), v(bf16, S, 128), v(bf16, S, 768), v(f32, 4, 8, S),
            v(bf16, 4, 10, 256, 256), v(f32, 2, S, 128), v(f32, 2, S, 128),
            v(bf16, 3, 2, 128, D), v(bf16, 3, 2, 128, D), v(f32, 2, 128, D),
            v(bf16, 3, 2, 128, D), v(bf16, 3, 2, 128, D), v(f32, 2, 128, D),
            v(f32, 128, D), v(f32, R, D),
            v(bf16, 512, D), v(bf16, 512, D), v(bf16, 512, D), v(bf16, 512, D), v(bf16, 512, 768), v(bf16, 256, D),
            v(f32, 512, D), v(f32, 512, D), v(f32, 256, D),
            v(bf16, 3, 128, D), v(bf16, 3, 128, D), v(bf16, 3, 128, 768), v(bf16, 3, 128, D),
            v(f32, 128, D), v(f32, 128, 768), v(f32, 128, D),
            v(bf16, R, D), v(f32, R, D), v(f32, 128, D),
            v(f32, 8, 16, 128), v(f32, 4, 16, 128), v(f32, 3, 16, 128), v(f32, 3, 16, 128),
            v(f32, 16, 128), v(f32, 4, 16, 128), v(f32, 8, 8, D), v(f32, 16, D), v(f32, 24, D), v(f32, 8, 768),
            pltpu.SemaphoreType.DMA((16,)),
            pltpu.SemaphoreType.DMA((NSEM,)),
            pltpu.SemaphoreType.DMA((NSEM,)),
        ]

    def on_device(tokens, lengths, cotangent, g1, b1, wq, qb, vb, wo, ob, g2, b2, wu, ub, wd, db):
        ctx = lax.axis_index("ctx")
        vectors = jnp.stack([g1, b1, qb, vb, ob, g2, b2, db]).astype(f32)
        place = (jnp.arange(128) // 32) == ctx
        small = jnp.concatenate([
            jnp.where(place[None], jnp.tile(vectors, (1, 4)), 0.0),
            ub.astype(f32)[None], jnp.zeros((7, 128), f32)])
        vm = pl.BlockSpec(memory_space=pltpu.VMEM)
        sds = jax.ShapeDtypeStruct
        out, grad, dqkv, dout, dup, ddown, sums = pl.pallas_call(
            block_kernel,
            out_shape=(sds((R, D), bf16), sds((R, D), f32), sds((32, 3 * D), f32), sds((32, D), f32),
                       sds((32, 4 * D), f32), sds((128, D), f32), sds((16, 128), f32)),
            in_specs=[pl.BlockSpec(memory_space=pltpu.SMEM)] + [vm] * 7,
            out_specs=tuple([pl.BlockSpec(memory_space=pl.ANY)] * 6 + [vm]),
            scratch_shapes=scratch(),
            compiler_params=pltpu.CompilerParams(
                collective_id=0, has_side_effects=True, vmem_limit_bytes=LIMIT),
            name="block",
        )(lengths, tokens[0], cotangent[0], small, wq, wo, wu, wd)
        anyspec = pl.BlockSpec(memory_space=pl.ANY)
        big = (out, grad, dqkv, dout, dup, ddown)
        res = pl.pallas_call(
            finish_kernel,
            out_shape=tuple(sds(v.shape, v.dtype) for v in big)
            + tuple([sds((32,), f32)] * 8) + (sds((128,), f32), sds((1, 3), f32)),
            in_specs=[pl.BlockSpec(memory_space=pltpu.SMEM), vm] + [anyspec] * 6,
            out_specs=tuple([anyspec] * 6 + [vm] * 10),
            scratch_shapes=[pltpu.VMEM(v.shape, v.dtype) for v in big]
            + [pltpu.SemaphoreType.DMA((6,)), pltpu.SemaphoreType.DMA((6,))],
            compiler_params=pltpu.CompilerParams(vmem_limit_bytes=8 << 20),
            name="finish",
        )(lengths, sums, *big)
        out, grad, dqkv, dout, dup, ddown, g1, b1, qb, vb, ob, g2, b2, db, ub, stats = res
        return (out[None], grad[None], g1, b1, dqkv, qb, vb, dout, ob, g2, b2, dup, ub, ddown, db, stats)

    return on_device


HEADS = 16


epsilon = 1e-05


def normalize(inputs, gain, shift):
    average = jnp.mean(inputs, axis=-1, keepdims=True)
    centred = inputs - average
    variance = jnp.mean(centred * centred, axis=-1, keepdims=True)
    return centred * lax.rsqrt(variance + epsilon) * gain + shift


def gelu_tanh(inputs):
    return jax.nn.gelu(inputs, approximate=True)


def inner_rows(left, right):
    return lax.dot_general(
        left, right, (((0,), (0,)), ((), ())), preferred_element_type=jnp.float32
    )


def outer_cols(left, right):
    return lax.dot_general(
        left, right, (((1,), (1,)), ((), ())), preferred_element_type=jnp.float32
    )


def alibi_scores(query_block, key_block, query_pos, key_pos, slope_block):
    raw = jnp.einsum("qhd,khd->hqk", query_block, key_block, preferred_element_type=jnp.float32)
    offset = (key_pos[None, :] - query_pos[:, None]).astype(jnp.float32)
    scores = raw * query_block.shape[-1] ** (-0.5) + slope_block[:, None, None] * offset[None]
    allowed = key_pos[None, :] <= query_pos[:, None]
    return (scores, allowed)


def score_grads(
    query_block,
    key_block,
    value_block,
    grad_block,
    query_pos,
    key_pos,
    slope_block,
    log_block,
    delta_block,
):
    scores, allowed = alibi_scores(query_block, key_block, query_pos, key_pos, slope_block)
    probs = jnp.where(allowed[None], jnp.exp(scores - log_block[..., None]), 0.0)
    grad_probs = jnp.einsum(
        "qhd,khd->hqk", grad_block, value_block, preferred_element_type=jnp.float32
    )
    delta_block = jnp.sum(probs * grad_probs, axis=-1)
    grad_scores = (probs * (grad_probs - delta_block[..., None])).astype(jnp.bfloat16)
    return (probs, grad_scores, delta_block)


def on_device(
    tokens,
    lengths,
    cotangent,
    ln1_gain,
    ln1_bias,
    qkv_weight,
    query_bias,
    value_bias,
    out_weight,
    out_bias,
    ln2_gain,
    ln2_bias,
    up_weight,
    up_bias,
    down_weight,
    down_bias,
):
    shards = (
        ln1_gain,
        ln1_bias,
        qkv_weight,
        query_bias,
        value_bias,
        out_weight,
        out_bias,
        ln2_gain,
        ln2_bias,
        up_weight,
        up_bias,
        down_weight,
        down_bias,
    )
    row_count = tokens.shape[1]
    model_width = tokens.shape[2]
    head_count = HEADS
    head_width = model_width // head_count
    per_block = 2
    block_count = head_count // per_block
    slot_rows = row_count * lax.axis_size("ctx")
    positions = lax.axis_index("ctx") * row_count + jnp.arange(row_count, dtype=jnp.int32)
    length = lengths[0]
    valid_rows = (positions < length).astype(jnp.float32)[:, None]
    slopes = jnp.exp2(-8.0 * (jnp.arange(head_count, dtype=jnp.float32) + 1.0) / head_count)
    key_positions = jnp.arange(slot_rows, dtype=jnp.int32)
    scale = head_width ** (-0.5)
    full_weights = (
        lax.all_gather(shards[0], ("seq", "ctx"), axis=0, tiled=True),
        lax.all_gather(shards[1], ("seq", "ctx"), axis=0, tiled=True),
        lax.all_gather(shards[2], ("seq", "ctx"), axis=0, tiled=True),
        lax.all_gather(shards[3], ("seq", "ctx"), axis=0, tiled=True),
        lax.all_gather(shards[4], ("seq", "ctx"), axis=0, tiled=True),
        lax.all_gather(shards[5], ("seq", "ctx"), axis=0, tiled=True),
        lax.all_gather(shards[6], ("seq", "ctx"), axis=0, tiled=True),
        lax.all_gather(shards[7], ("seq", "ctx"), axis=0, tiled=True),
        lax.all_gather(shards[8], ("seq", "ctx"), axis=0, tiled=True),
        lax.all_gather(shards[9], ("seq", "ctx"), axis=0, tiled=True),
        lax.all_gather(shards[10], ("seq", "ctx"), axis=0, tiled=True),
        lax.all_gather(shards[11], ("seq", "ctx"), axis=0, tiled=True),
        lax.all_gather(shards[12], ("seq", "ctx"), axis=0, tiled=True),
    )
    (
        gain_one,
        shift_one,
        w_qkv,
        bias_query,
        bias_value,
        w_out,
        bias_out,
        gain_two,
        shift_two,
        w_up,
        bias_up,
        w_down,
        bias_down,
    ) = full_weights

    def pick(array, index):
        return lax.dynamic_slice_in_dim(array, index * per_block, per_block, 1)

    def pick_slopes(index):
        return lax.dynamic_slice_in_dim(slopes, index * per_block, per_block, 0)

    def to_blocks(array):
        return array.transpose(1, 0, 2, 3).reshape(array.shape[1], model_width)

    source = tokens[0].astype(jnp.float32)
    normed_one, back_one = jax.vjp(normalize, source, gain_one, shift_one)
    normed_low = normed_one.astype(jnp.bfloat16)
    mixed = jnp.dot(normed_low, w_qkv, preferred_element_type=jnp.float32)
    query = (mixed[:, :model_width] + bias_query).astype(jnp.bfloat16)
    keys = mixed[:, model_width : 2 * model_width].astype(jnp.bfloat16)
    values = (mixed[:, 2 * model_width :] + bias_value).astype(jnp.bfloat16)
    all_keys, all_values = (
        lax.all_gather(keys, "ctx", axis=0, tiled=True),
        lax.all_gather(values, "ctx", axis=0, tiled=True),
    )
    query_heads = query.reshape(row_count, head_count, head_width)
    key_heads = all_keys.reshape(slot_rows, head_count, head_width)
    value_heads = all_values.reshape(slot_rows, head_count, head_width)

    def forward_block(index):
        scores, allowed = alibi_scores(
            pick(query_heads, index),
            pick(key_heads, index),
            positions,
            key_positions,
            pick_slopes(index),
        )
        masked = jnp.where(allowed[None], scores, -1e30)
        highest = jnp.max(masked, axis=-1)
        total = jnp.sum(jnp.exp(masked - highest[..., None]), axis=-1)
        log_total = highest + jnp.log(total)
        probs = jnp.where(allowed[None], jnp.exp(scores - log_total[..., None]), 0.0)
        block_out = jnp.einsum(
            "hqk,khd->qhd",
            probs.astype(jnp.bfloat16),
            pick(value_heads, index),
            preferred_element_type=jnp.float32,
        )
        return (block_out, log_total)

    head_out, log_totals = lax.map(forward_block, jnp.arange(block_count))
    attended = to_blocks(head_out).astype(jnp.bfloat16)
    branch = jnp.dot(attended, w_out, preferred_element_type=jnp.float32) + bias_out
    resid = source + branch
    normed_two, back_two = jax.vjp(normalize, resid, gain_two, shift_two)
    normed_two_low = normed_two.astype(jnp.bfloat16)
    pre_act = jnp.dot(normed_two_low, w_up, preferred_element_type=jnp.float32) + bias_up
    activated, back_act = jax.vjp(gelu_tanh, pre_act)
    activated_low = activated.astype(jnp.bfloat16)
    ffn = jnp.dot(activated_low, w_down, preferred_element_type=jnp.float32) + bias_down
    output = (valid_rows * (resid + ffn)).astype(jnp.bfloat16)[None]
    squares = jnp.stack(
        [
            jnp.sum(valid_rows * branch * branch),
            jnp.sum(valid_rows * resid * resid),
            jnp.sum(valid_rows * ffn * ffn),
        ]
    )
    totals = lax.psum(squares, "ctx")
    stats = jnp.sqrt(totals / (length.astype(jnp.float32) * model_width))[None]
    w_qkv, w_out, w_up, w_down = (
        lax.all_gather(qkv_weight, ("seq", "ctx"), axis=0, tiled=True),
        lax.all_gather(out_weight, ("seq", "ctx"), axis=0, tiled=True),
        lax.all_gather(up_weight, ("seq", "ctx"), axis=0, tiled=True),
        lax.all_gather(down_weight, ("seq", "ctx"), axis=0, tiled=True),
    )
    grad_out = cotangent[0].astype(jnp.float32) * valid_rows
    grad_ffn = grad_out.astype(jnp.bfloat16)
    grad_down_w = inner_rows(activated_low, grad_ffn)
    grad_down_b = jnp.sum(grad_ffn.astype(jnp.float32), axis=0)
    grad_activated = outer_cols(grad_ffn, w_down)
    (grad_pre,) = back_act(grad_activated)
    grad_pre_low = grad_pre.astype(jnp.bfloat16)
    grad_up_w = inner_rows(normed_two_low, grad_pre_low)
    grad_up_b = jnp.sum(grad_pre_low.astype(jnp.float32), axis=0)
    grad_normed_two = outer_cols(grad_pre_low, w_up)
    grad_resid_norm, grad_gain_two, grad_shift_two = back_two(grad_normed_two)
    grad_resid = grad_out + grad_resid_norm
    grad_branch = grad_resid.astype(jnp.bfloat16)
    grad_out_w = inner_rows(attended, grad_branch)
    grad_out_b = jnp.sum(grad_branch.astype(jnp.float32), axis=0)
    grad_attended = outer_cols(grad_branch, w_out).astype(jnp.bfloat16)
    grad_heads = grad_attended.reshape(row_count, head_count, head_width)

    def backward_block(index):
        query_block = pick(query_heads, index)
        key_block = pick(key_heads, index)
        grad_block = pick(grad_heads, index)
        probs, grad_scores, delta_block = score_grads(
            query_block,
            key_block,
            pick(value_heads, index),
            grad_block,
            positions,
            key_positions,
            pick_slopes(index),
            log_totals[index],
            None,
        )
        grad_query_block = (
            jnp.einsum("hqk,khd->qhd", grad_scores, key_block, preferred_element_type=jnp.float32)
            * scale
        )
        grad_key_block = (
            jnp.einsum("hqk,qhd->khd", grad_scores, query_block, preferred_element_type=jnp.float32)
            * scale
        )
        grad_value_block = jnp.einsum(
            "hqk,qhd->khd",
            probs.astype(jnp.bfloat16),
            grad_block,
            preferred_element_type=jnp.float32,
        )
        return (grad_query_block, grad_key_block, grad_value_block)

    query_parts, key_parts, value_parts = lax.map(backward_block, jnp.arange(block_count))
    grad_query_all = to_blocks(query_parts)
    own_keys, own_values = (
        lax.psum_scatter(
            to_blocks(key_parts).astype(jnp.bfloat16), "ctx", scatter_dimension=0, tiled=True
        ).astype(jnp.float32),
        lax.psum_scatter(
            to_blocks(value_parts).astype(jnp.bfloat16), "ctx", scatter_dimension=0, tiled=True
        ).astype(jnp.float32),
    )
    grad_query_low = grad_query_all.astype(jnp.bfloat16)
    grad_key_low = own_keys.astype(jnp.bfloat16)
    grad_value_low = own_values.astype(jnp.bfloat16)
    grad_mixed = jnp.concatenate([grad_query_low, grad_key_low, grad_value_low], axis=1)
    grad_qkv_w = inner_rows(normed_low, grad_mixed)
    grad_query_bias = jnp.sum(grad_query_low.astype(jnp.float32), axis=0)
    grad_value_bias = jnp.sum(grad_value_low.astype(jnp.float32), axis=0)
    grad_normed_one = outer_cols(grad_mixed, w_qkv)
    grad_source_norm, grad_gain_one, grad_shift_one = back_one(grad_normed_one)
    grad_tokens = (grad_resid + grad_source_norm)[None]
    summed = (
        lax.psum_scatter(
            grad_gain_one.astype(jnp.float32), ("seq", "ctx"), scatter_dimension=0, tiled=True
        ),
        lax.psum_scatter(
            grad_shift_one.astype(jnp.float32), ("seq", "ctx"), scatter_dimension=0, tiled=True
        ),
        lax.psum_scatter(grad_qkv_w, ("seq", "ctx"), scatter_dimension=0, tiled=True),
        lax.psum_scatter(grad_query_bias, ("seq", "ctx"), scatter_dimension=0, tiled=True),
        lax.psum_scatter(grad_value_bias, ("seq", "ctx"), scatter_dimension=0, tiled=True),
        lax.psum_scatter(grad_out_w, ("seq", "ctx"), scatter_dimension=0, tiled=True),
        lax.psum_scatter(grad_out_b, ("seq", "ctx"), scatter_dimension=0, tiled=True),
        lax.psum_scatter(
            grad_gain_two.astype(jnp.float32), ("seq", "ctx"), scatter_dimension=0, tiled=True
        ),
        lax.psum_scatter(
            grad_shift_two.astype(jnp.float32), ("seq", "ctx"), scatter_dimension=0, tiled=True
        ),
        lax.psum_scatter(grad_up_w, ("seq", "ctx"), scatter_dimension=0, tiled=True),
        lax.psum_scatter(grad_up_b, ("seq", "ctx"), scatter_dimension=0, tiled=True),
        lax.psum_scatter(grad_down_w, ("seq", "ctx"), scatter_dimension=0, tiled=True),
        lax.psum_scatter(grad_down_b, ("seq", "ctx"), scatter_dimension=0, tiled=True),
    )
    return (output, grad_tokens) + tuple(summed) + (stats,)


def solution(mesh):
    small_slice = mesh.shape["seq"] == 8 and mesh.shape["ctx"] == 4
    placed = (
        P("seq", "ctx", None),
        P("seq"),
        P("seq", "ctx", None),
        P(("seq", "ctx")),
        P(("seq", "ctx")),
        P(("seq", "ctx"), None),
        P(("seq", "ctx")),
        P(("seq", "ctx")),
        P(("seq", "ctx"), None),
        P(("seq", "ctx")),
        P(("seq", "ctx")),
        P(("seq", "ctx")),
        P(("seq", "ctx"), None),
        P(("seq", "ctx")),
        P(("seq", "ctx"), None),
        P(("seq", "ctx")),
    )
    return jax.shard_map(
        fast(mesh) if small_slice else on_device,
        mesh=mesh,
        in_specs=placed,
        out_specs=(
            P("seq", "ctx", None),
            P("seq", "ctx", None),
            P(("seq", "ctx")),
            P(("seq", "ctx")),
            P(("seq", "ctx"), None),
            P(("seq", "ctx")),
            P(("seq", "ctx")),
            P(("seq", "ctx"), None),
            P(("seq", "ctx")),
            P(("seq", "ctx")),
            P(("seq", "ctx")),
            P(("seq", "ctx"), None),
            P(("seq", "ctx")),
            P(("seq", "ctx"), None),
            P(("seq", "ctx")),
            P("seq", None),
        ),
        check_vma=False,
    )
```

```python
import itertools

import jax
import jax.numpy as jnp
from jax import lax
from jax.experimental import pallas as pl
from jax.experimental.pallas import tpu as pltpu
from jax.sharding import PartitionSpec as P

MESH = pl.DeviceIdType.MESH
bf16, f32 = jnp.bfloat16, jnp.float32
LOG2E = 1.4426950408889634
D = 1024
R = 256
S = 1024
LIMIT = 66_000_000
NSEM = 170
ORDER = (2, 3, 1)


def nn(a, b):
    return lax.dot_general(a, b, (((1,), (0,)), ((), ())), preferred_element_type=f32)


def nt(a, b):
    return lax.dot_general(a, b, (((1,), (1,)), ((), ())), preferred_element_type=f32)


def tn(a, b):
    return lax.dot_general(a, b, (((0,), (0,)), ((), ())), preferred_element_type=f32)


def mul(v, m):
    return pl.multiple_of(v, m)


def loop(n, body, start=0):
    def step(i, carry):
        body(i)
        return carry

    lax.fori_loop(start, n, step, 0)


def layer_stats(v):
    mean = jnp.sum(v, axis=-1, keepdims=True) * (1.0 / D)
    cen = v - mean
    var = jnp.sum(cen * cen, axis=-1, keepdims=True) * (1.0 / D)
    rstd = lax.rsqrt(var + 1e-5)
    return cen * rstd, rstd


def layer_back(g2, gain, z, rstd):
    g = g2 * gain
    m1 = jnp.sum(g, axis=-1, keepdims=True) * (1.0 / D)
    m2 = jnp.sum(g * z, axis=-1, keepdims=True) * (1.0 / D)
    return rstd * (g - m1 - z * m2)


def block_kernel(
    length_ref, tok, cot, small, qkv_in, out_in, up_in, down_in,
    o_out, o_grad, o_dqkv, o_dout, o_dup, o_ddown, o_small,
    wqkv, wout, wup, wdown, smc, smb, vec,
    n1, n2, gf, gb, act, gpre, qkv, vt, kt, attt, dot_, do_, dmix, linv,
    ptri, acck, accv,
    rs_s, rs_r, rs_own, rt_s, rt_r, rt_own, tmp, res,
    xs_down, xs_up, xr_down, xr_up, xr_qkv, xr_out, own_a, own_b, own_out,
    zr_down, zr_up, zr_qkv, zr_out, fin_up, fin_qkv, fin_out,
    st_out, st_grad, fin_down, sg, sgx, sgs, sgz, sgf, sgc, gvec, gmat, stat, qbias,
    lsem, ssem, rsem,
):
    seq, ctx = lax.axis_index("seq"), lax.axis_index("ctx")
    z, x = seq // 2, seq % 2
    y, k = ctx // 2, ctx % 2
    ids = itertools.count()
    lids = itertools.count()

    mate = {"ctx": y * 2 + (k + 1) % 2}
    ypeer = {"ctx": ((y + 1) % 2) * 2 + k}
    xpeer = {"seq": z * 2 + (x + 1) % 2}

    def cpeer(d):
        return {"ctx": (ctx + d) % 4}

    def zpeer(d):
        return {"seq": ((z + d) % 4) * 2 + x}

    def take(n=1):
        first = next(ids)
        for _ in range(n - 1):
            next(ids)
        return first

    def rcopy(src, dst, dev, i):
        return pltpu.make_async_remote_copy(
            src_ref=src, dst_ref=dst, send_sem=ssem.at[i], recv_sem=rsem.at[i],
            device_id=dev, device_id_type=MESH)

    def wait_bytes(ref, sem):
        pltpu.make_async_copy(ref, ref, sem).wait()

    sends = []

    def sent(ref, i, cond=None):
        sends.append((ref, i, cond))

    def flush():
        for ref, i, cond in sends:
            if cond is None:
                wait_bytes(ref, ssem.at[i])
            else:
                @pl.when(cond)
                def _(ref=ref, i=i):
                    wait_bytes(ref, ssem.at[i])
        sends.clear()

    rows = lambda c: pl.ds(mul(c * R, R), R)
    srow = lambda s: pl.ds(s * 128 if isinstance(s, int) else mul(s * 128, 128), 128)

    barrier = pltpu.get_barrier_semaphore()
    for d in (1, 2, 3):
        pl.semaphore_signal(barrier, inc=1, device_id=cpeer(d), device_id_type=MESH)
        pl.semaphore_signal(barrier, inc=1, device_id=zpeer(d), device_id_type=MESH)
    pl.semaphore_signal(barrier, inc=1, device_id=xpeer, device_id_type=MESH)
    pl.semaphore_wait(barrier, 7)

    i_smc = take(4)
    for d in (1, 2, 3):
        rcopy(small, smc.at[d], cpeer(d), i_smc + d).start()
        sent(small, i_smc + d)
    own32 = pl.ds(mul(seq * 128 + ctx * 32, 32), 32)

    def qkv_pieces(c):
        for j in range(6):
            yield (pl.ds(mul((j % 3) * D + (c + 4 * (j // 3)) * 128, 128), 128),
                   pl.ds(j * 128, 128))

    i_qa = take(4)
    for d in (1, 2, 3):
        for a, b in qkv_pieces((ctx + d) % 4):
            rcopy(qkv_in.at[:, a], wqkv.at[own32, b], cpeer(d), i_qa + d).start()
        sent(wqkv.at[pl.ds(0, 32), :], i_qa + d)
    l_q = next(lids)
    for a, b in qkv_pieces(ctx):
        pltpu.make_async_copy(qkv_in.at[:, a], wqkv.at[own32, b], lsem.at[l_q]).start()

    t = seq % 4
    out32 = pl.ds(mul((seq // 4) * 128 + ctx * 32, 32), 32)
    i_oa = take()
    l_o = next(lids)

    @pl.when(ctx != t)
    def _():
        rcopy(out_in, wout.at[out32, :], {"ctx": t}, i_oa).start()

    sent(out_in, i_oa, ctx != t)

    @pl.when(ctx == t)
    def _():
        pltpu.make_async_copy(out_in, wout.at[out32, :], lsem.at[l_o]).start()

    i_ua = take(4)
    for d in (1, 2, 3):
        c2 = (ctx + d) % 4
        for s in range(8):
            rcopy(up_in.at[:, pl.ds(mul((s * 4 + c2) * 128, 128), 128)],
                  wup.at[own32, pl.ds(s * 128, 128)], cpeer(d), i_ua + d).start()
        sent(wup.at[pl.ds(0, 32), :], i_ua + d)
    l_u = next(lids)
    for s in range(8):
        pltpu.make_async_copy(up_in.at[:, pl.ds(mul((s * 4 + ctx) * 128, 128), 128)],
                              wup.at[own32, pl.ds(s * 128, 128)], lsem.at[l_u]).start()

    for d in (1, 2, 3):
        rcopy(small, smc.at[d], cpeer(d), i_smc + d).wait_recv()
    rowid = lax.broadcasted_iota(jnp.int32, (16, 128), 0)
    smb[seq] = small[...] + jnp.where(rowid < 8, smc[1] + smc[2] + smc[3], 0.0)

    def gather_z(block, zi, src=None):
        own = block(seq) if src is None else src
        for d in ORDER:
            rcopy(own, block(seq), zpeer(d), zi + d).start()
            sent(own, zi + d)

    def gather_x(block, xi, src=None):
        own = block(seq) if src is None else src
        rcopy(own, block(seq), xpeer, xi).start()
        sent(own, xi)

    def gather_forward(block, zi, xi, d):
        b = block(((z - d + 4) % 4) * 2 + x)
        rcopy(b, b, xpeer, zi + d).wait_recv()
        rcopy(b, b, xpeer, xi + d).start()
        sent(block(0), xi + d)

    def gather_finish(block, xi):
        for d in range(4):
            b = block(seq)
            rcopy(b, b, xpeer, xi + d).wait_recv()

    def relay_start(block, i, src=None):
        own = block(seq) if src is None else src
        for cond, step, first in ((z < 3, 1, i), (z > 0, -1, i + 4)):
            @pl.when(cond)
            def _(step=step, first=first):
                rcopy(own, block(seq), {"seq": (z + step) * 2 + x}, first + 1).start()

            sent(own, first + 1, cond)

    def relay_x(block, i, src=None):
        own = block(seq) if src is None else src
        rcopy(own, block(seq), xpeer, i + 8 + z).start()
        sent(own, i + 8 + z)

    def relay_step(block, i, j):
        for has, on, step, first in ((z >= j, z < 3, 1, i), (z + j <= 3, z > 0, -1, i + 4)):
            zz = z - j * step

            @pl.when(has)
            def _(on=on, step=step, first=first, zz=zz):
                b = block(zz * 2 + x)
                rcopy(b, b, xpeer, first + j).wait_recv()
                if j < 3:
                    @pl.when(on)
                    def _():
                        rcopy(b, b, {"seq": (z + step) * 2 + x}, first + j + 1).start()
                rcopy(b, b, xpeer, i + 8 + zz).start()

            if j < 3:
                sent(block(0), first + j + 1, jnp.logical_and(has, on))

    def relay_finish(block, i):
        for zz in range(4):
            rcopy(block(0), block(0), xpeer, i + 8 + zz).wait_recv()

    def relay_sent(block, i):
        for j in (1, 2, 3):
            for has, zz in ((z >= j, z - j), (z + j <= 3, z + j)):
                @pl.when(has)
                def _(zz=zz):
                    wait_bytes(block(0), ssem.at[i + 8 + zz])

    small_block = lambda s: smb.at[s]
    i_sz, i_sx = take(4), take(4)
    gather_z(small_block, i_sz)
    gather_x(small_block, i_sx)

    for d in (1, 2, 3):
        wait_bytes(wqkv.at[pl.ds(0, 32), :], rsem.at[i_qa + d])
    wait_bytes(wqkv.at[pl.ds(0, 32), :], lsem.at[l_q])
    qkv_block = lambda s: wqkv.at[srow(s), :]
    i_qr = take(12)
    relay_start(qkv_block, i_qr)
    for d in ORDER:
        gather_forward(small_block, i_sz, i_sx, d)
    relay_x(qkv_block, i_qr)
    l_d = next(lids)
    down_block = lambda s: wdown.at[srow(s), :]
    i_dr = take(12)
    relay_x(down_block, i_dr, src=down_in)
    pltpu.make_async_copy(down_in, down_block(seq), lsem.at[l_d]).start()

    gather_finish(small_block, i_sx)
    for s in range(8):
        vec[:, s * 128 : (s + 1) * 128] = smb[s]

    length = length_ref[0]
    my = mul(ctx * R, R)

    def valid_rows(r0, n):
        pos = lax.broadcasted_iota(jnp.int32, (n, 1), 0) + (ctx * R + r0)
        return jnp.where(pos < length, 1.0, 0.0).astype(f32)

    CH = 2
    RC = R // CH

    def chunk(buf, c, ch):
        return buf.at[pl.ds(mul(c * R + ch * RC, RC), RC), :]

    def ag_start(buf, i, ch):
        own = chunk(buf, ctx, ch)
        rcopy(own, own, ypeer, i + CH + ch).start()
        rcopy(own, own, mate, i + ch).start()
        if buf is not gf and buf is not n2:
            sent(own, i + CH + ch)
            sent(own, i + ch)

    def ag_forward(buf, i, ch):
        b = chunk(buf, ((y + 1) % 2) * 2 + k, ch)
        rcopy(b, b, mate, i + CH + ch).wait_recv()
        rcopy(b, b, mate, i + 2 * CH + ch).start()
        if buf is not gf and buf is not n2:
            sent(buf.at[pl.ds(0, RC), :], i + 2 * CH + ch)

    def ag_wait(buf, i, which):
        for ch in range(CH):
            b = chunk(buf, ctx, ch)
            rcopy(b, b, mate, i + which * CH + ch).wait_recv()

    i_n1 = take(3 * CH)
    for ch in range(CH):
        def first(q, ch=ch):
            r0 = mul(ch * RC + q * 32, 32)
            zz, _ = layer_stats(tok[pl.ds(r0, 32), :].astype(f32))
            n1[pl.ds(mul(my + r0, 32), 32), :] = (zz * vec[0:1, :] + vec[1:2, :]).astype(bf16)

        loop(RC // 32, first)
        ag_start(n1, i_n1, ch)


    def mask_rows(q):
        r0 = mul(q * 32, 32)
        g = cot[pl.ds(r0, 32), :].astype(f32) * valid_rows(r0, 32)
        gf[pl.ds(mul(my + r0, 32), 32), :] = g.astype(bf16)

    loop(R // 32, mask_rows)
    i_gf = take(3 * CH)
    for ch in range(CH):
        ag_start(gf, i_gf, ch)
    for j in range(6):
        if j % 3 == 1:
            qbias[:, j * 128 : (j + 1) * 128] = jnp.zeros((8, 128), f32)
        else:
            r = 2 + j % 3 // 2
            b = vec[r : r + 1, pl.ds(mul((ctx + 4 * (j // 3)) * 128, 128), 128)]
            qbias[:, j * 128 : (j + 1) * 128] = jnp.broadcast_to(b, (8, 128))
    relay_step(qkv_block, i_qr, 1)
    relay_step(qkv_block, i_qr, 2)
    i_oz, i_ox = take(4), take(4)
    out_block = lambda zz: wout.at[pl.ds(mul((zz // 2) * 128, 128), 128), :]

    @pl.when(ctx == t)
    def _():
        wait_bytes(wout.at[pl.ds(0, 96), :], rsem.at[i_oa])
        wait_bytes(wout.at[pl.ds(0, 32), :], lsem.at[l_o])
        for d in (1, 2, 3):
            rcopy(out_block(z), out_block(z), zpeer(d), i_oz + d).start()
        rcopy(out_block(z), out_block(z), xpeer, i_ox).start()

    for d in (1, 2, 3):
        sent(out_block(z), i_oz + d, ctx == t)
    sent(out_block(z), i_ox, ctx == t)

    ag_forward(n1, i_n1, 0)
    relay_step(qkv_block, i_qr, 3)
    for d in (1, 2, 3):
        wait_bytes(wup.at[pl.ds(0, 32), :], rsem.at[i_ua + d])
    wait_bytes(wup.at[pl.ds(0, 32), :], lsem.at[l_u])
    up_block = lambda s: wup.at[srow(s), :]
    i_ur = take(12)
    relay_start(up_block, i_ur)
    ag_forward(n1, i_n1, 1)

    ag_wait(n1, i_n1, 0)
    relay_finish(qkv_block, i_qr)
    mine = x == k
    for d in (1, 2, 3):
        zz = (z - d + 4) % 4

        @pl.when(jnp.logical_and(mine, zz % 2 == y))
        def _(d=d, zz=zz):
            rcopy(out_block(zz), out_block(zz), xpeer, i_oz + d).wait_recv()
            rcopy(out_block(zz), out_block(zz), xpeer, i_ox + d).start()

        sent(out_block(zz), i_ox + d, jnp.logical_and(mine, zz % 2 == y))
    relay_x(up_block, i_ur)

    def project(it):
        blk = ((y + it // 2) % 2) * 2 + (k + it % 2) % 2

        @pl.when(it == 3)
        def _():
            ag_wait(n1, i_n1, 2)

        qkv[rows(blk), :] = (nn(n1[rows(blk), :], wqkv[...]) + qbias[0:1, :]).astype(bf16)

    loop(4, project)
    relay_step(up_block, i_ur, 1)
    relay_start(down_block, i_dr, src=down_in)

    def turn(i):
        c0 = pl.ds(mul(i * 128, 128), 128)
        vt[c0, :] = qkv[:, pl.ds(mul(i * 384 + 256, 128), 128)].T
        kt[c0, :] = qkv[:, pl.ds(mul(i * 384 + 128, 128), 128)].T

    loop(2, turn)

    lane = lax.broadcasted_iota(jnp.int32, (256, 128), 1)
    krow = lax.broadcasted_iota(jnp.int32, (256, 256), 0)
    qcol = lax.broadcasted_iota(jnp.int32, (256, 256), 1)

    def tri(kb, qb):
        return (qb * (qb + 1)) // 2 + kb

    def half(v, j):
        return jnp.where((lane // 64) == j, v, jnp.zeros_like(v))

    def pair_forward(i):
        for j in range(2):
            slope = jnp.exp2(jnp.full((1024, 128), -0.5, f32)
                             * (2 * ctx + 8 * i + j + 1).astype(f32)) * LOG2E
            b = slope * lax.broadcasted_iota(jnp.int32, (1024, 128), 0).astype(f32)
            for kb in range(4):
                own_b[j * 256 : (j + 1) * 256, kb * 128 : (kb + 1) * 128] = b[kb * 256 : (kb + 1) * 256]

        def queries(qb):
            q0 = pl.ds(mul(qb * 256, 256), 256)
            qblk = qkv[q0, pl.ds(mul(i * 384, 128), 128)]

            def scores(kb, best):
                k0 = pl.ds(mul(kb * 256, 256), 256)
                kblk = qkv[k0, pl.ds(mul(i * 384 + 128, 128), 128)]
                new = []
                for j in range(2):
                    b = own_b[j * 256 : (j + 1) * 256, pl.ds(mul(kb * 128, 128), 128)]
                    sc = nt(half(kblk, j), qblk) * (0.125 * LOG2E) + jnp.concatenate([b, b], axis=1)
                    sc = jnp.where(krow + kb * 256 <= qcol + qb * 256, sc, -1e30)
                    own_a[j * 256 : (j + 1) * 256, k0] = sc
                    new.append(jnp.maximum(best[j], jnp.max(sc.reshape(32, 8, 256), axis=0)))
                return tuple(new)

            low = jnp.full((8, 256), -3e38, f32)
            best = lax.fori_loop(0, qb + 1, scores, (low, low))
            top = [jnp.max(b, axis=0, keepdims=True) for b in best]

            def weigh(kb, carry):
                k0 = pl.ds(mul(kb * 256, 256), 256)
                new = []
                for j in range(2):
                    total, acc = carry[2 * j], carry[2 * j + 1]
                    p = jnp.exp2(own_a[j * 256 : (j + 1) * 256, k0] - top[j])
                    total = total + jnp.sum(p.reshape(32, 8, 256), axis=0)
                    p = p.astype(bf16)
                    ptri[2 * i + j, tri(kb, qb)] = p
                    v = vt[pl.ds(mul(i * 128 + j * 64, 64), 64), k0]
                    new += [total, acc + nn(v, p)]
                return tuple(new)

            zero = (jnp.zeros((8, 256), f32), jnp.zeros((64, 256), f32))
            out = lax.fori_loop(0, qb + 1, weigh, zero + zero)
            for j in range(2):
                inv = 1.0 / jnp.sum(out[2 * j], axis=0, keepdims=True)
                linv[2 * i + j, :, q0] = jnp.broadcast_to(inv, (8, 256))
                attt[pl.ds(mul(i * 128 + j * 64, 64), 64), q0] = (out[2 * j + 1] * inv).astype(bf16)

        loop(4, queries)

    pair_forward(0)
    for ch in range(CH):
        ag_forward(gf, i_gf, ch)
    pair_forward(1)

    relay_step(up_block, i_ur, 2)
    def rs_run(partial, sb, rb, own, i):
        def step(tt):
            g, ch, sub = tt // 4, tt % 2, (tt // 2) % 2
            blk = ((y + 1 - g) % 2) * 2 + (k + 1 - sub) % 2
            partial(blk, ch, tmp)

            @pl.when(jnp.logical_and(g == 0, sub == 0))
            def _():
                sb[0, ch] = tmp[...].astype(bf16)
                rcopy(sb.at[0, ch], rb.at[0, ch], mate, i + ch).start()

            @pl.when(jnp.logical_and(g == 0, sub == 1))
            def _():
                rcopy(sb.at[0, ch], rb.at[0, ch], mate, i + ch).wait_recv()
                sb[1, ch] = (tmp[...] + rb[0, ch].astype(f32)).astype(bf16)
                rcopy(sb.at[1, ch], rb.at[1, ch], ypeer, i + CH + ch).start()

            @pl.when(jnp.logical_and(g == 1, sub == 0))
            def _():
                sb[2, ch] = tmp[...].astype(bf16)
                rcopy(sb.at[2, ch], rb.at[2, ch], mate, i + 2 * CH + ch).start()

            @pl.when(jnp.logical_and(g == 1, sub == 1))
            def _():
                own[ch] = tmp[...]

        loop(4 * CH, step)

    def rs_wait(sb, rb, i, ch):
        rcopy(sb.at[2, ch], rb.at[2, ch], mate, i + 2 * CH + ch).wait_recv()
        rcopy(sb.at[1, ch], rb.at[1, ch], mate, i + CH + ch).wait_recv()

    def rs_sum(rb, own, ch, r):
        return own[ch, r, :] + rb[2, ch, r, :].astype(f32) + rb[1, ch, r, :].astype(f32)

    def rs_sent(sb, i):
        for j in range(3):
            for ch in range(CH):
                wait_bytes(sb.at[j, ch], ssem.at[i + j * CH + ch])

    for d in range(4):
        zz = (z - d + 4) % 4

        @pl.when(jnp.logical_and(x != k, zz % 2 == y))
        def _(d=d):
            rcopy(out_block(z), out_block(z), xpeer, i_ox + d).wait_recv()

    def branch_part(blk, ch, dst):
        a = attt[:, pl.ds(mul(blk * R + ch * RC, RC), RC)]
        dst[...] = tn(a, wout[...])

    i_br = take(3 * CH)
    rs_run(branch_part, rs_s, rs_r, rs_own, i_br)
    relay_step(up_block, i_ur, 3)
    relay_step(down_block, i_dr, 1)

    i_n2 = take(3 * CH)
    stat[...] = jnp.zeros_like(stat)
    for ch in range(CH):
        rs_wait(rs_s, rs_r, i_br, ch)

        def second(q, ch=ch):
            r = pl.ds(mul(q * 32, 32), 32)
            r1 = pl.ds(mul(ch * RC + q * 32, 32), 32)
            branch = rs_sum(rs_r, rs_own, ch, r) + vec[4:5, :]
            resid = tok[r1, :].astype(f32) + branch
            res[r1, :] = resid
            zz, _ = layer_stats(resid)
            n2[pl.ds(mul(my + ch * RC + q * 32, 32), 32), :] = (
                zz * vec[5:6, :] + vec[6:7, :]).astype(bf16)
            v = valid_rows(ch * RC + q * 32, 32)
            stat[0:8, :] += jnp.sum((branch * branch * v).reshape(4, 8, D), axis=0)
            stat[8:16, :] += jnp.sum((resid * resid * v).reshape(4, 8, D), axis=0)

        loop(RC // 32, second)
        ag_start(n2, i_n2, ch)

    relay_step(down_block, i_dr, 2)
    relay_finish(up_block, i_ur)

    def feed(it):
        blk = ((y + it // 2) % 2) * 2 + (k + it % 2) % 2

        @pl.when(it == 1)
        def _():
            ag_wait(n2, i_n2, 0)
            ag_forward(n2, i_n2, 0)
            relay_step(down_block, i_dr, 3)

        @pl.when(it == 2)
        def _():
            ag_forward(n2, i_n2, 1)

        @pl.when(it == 3)
        def _():
            ag_wait(n2, i_n2, 2)

        def cols(n):
            c0 = pl.ds(mul(n * 512, 512), 512)
            pre = nn(n2[rows(blk), :], wup[:, c0]) + vec[8:9, c0]
            sq = pre * pre
            th = jnp.tanh(0.7978845608028654 * pre * (1.0 + 0.044715 * sq))
            a1 = 0.5 * (1.0 + th)
            act[rows(blk), c0] = (pre * a1).astype(bf16)
            der = a1 + 0.5 * pre * (1.0 - th * th) * (
                0.7978845608028654 * (1.0 + 0.134145 * sq))
            gpre[rows(blk), c0] = der.astype(bf16)

        loop(2, cols)

    loop(4, feed)

    def dw_half(a, b, c0, n, xx, hh):
        c1 = pl.ds(mul((hh * 2 + xx) * 128, 128), 128)
        c2 = pl.ds(mul(((3 - hh) * 2 + xx) * 128, 128), 128)
        return tn(jnp.concatenate([a[:, c1], a[:, c2]], axis=1), b[:, c0 : c0 + n])

    def dw_away(a, b, c0, n, xb, xr, i):
        def away(hh):
            r = pl.ds(mul(hh * 256, 256), 256)
            xb[r, c0 : c0 + n] = dw_half(a, b, c0, n, (x + 1) % 2, hh).astype(bf16)
            rcopy(xb.at[r, pl.ds(c0, n)], xr.at[r, pl.ds(c0, n)], xpeer, i + hh).start()
            sent(xb.at[pl.ds(0, 256), pl.ds(c0, n)], i + hh)

        for hh in range(2):
            away(hh)

    def dw_keep(a, b, c0, n, own):
        def keep(hh):
            own[pl.ds(mul(hh * 256, 256), 256), c0 : c0 + n] = dw_half(a, b, c0, n, x, hh)

        loop(2, keep)

    def dw_z(hh, c0, n, xr, own, zb, zo, zr, fin, i, iz):
        wait_bytes(xr.at[pl.ds(0, 256), pl.ds(c0, n)], rsem.at[i + hh])
        c = slice(c0, c0 + n)
        for sub, zz in enumerate((hh, 3 - hh)):
            r = slice(hh * 256 + sub * 128, hh * 256 + sub * 128 + 128)
            ro = slice(zo + zz * 128, zo + zz * 128 + 128)
            dz = (zz - z + 4) % 4

            @pl.when(zz == z)
            def _(r=r):
                fin[:, c] = own[r, c] + xr[r, c].astype(f32)

            @pl.when(zz != z)
            def _(r=r, ro=ro, zz=zz, dz=dz):
                zb[ro, c] = (own[r, c] + xr[r, c].astype(f32)).astype(bf16)
                rcopy(zb.at[ro, c], zr.at[dz - 1, :, c], {"seq": zz * 2 + x}, iz + dz).start()

            sent(zb.at[ro, c], iz + dz, zz != z)

    def dw_end(c0, n, zr, fin, iz):
        c = slice(c0, c0 + n)
        for d in (1, 2, 3):
            wait_bytes(zr.at[d - 1, :, c], rsem.at[iz + d])
        fin[:, c] += (zr[0, :, c].astype(f32) + zr[1, :, c].astype(f32)) + zr[2, :, c].astype(f32)

    ag_wait(gf, i_gf, 0)
    ag_wait(gf, i_gf, 2)
    i_dwx, i_dwz = take(2), take(4)
    dw_away(act, gf, 0, D, xs_down, xr_down, i_dwx)
    dw_keep(act, gf, 0, D, own_a)
    relay_finish(down_block, i_dr)
    wait_bytes(down_in, lsem.at[l_d])
    gvec[...] = jnp.zeros_like(gvec)

    def grad_feed(it):
        r = pl.ds(mul(it * R, R), R)

        def cols(n):
            c0 = pl.ds(mul(n * 512, 512), 512)
            ga = nt(gf[r, :], wdown[c0, :])
            g = (ga * gpre[r, c0].astype(f32)).astype(bf16)
            gpre[r, c0] = g
            gvec[2, :, c0] += jnp.sum(g.astype(f32).reshape(R // 8, 8, 512), axis=0)

        loop(2, cols)

    loop(4, grad_feed)

    rs_sent(rs_s, i_br)

    def gn2_part(blk, ch, dst):
        dst[...] = nt(gpre[pl.ds(mul(blk * R + ch * RC, RC), RC), :], wup[...])

    i_g2 = take(3 * CH)
    rs_run(gn2_part, rs_s, rs_r, rs_own, i_g2)

    def down_z(hh):
        dw_z(hh, 0, D, xr_down, own_a, gpre, 0, zr_down, fin_down, i_dwx, i_dwz)

    def up_z(hh):
        dw_z(hh, 0, D, xr_up, own_b, gpre, 512, zr_up, fin_up, i_uwx, i_uwz)

    i_uwx, i_uwz = take(2), take(4)
    dw_away(n2, gpre, 0, D, xs_up, xr_up, i_uwx)
    dw_keep(n2, gpre, 0, D, own_b)
    down_z(0)

    i_gb = take(3 * CH)
    for ch in range(CH):
        rs_wait(rs_s, rs_r, i_g2, ch)

        def third(q, ch=ch):
            r = pl.ds(mul(q * 32, 32), 32)
            r1 = pl.ds(mul(ch * RC + q * 32, 32), 32)
            g2 = rs_sum(rs_r, rs_own, ch, r)
            zz, rstd = layer_stats(res[r1, :])
            gout = cot[r1, :].astype(f32) * valid_rows(ch * RC + q * 32, 32)
            gres = gout + layer_back(g2, vec[5:6, :], zz, rstd)
            st_grad[r1, :] = gres
            low = gres.astype(bf16)
            gb[pl.ds(mul(my + ch * RC + q * 32, 32), 32), :] = low
            fold = lambda v: jnp.sum(v.reshape(4, 8, D), axis=0)
            gvec[4] += fold(low.astype(f32))
            gvec[5] += fold(g2 * zz)
            gvec[6] += fold(g2)
            gvec[7] += fold(gout)

        loop(RC // 32, third)
        ag_start(gb, i_gb, ch)

    down_z(1)
    ag_forward(gb, i_gb, 0)

    def ffn_part(blk, ch, dst):
        dst[...] = nn(act[pl.ds(mul(blk * R + ch * RC, RC), RC), :], wdown[...])

    i_ff = take(3 * CH)
    rs_run(ffn_part, rt_s, rt_r, rt_own, i_ff)
    ag_forward(gb, i_gb, 1)

    ag_wait(gb, i_gb, 0)
    ag_wait(gb, i_gb, 2)

    def att_grad(i):
        c0 = pl.ds(mul(i * 256, 256), 256)
        dot_[:, c0] = nt(wout[...], gb[c0, :]).astype(bf16)

    loop(4, att_grad)
    own_out[...] = nn(attt[...], gb[...])
    i_owx, i_owz = take(), take(4)
    for j in range(3 * CH):
        wait_bytes(gf.at[pl.ds(0, RC), :], ssem.at[i_gf + j])
        wait_bytes(n2.at[pl.ds(0, RC), :], ssem.at[i_n2 + j])
    xs_out = gf.at[pl.ds(512, 256), :]

    @pl.when(x != k)
    def _():
        gf[512:768, :] = own_out[...].astype(bf16)
        rcopy(xs_out, xr_out, xpeer, i_owx).start()

    sent(xs_out, i_owx, x != k)

    lane2 = lax.broadcasted_iota(jnp.int32, (1024, 128), 1)

    def pair_backward(i):
        p0 = pl.ds(mul(i * 128, 128), 128)
        for j in range(2):
            r0 = pl.ds(mul(i * 128 + j * 64, 64), 64)
            li = linv[2 * i + j, 0:1, :]
            dd = dot_[r0, :].astype(f32) * li
            delta = jnp.sum(dd * attt[r0, :].astype(f32), axis=0, keepdims=True)
            linv[2 * i + j, :, :] = jnp.broadcast_to(delta, (8, 1024))
            dot_[r0, :] = dd.astype(bf16)
        do_[...] = dot_[p0, :].T
        acck[...] = jnp.zeros_like(acck)
        accv[...] = jnp.zeros_like(accv)

        def queries(qb):
            q0 = pl.ds(mul(qb * 256, 256), 256)
            qblk = qkv[q0, pl.ds(mul(i * 384, 128), 128)]
            doblk = do_[q0, :]
            dt = dot_[p0, q0]

            def keys(kb, carry):
                k0 = pl.ds(mul(kb * 256, 256), 256)
                vblk = qkv[k0, pl.ds(mul(i * 384 + 256, 128), 128)]
                new = []
                for j in range(2):
                    p = ptri[2 * i + j, tri(kb, qb)]
                    dp = nn(half(vblk, j), dt) - linv[2 * i + j, 0:1, q0]
                    ds = (p.astype(f32) * dp).astype(bf16)
                    accv[j, k0, :] += nn(p, doblk)
                    acck[j, k0, :] += nn(ds, qblk)
                    kk = kt[pl.ds(mul(i * 128 + j * 64, 64), 64), k0]
                    new.append(carry[j] + nn(kk, ds))
                return tuple(new)

            zero = jnp.zeros((64, 256), f32)
            dq = lax.fori_loop(0, qb + 1, keys, (zero, zero))
            dq = jnp.concatenate(dq, axis=0) * 0.125
            dmix[q0, pl.ds(mul(i * 384, 128), 128)] = dq.T.astype(bf16)

        loop(4, queries)
        dk = jnp.where(lane2 < 64, acck[0], acck[1]) * 0.125
        dv = jnp.where(lane2 < 64, accv[0], accv[1])
        dmix[:, pl.ds(mul(i * 384 + 128, 128), 128)] = dk.astype(bf16)
        dmix[:, pl.ds(mul(i * 384 + 256, 128), 128)] = dv.astype(bf16)

    up_z(0)
    pair_backward(0)
    i_qwx, i_qwz = (take(2), take(2)), (take(4), take(4))
    dw_away(n1, dmix, 0, 384, gf, xr_qkv, i_qwx[0])
    pair_backward(1)

    rs_sent(rs_s, i_g2)

    def gn1_part(blk, ch, dst):
        dst[...] = nt(dmix[pl.ds(mul(blk * R + ch * RC, RC), RC), :], wqkv[...])

    i_g1 = take(3 * CH)
    up_z(1)
    rs_run(gn1_part, rs_s, rs_r, rs_own, i_g1)
    dw_away(n1, dmix, 384, 384, gf, xr_qkv, i_qwx[1])
    dw_keep(n1, dmix, 0, 768, own_a)

    def qkv_z(h):
        for hh in range(2):
            dw_z(hh, h * 384, 384, xr_qkv, own_a, n2, 0, zr_qkv, fin_qkv, i_qwx[h], i_qwz[h])

    for i in range(2):
        zi = y + 2 * i
        dz = (zi - z + 4) % 4

        @pl.when(x == k)
        def _(i=i, zi=zi, dz=dz):
            if i == 0:
                wait_bytes(xr_out, rsem.at[i_owx])
            half_rows = slice(i * 128, (i + 1) * 128)
            total = own_out[half_rows, :] + xr_out[half_rows, :].astype(f32)

            @pl.when(zi == z)
            def _():
                fin_out[...] = total

            @pl.when(zi != z)
            def _():
                n2[512 + i * 128 : 640 + i * 128, :] = total.astype(bf16)
                rcopy(n2.at[pl.ds(512 + i * 128, 128), :], zr_out.at[dz - 1], {"seq": zi * 2 + x}, i_owz + dz).start()

        sent(n2.at[pl.ds(512, 128), :], i_owz + dz, jnp.logical_and(x == k, zi != z))

    qkv_z(0)
    for ch in range(CH):
        rs_wait(rs_s, rs_r, i_g1, ch)

        def fourth(q, ch=ch):
            r = pl.ds(mul(q * 32, 32), 32)
            r1 = pl.ds(mul(ch * RC + q * 32, 32), 32)
            g1 = rs_sum(rs_r, rs_own, ch, r)
            zz, rstd = layer_stats(tok[r1, :].astype(f32))
            st_grad[r1, :] += layer_back(g1, vec[0:1, :], zz, rstd)
            fold = lambda v: jnp.sum(v.reshape(4, 8, D), axis=0)
            gvec[0] += fold(g1 * zz)
            gvec[1] += fold(g1)

        loop(RC // 32, fourth)
    l_g = next(lids)
    pltpu.make_async_copy(st_grad, o_grad, lsem.at[l_g]).start()

    gmat[...] = jnp.zeros_like(gmat)
    for r, v in ((0, 0), (1, 1), (4, 4), (5, 5), (6, 6), (7, 7), (8, 2)):
        gmat[r : r + 1, :] = jnp.sum(gvec[v], axis=0, keepdims=True)
    for r, p in ((2, 0), (3, 256)):
        for i in range(2):
            v = dmix[:, i * 384 + p : i * 384 + p + 128].astype(f32)
            v = jnp.sum(jnp.sum(v.reshape(128, 8, 128), axis=0), axis=0, keepdims=True)
            gmat[r : r + 1, pl.ds(mul((ctx + 4 * i) * 128, 128), 128)] = v
    for s in range(8):
        sg[s] = gmat[:, s * 128 : (s + 1) * 128]
    i_sgx, i_sgz, i_sgc = take(4), take(4), take(4)
    for j in range(4):
        src = sg.at[j * 2 + (x + 1) % 2]
        rcopy(src, sgx.at[j], xpeer, i_sgx + j).start()
        sent(src, i_sgx + j)

    qkv_z(1)
    for j in range(4):
        rcopy(sg.at[j], sgx.at[j], xpeer, i_sgx + j).wait_recv()
    for d in (1, 2, 3):
        zz = (z + d) % 4
        sgs[d - 1] = sg[zz * 2 + x] + sgx[zz]
        rcopy(sgs.at[d - 1], sgz.at[d - 1], zpeer(d), i_sgz + d).start()
        sent(sgs.at[d - 1], i_sgz + d)

    dw_end(0, D, zr_down, fin_down, i_dwz)
    l_dd = next(lids)
    pltpu.make_async_copy(fin_down, o_ddown, lsem.at[l_dd]).start()
    dw_end(0, D, zr_up, fin_up, i_uwz)
    i_uf, i_qf, i_of = take(4), (take(4), take(4)), take(4)

    def up_piece(fin, c, s):
        return (fin.at[pl.ds(mul(c * 32, 32), 32), pl.ds(s * 128, 128)],
                o_dup.at[:, pl.ds(mul((s * 4 + ctx) * 128, 128), 128)])

    for d in (1, 2, 3):
        for s in range(8):
            a, b = up_piece(fin_up, (ctx + d) % 4, s)
            rcopy(a, b, cpeer(d), i_uf + d).start()
        sent(fin_up.at[pl.ds(0, 32), :], i_uf + d)
    mine32 = pl.ds(mul(ctx * 32, 32), 32)
    l_up = next(lids)
    for s in range(8):
        a, b = up_piece(fin_up, ctx, s)
        pltpu.make_async_copy(a, b, lsem.at[l_up]).start()

    l_do = next(lids)

    @pl.when(ctx == t)
    def _():
        for d in (1, 2, 3):
            wait_bytes(zr_out.at[d - 1], rsem.at[i_owz + d])
        fin_out[...] += (zr_out[0].astype(f32) + zr_out[1].astype(f32)) + zr_out[2].astype(f32)
        for d in (1, 2, 3):
            src = fin_out.at[pl.ds(mul(((ctx + d) % 4) * 32, 32), 32), :]
            rcopy(src, o_dout, cpeer(d), i_of + d).start()
        pltpu.make_async_copy(fin_out.at[mine32, :], o_dout, lsem.at[l_do]).start()

    for d in (1, 2, 3):
        sent(fin_out.at[pl.ds(0, 32), :], i_of + d, ctx == t)

    for ch in range(CH):
        rs_wait(rt_s, rt_r, i_ff, ch)

        def last(q, ch=ch):
            r = pl.ds(mul(q * 32, 32), 32)
            r1 = pl.ds(mul(ch * RC + q * 32, 32), 32)
            ffn = rs_sum(rt_r, rt_own, ch, r) + vec[7:8, :]
            v = valid_rows(ch * RC + q * 32, 32)
            st_out[r1, :] = (v * (res[r1, :] + ffn)).astype(bf16)
            stat[16:24, :] += jnp.sum((ffn * ffn * v).reshape(4, 8, D), axis=0)

        loop(RC // 32, last)
    l_t = next(lids)
    pltpu.make_async_copy(st_out, o_out, lsem.at[l_t]).start()

    for d in (1, 2, 3):
        wait_bytes(sgz.at[d - 1], rsem.at[i_sgz + d])
    sgf[...] = sg[seq] + sgx[z] + (sgz[0] + sgz[1] + sgz[2])
    for j in range(3):
        v = jnp.sum(stat[j * 8 : (j + 1) * 8, :], axis=0, keepdims=True)
        sgf[9 + j : 10 + j, :] = jnp.broadcast_to(jnp.sum(v, axis=1, keepdims=True), (1, 128))
    for d in (1, 2, 3):
        rcopy(sgf, sgc.at[d], cpeer(d), i_sgc + d).start()
        sent(sgf, i_sgc + d)

    l_dq = []
    for h in range(2):
        dw_end(h * 384, 384, zr_qkv, fin_qkv, i_qwz[h])
        pieces = list(qkv_pieces(ctx))[3 * h : 3 * h + 3]
        for d in (1, 2, 3):
            c2 = (ctx + d) % 4
            for a, b in pieces:
                rcopy(fin_qkv.at[pl.ds(mul(c2 * 32, 32), 32), b], o_dqkv.at[:, a], cpeer(d), i_qf[h] + d).start()
            sent(fin_qkv.at[pl.ds(0, 32), pl.ds(0, 384)], i_qf[h] + d)
        l_dq.append(next(lids))
        for a, b in pieces:
            pltpu.make_async_copy(fin_qkv.at[mine32, b], o_dqkv.at[:, a], lsem.at[l_dq[h]]).start()

    for d in (1, 2, 3):
        wait_bytes(sgc.at[d], rsem.at[i_sgc + d])
    o_small[...] = sgf[...] + jnp.where(rowid != 8, sgc[1] + sgc[2] + sgc[3], 0.0)

    @pl.when(ctx != t)
    def _():
        wait_bytes(fin_out.at[pl.ds(0, 32), :], rsem.at[i_of + (ctx - t + 4) % 4])

    @pl.when(ctx == t)
    def _():
        wait_bytes(fin_out.at[pl.ds(0, 32), :], lsem.at[l_do])

    for d in (1, 2, 3):
        wait_bytes(fin_up.at[pl.ds(0, 32), :], rsem.at[i_uf + d])
        for h in range(2):
            wait_bytes(fin_qkv.at[pl.ds(0, 32), pl.ds(0, 384)], rsem.at[i_qf[h] + d])
    rs_sent(rs_s, i_g1)
    rs_sent(rt_s, i_ff)
    for block, i in ((qkv_block, i_qr), (up_block, i_ur), (down_block, i_dr)):
        relay_sent(block, i)
    flush()
    for ref, i in ((st_grad, l_g), (st_out, l_t), (fin_down, l_dd), (fin_up.at[pl.ds(0, 32), :], l_up),
                   (fin_qkv.at[pl.ds(0, 32), pl.ds(0, 384)], l_dq[0]),
                   (fin_qkv.at[pl.ds(0, 32), pl.ds(0, 384)], l_dq[1])):
        wait_bytes(ref, lsem.at[i])
    assert next(ids) <= NSEM, next(ids)


def finish_kernel(length_ref, sums, *refs):
    big, outs, vecs = refs[:6], refs[6:12], refs[12:20]
    o_ub, o_stats = refs[20:22]
    stage, s_in, s_out = refs[22:28], refs[28], refs[29]
    for i in range(6):
        pltpu.make_async_copy(big[i], stage[i], s_in.at[i]).start()
    ctx = lax.axis_index("ctx")
    mine = sums[0:8, 0:32]
    for c in range(1, 4):
        mine = jnp.where(ctx == c, sums[0:8, c * 32 : (c + 1) * 32], mine)
    for r in range(8):
        vecs[r][...] = mine[r, :]
    o_ub[...] = sums[8, :]
    lane = lax.broadcasted_iota(jnp.int32, (1, 128), 1)
    v = jnp.where(lane == 0, sums[9:10, :], jnp.where(lane == 1, sums[10:11, :], sums[11:12, :]))
    o_stats[...] = jnp.sqrt(v / (length_ref[0].astype(f32) * D))[:, 0:3]
    for i in range(6):
        pltpu.make_async_copy(big[i], stage[i], s_in.at[i]).wait()
        pltpu.make_async_copy(stage[i], outs[i], s_out.at[i]).start()
    for i in range(6):
        pltpu.make_async_copy(stage[i], outs[i], s_out.at[i]).wait()


def fast(mesh):
    def scratch():
        v = lambda dt, *shape: pltpu.VMEM(shape, dt)
        return [
            v(bf16, D, 768), v(bf16, 256, D), v(bf16, D, D), v(bf16, D, D),
            v(f32, 4, 16, 128), v(f32, 8, 16, 128), v(f32, 16, D),
            v(bf16, S, D), v(bf16, S, D), v(bf16, S, D), v(bf16, S, D), v(bf16, S, D), v(bf16, S, D),
            v(bf16, S, 768), v(bf16, 256, S), v(bf16, 256, S), v(bf16, 256, S),
            v(bf16, 256, S), v(bf16, S, 128), v(bf16, S, 768), v(f32, 4, 8, S),
            v(bf16, 4, 10, 256, 256), v(f32, 2, S, 128), v(f32, 2, S, 128),
            v(bf16, 3, 2, 128, D), v(bf16, 3, 2, 128, D), v(f32, 2, 128, D),
            v(bf16, 3, 2, 128, D), v(bf16, 3, 2, 128, D), v(f32, 2, 128, D),
            v(f32, 128, D), v(f32, R, D),
            v(bf16, 512, D), v(bf16, 512, D), v(bf16, 512, D), v(bf16, 512, D), v(bf16, 512, 768), v(bf16, 256, D),
            v(f32, 512, D), v(f32, 512, D), v(f32, 256, D),
            v(bf16, 3, 128, D), v(bf16, 3, 128, D), v(bf16, 3, 128, 768), v(bf16, 3, 128, D),
            v(f32, 128, D), v(f32, 128, 768), v(f32, 128, D),
            v(bf16, R, D), v(f32, R, D), v(f32, 128, D),
            v(f32, 8, 16, 128), v(f32, 4, 16, 128), v(f32, 3, 16, 128), v(f32, 3, 16, 128),
            v(f32, 16, 128), v(f32, 4, 16, 128), v(f32, 8, 8, D), v(f32, 16, D), v(f32, 24, D), v(f32, 8, 768),
            pltpu.SemaphoreType.DMA((16,)),
            pltpu.SemaphoreType.DMA((NSEM,)),
            pltpu.SemaphoreType.DMA((NSEM,)),
        ]

    def on_device(tokens, lengths, cotangent, g1, b1, wq, qb, vb, wo, ob, g2, b2, wu, ub, wd, db):
        ctx = lax.axis_index("ctx")
        vectors = jnp.stack([g1, b1, qb, vb, ob, g2, b2, db]).astype(f32)
        place = (jnp.arange(128) // 32) == ctx
        small = jnp.concatenate([
            jnp.where(place[None], jnp.tile(vectors, (1, 4)), 0.0),
            ub.astype(f32)[None], jnp.zeros((7, 128), f32)])
        vm = pl.BlockSpec(memory_space=pltpu.VMEM)
        sds = jax.ShapeDtypeStruct
        out, grad, dqkv, dout, dup, ddown, sums = pl.pallas_call(
            block_kernel,
            out_shape=(sds((R, D), bf16), sds((R, D), f32), sds((32, 3 * D), f32), sds((32, D), f32),
                       sds((32, 4 * D), f32), sds((128, D), f32), sds((16, 128), f32)),
            in_specs=[pl.BlockSpec(memory_space=pltpu.SMEM)] + [vm] * 7,
            out_specs=tuple([pl.BlockSpec(memory_space=pl.ANY)] * 6 + [vm]),
            scratch_shapes=scratch(),
            compiler_params=pltpu.CompilerParams(
                collective_id=0, has_side_effects=True, vmem_limit_bytes=LIMIT),
            name="block",
        )(lengths, tokens[0], cotangent[0], small, wq, wo, wu, wd)
        anyspec = pl.BlockSpec(memory_space=pl.ANY)
        big = (out, grad, dqkv, dout, dup, ddown)
        res = pl.pallas_call(
            finish_kernel,
            out_shape=tuple(sds(v.shape, v.dtype) for v in big)
            + tuple([sds((32,), f32)] * 8) + (sds((128,), f32), sds((1, 3), f32)),
            in_specs=[pl.BlockSpec(memory_space=pltpu.SMEM), vm] + [anyspec] * 6,
            out_specs=tuple([anyspec] * 6 + [vm] * 10),
            scratch_shapes=[pltpu.VMEM(v.shape, v.dtype) for v in big]
            + [pltpu.SemaphoreType.DMA((6,)), pltpu.SemaphoreType.DMA((6,))],
            compiler_params=pltpu.CompilerParams(vmem_limit_bytes=LIMIT),
            name="finish",
        )(lengths, sums, *big)
        out, grad, dqkv, dout, dup, ddown, g1, b1, qb, vb, ob, g2, b2, db, ub, stats = res
        return (out[None], grad[None], g1, b1, dqkv, qb, vb, dout, ob, g2, b2, dup, ub, ddown, db, stats)

    return on_device


HEADS = 16


epsilon = 1e-05


def normalize(inputs, gain, shift):
    average = jnp.mean(inputs, axis=-1, keepdims=True)
    centred = inputs - average
    variance = jnp.mean(centred * centred, axis=-1, keepdims=True)
    return centred * lax.rsqrt(variance + epsilon) * gain + shift


def gelu_tanh(inputs):
    return jax.nn.gelu(inputs, approximate=True)


def inner_rows(left, right):
    return lax.dot_general(
        left, right, (((0,), (0,)), ((), ())), preferred_element_type=jnp.float32
    )


def outer_cols(left, right):
    return lax.dot_general(
        left, right, (((1,), (1,)), ((), ())), preferred_element_type=jnp.float32
    )


def alibi_scores(query_block, key_block, query_pos, key_pos, slope_block):
    raw = jnp.einsum("qhd,khd->hqk", query_block, key_block, preferred_element_type=jnp.float32)
    offset = (key_pos[None, :] - query_pos[:, None]).astype(jnp.float32)
    scores = raw * query_block.shape[-1] ** (-0.5) + slope_block[:, None, None] * offset[None]
    allowed = key_pos[None, :] <= query_pos[:, None]
    return (scores, allowed)


def score_grads(
    query_block,
    key_block,
    value_block,
    grad_block,
    query_pos,
    key_pos,
    slope_block,
    log_block,
    delta_block,
):
    scores, allowed = alibi_scores(query_block, key_block, query_pos, key_pos, slope_block)
    probs = jnp.where(allowed[None], jnp.exp(scores - log_block[..., None]), 0.0)
    grad_probs = jnp.einsum(
        "qhd,khd->hqk", grad_block, value_block, preferred_element_type=jnp.float32
    )
    delta_block = jnp.sum(probs * grad_probs, axis=-1)
    grad_scores = (probs * (grad_probs - delta_block[..., None])).astype(jnp.bfloat16)
    return (probs, grad_scores, delta_block)


def on_device(
    tokens,
    lengths,
    cotangent,
    ln1_gain,
    ln1_bias,
    qkv_weight,
    query_bias,
    value_bias,
    out_weight,
    out_bias,
    ln2_gain,
    ln2_bias,
    up_weight,
    up_bias,
    down_weight,
    down_bias,
):
    shards = (
        ln1_gain,
        ln1_bias,
        qkv_weight,
        query_bias,
        value_bias,
        out_weight,
        out_bias,
        ln2_gain,
        ln2_bias,
        up_weight,
        up_bias,
        down_weight,
        down_bias,
    )
    row_count = tokens.shape[1]
    model_width = tokens.shape[2]
    head_count = HEADS
    head_width = model_width // head_count
    per_block = 2
    block_count = head_count // per_block
    slot_rows = row_count * lax.axis_size("ctx")
    positions = lax.axis_index("ctx") * row_count + jnp.arange(row_count, dtype=jnp.int32)
    length = lengths[0]
    valid_rows = (positions < length).astype(jnp.float32)[:, None]
    slopes = jnp.exp2(-8.0 * (jnp.arange(head_count, dtype=jnp.float32) + 1.0) / head_count)
    key_positions = jnp.arange(slot_rows, dtype=jnp.int32)
    scale = head_width ** (-0.5)
    full_weights = (
        lax.all_gather(shards[0], ("seq", "ctx"), axis=0, tiled=True),
        lax.all_gather(shards[1], ("seq", "ctx"), axis=0, tiled=True),
        lax.all_gather(shards[2], ("seq", "ctx"), axis=0, tiled=True),
        lax.all_gather(shards[3], ("seq", "ctx"), axis=0, tiled=True),
        lax.all_gather(shards[4], ("seq", "ctx"), axis=0, tiled=True),
        lax.all_gather(shards[5], ("seq", "ctx"), axis=0, tiled=True),
        lax.all_gather(shards[6], ("seq", "ctx"), axis=0, tiled=True),
        lax.all_gather(shards[7], ("seq", "ctx"), axis=0, tiled=True),
        lax.all_gather(shards[8], ("seq", "ctx"), axis=0, tiled=True),
        lax.all_gather(shards[9], ("seq", "ctx"), axis=0, tiled=True),
        lax.all_gather(shards[10], ("seq", "ctx"), axis=0, tiled=True),
        lax.all_gather(shards[11], ("seq", "ctx"), axis=0, tiled=True),
        lax.all_gather(shards[12], ("seq", "ctx"), axis=0, tiled=True),
    )
    (
        gain_one,
        shift_one,
        w_qkv,
        bias_query,
        bias_value,
        w_out,
        bias_out,
        gain_two,
        shift_two,
        w_up,
        bias_up,
        w_down,
        bias_down,
    ) = full_weights

    def pick(array, index):
        return lax.dynamic_slice_in_dim(array, index * per_block, per_block, 1)

    def pick_slopes(index):
        return lax.dynamic_slice_in_dim(slopes, index * per_block, per_block, 0)

    def to_blocks(array):
        return array.transpose(1, 0, 2, 3).reshape(array.shape[1], model_width)

    source = tokens[0].astype(jnp.float32)
    normed_one, back_one = jax.vjp(normalize, source, gain_one, shift_one)
    normed_low = normed_one.astype(jnp.bfloat16)
    mixed = jnp.dot(normed_low, w_qkv, preferred_element_type=jnp.float32)
    query = (mixed[:, :model_width] + bias_query).astype(jnp.bfloat16)
    keys = mixed[:, model_width : 2 * model_width].astype(jnp.bfloat16)
    values = (mixed[:, 2 * model_width :] + bias_value).astype(jnp.bfloat16)
    all_keys, all_values = (
        lax.all_gather(keys, "ctx", axis=0, tiled=True),
        lax.all_gather(values, "ctx", axis=0, tiled=True),
    )
    query_heads = query.reshape(row_count, head_count, head_width)
    key_heads = all_keys.reshape(slot_rows, head_count, head_width)
    value_heads = all_values.reshape(slot_rows, head_count, head_width)

    def forward_block(index):
        scores, allowed = alibi_scores(
            pick(query_heads, index),
            pick(key_heads, index),
            positions,
            key_positions,
            pick_slopes(index),
        )
        masked = jnp.where(allowed[None], scores, -1e30)
        highest = jnp.max(masked, axis=-1)
        total = jnp.sum(jnp.exp(masked - highest[..., None]), axis=-1)
        log_total = highest + jnp.log(total)
        probs = jnp.where(allowed[None], jnp.exp(scores - log_total[..., None]), 0.0)
        block_out = jnp.einsum(
            "hqk,khd->qhd",
            probs.astype(jnp.bfloat16),
            pick(value_heads, index),
            preferred_element_type=jnp.float32,
        )
        return (block_out, log_total)

    head_out, log_totals = lax.map(forward_block, jnp.arange(block_count))
    attended = to_blocks(head_out).astype(jnp.bfloat16)
    branch = jnp.dot(attended, w_out, preferred_element_type=jnp.float32) + bias_out
    resid = source + branch
    normed_two, back_two = jax.vjp(normalize, resid, gain_two, shift_two)
    normed_two_low = normed_two.astype(jnp.bfloat16)
    pre_act = jnp.dot(normed_two_low, w_up, preferred_element_type=jnp.float32) + bias_up
    activated, back_act = jax.vjp(gelu_tanh, pre_act)
    activated_low = activated.astype(jnp.bfloat16)
    ffn = jnp.dot(activated_low, w_down, preferred_element_type=jnp.float32) + bias_down
    output = (valid_rows * (resid + ffn)).astype(jnp.bfloat16)[None]
    squares = jnp.stack(
        [
            jnp.sum(valid_rows * branch * branch),
            jnp.sum(valid_rows * resid * resid),
            jnp.sum(valid_rows * ffn * ffn),
        ]
    )
    totals = lax.psum(squares, "ctx")
    stats = jnp.sqrt(totals / (length.astype(jnp.float32) * model_width))[None]
    w_qkv, w_out, w_up, w_down = (
        lax.all_gather(qkv_weight, ("seq", "ctx"), axis=0, tiled=True),
        lax.all_gather(out_weight, ("seq", "ctx"), axis=0, tiled=True),
        lax.all_gather(up_weight, ("seq", "ctx"), axis=0, tiled=True),
        lax.all_gather(down_weight, ("seq", "ctx"), axis=0, tiled=True),
    )
    grad_out = cotangent[0].astype(jnp.float32) * valid_rows
    grad_ffn = grad_out.astype(jnp.bfloat16)
    grad_down_w = inner_rows(activated_low, grad_ffn)
    grad_down_b = jnp.sum(grad_ffn.astype(jnp.float32), axis=0)
    grad_activated = outer_cols(grad_ffn, w_down)
    (grad_pre,) = back_act(grad_activated)
    grad_pre_low = grad_pre.astype(jnp.bfloat16)
    grad_up_w = inner_rows(normed_two_low, grad_pre_low)
    grad_up_b = jnp.sum(grad_pre_low.astype(jnp.float32), axis=0)
    grad_normed_two = outer_cols(grad_pre_low, w_up)
    grad_resid_norm, grad_gain_two, grad_shift_two = back_two(grad_normed_two)
    grad_resid = grad_out + grad_resid_norm
    grad_branch = grad_resid.astype(jnp.bfloat16)
    grad_out_w = inner_rows(attended, grad_branch)
    grad_out_b = jnp.sum(grad_branch.astype(jnp.float32), axis=0)
    grad_attended = outer_cols(grad_branch, w_out).astype(jnp.bfloat16)
    grad_heads = grad_attended.reshape(row_count, head_count, head_width)

    def backward_block(index):
        query_block = pick(query_heads, index)
        key_block = pick(key_heads, index)
        grad_block = pick(grad_heads, index)
        probs, grad_scores, delta_block = score_grads(
            query_block,
            key_block,
            pick(value_heads, index),
            grad_block,
            positions,
            key_positions,
            pick_slopes(index),
            log_totals[index],
            None,
        )
        grad_query_block = (
            jnp.einsum("hqk,khd->qhd", grad_scores, key_block, preferred_element_type=jnp.float32)
            * scale
        )
        grad_key_block = (
            jnp.einsum("hqk,qhd->khd", grad_scores, query_block, preferred_element_type=jnp.float32)
            * scale
        )
        grad_value_block = jnp.einsum(
            "hqk,qhd->khd",
            probs.astype(jnp.bfloat16),
            grad_block,
            preferred_element_type=jnp.float32,
        )
        return (grad_query_block, grad_key_block, grad_value_block)

    query_parts, key_parts, value_parts = lax.map(backward_block, jnp.arange(block_count))
    grad_query_all = to_blocks(query_parts)
    own_keys, own_values = (
        lax.psum_scatter(
            to_blocks(key_parts).astype(jnp.bfloat16), "ctx", scatter_dimension=0, tiled=True
        ).astype(jnp.float32),
        lax.psum_scatter(
            to_blocks(value_parts).astype(jnp.bfloat16), "ctx", scatter_dimension=0, tiled=True
        ).astype(jnp.float32),
    )
    grad_query_low = grad_query_all.astype(jnp.bfloat16)
    grad_key_low = own_keys.astype(jnp.bfloat16)
    grad_value_low = own_values.astype(jnp.bfloat16)
    grad_mixed = jnp.concatenate([grad_query_low, grad_key_low, grad_value_low], axis=1)
    grad_qkv_w = inner_rows(normed_low, grad_mixed)
    grad_query_bias = jnp.sum(grad_query_low.astype(jnp.float32), axis=0)
    grad_value_bias = jnp.sum(grad_value_low.astype(jnp.float32), axis=0)
    grad_normed_one = outer_cols(grad_mixed, w_qkv)
    grad_source_norm, grad_gain_one, grad_shift_one = back_one(grad_normed_one)
    grad_tokens = (grad_resid + grad_source_norm)[None]
    summed = (
        lax.psum_scatter(
            grad_gain_one.astype(jnp.float32), ("seq", "ctx"), scatter_dimension=0, tiled=True
        ),
        lax.psum_scatter(
            grad_shift_one.astype(jnp.float32), ("seq", "ctx"), scatter_dimension=0, tiled=True
        ),
        lax.psum_scatter(grad_qkv_w, ("seq", "ctx"), scatter_dimension=0, tiled=True),
        lax.psum_scatter(grad_query_bias, ("seq", "ctx"), scatter_dimension=0, tiled=True),
        lax.psum_scatter(grad_value_bias, ("seq", "ctx"), scatter_dimension=0, tiled=True),
        lax.psum_scatter(grad_out_w, ("seq", "ctx"), scatter_dimension=0, tiled=True),
        lax.psum_scatter(grad_out_b, ("seq", "ctx"), scatter_dimension=0, tiled=True),
        lax.psum_scatter(
            grad_gain_two.astype(jnp.float32), ("seq", "ctx"), scatter_dimension=0, tiled=True
        ),
        lax.psum_scatter(
            grad_shift_two.astype(jnp.float32), ("seq", "ctx"), scatter_dimension=0, tiled=True
        ),
        lax.psum_scatter(grad_up_w, ("seq", "ctx"), scatter_dimension=0, tiled=True),
        lax.psum_scatter(grad_up_b, ("seq", "ctx"), scatter_dimension=0, tiled=True),
        lax.psum_scatter(grad_down_w, ("seq", "ctx"), scatter_dimension=0, tiled=True),
        lax.psum_scatter(grad_down_b, ("seq", "ctx"), scatter_dimension=0, tiled=True),
    )
    return (output, grad_tokens) + tuple(summed) + (stats,)


def solution(mesh):
    small_slice = mesh.shape["seq"] == 8 and mesh.shape["ctx"] == 4
    placed = (
        P("seq", "ctx", None),
        P("seq"),
        P("seq", "ctx", None),
        P(("seq", "ctx")),
        P(("seq", "ctx")),
        P(("seq", "ctx"), None),
        P(("seq", "ctx")),
        P(("seq", "ctx")),
        P(("seq", "ctx"), None),
        P(("seq", "ctx")),
        P(("seq", "ctx")),
        P(("seq", "ctx")),
        P(("seq", "ctx"), None),
        P(("seq", "ctx")),
        P(("seq", "ctx"), None),
        P(("seq", "ctx")),
    )
    return jax.shard_map(
        fast(mesh) if small_slice else on_device,
        mesh=mesh,
        in_specs=placed,
        out_specs=(
            P("seq", "ctx", None),
            P("seq", "ctx", None),
            P(("seq", "ctx")),
            P(("seq", "ctx")),
            P(("seq", "ctx"), None),
            P(("seq", "ctx")),
            P(("seq", "ctx")),
            P(("seq", "ctx"), None),
            P(("seq", "ctx")),
            P(("seq", "ctx")),
            P(("seq", "ctx")),
            P(("seq", "ctx"), None),
            P(("seq", "ctx")),
            P(("seq", "ctx"), None),
            P(("seq", "ctx")),
            P("seq", None),
        ),
        check_vma=False,
    )
```

```python
import itertools

import jax
import jax.numpy as jnp
from jax import lax
from jax.experimental import pallas as pl
from jax.experimental.pallas import tpu as pltpu
from jax.sharding import PartitionSpec as P

MESH = pl.DeviceIdType.MESH
bf16, f32 = jnp.bfloat16, jnp.float32
LOG2E = 1.4426950408889634
D = 1024
R = 256
S = 1024
LIMIT = 66_000_000
NRECV, NSEND, NLOCAL = 103, 52, 11
ORDER = (2, 3, 1)


def nn(a, b):
    return lax.dot_general(a, b, (((1,), (0,)), ((), ())), preferred_element_type=f32)


def nt(a, b):
    return lax.dot_general(a, b, (((1,), (1,)), ((), ())), preferred_element_type=f32)


def tn(a, b):
    return lax.dot_general(a, b, (((0,), (0,)), ((), ())), preferred_element_type=f32)


def mul(v, m):
    return pl.multiple_of(v, m)


def loop(n, body, start=0):
    def step(i, carry):
        body(i)
        return carry

    lax.fori_loop(start, n, step, 0)


def layer_stats(v):
    mean = jnp.sum(v, axis=-1, keepdims=True) * (1.0 / D)
    cen = v - mean
    var = jnp.sum(cen * cen, axis=-1, keepdims=True) * (1.0 / D)
    rstd = lax.rsqrt(var + 1e-5)
    return cen * rstd, rstd


def layer_back(g2, gain, z, rstd):
    g = g2 * gain
    m1 = jnp.sum(g, axis=-1, keepdims=True) * (1.0 / D)
    m2 = jnp.sum(g * z, axis=-1, keepdims=True) * (1.0 / D)
    return rstd * (g - m1 - z * m2)


def block_kernel(
    length_ref, tok, cot, small, qkv_in, out_in, up_in, down_in,
    o_out, o_grad, o_dqkv, o_dout, o_dup, o_ddown, o_small,
    wqkv, wout, wup, wdown, smc, smb, vec,
    n1, n2, gf, gb, act, gpre, qkv, vt, kt, attt, dot_, do_, dmix, linv,
    ptri, acck, accv,
    rs_s, rs_r, rs_own, rt_s, rt_r, rt_own, tmp, res,
    xs_down, xs_up, xr_down, xr_up, xr_qkv, xr_out, own_a, own_b, own_out,
    zr_down, zr_up, zr_qkv, zr_out, fin_up, fin_qkv, fin_out,
    st_out, st_grad, fin_down, sg, sgx, sgs, sgz, sgf, sgc, gvec, gmat, stat, qbias,
    lsem, ssem, rsem,
):
    seq, ctx = lax.axis_index("seq"), lax.axis_index("ctx")
    z, x = seq // 2, seq % 2
    y, k = ctx // 2, ctx % 2
    rids, sids = itertools.count(), itertools.count()
    lids = itertools.count()

    mate = {"ctx": y * 2 + (k + 1) % 2}
    ypeer = {"ctx": ((y + 1) % 2) * 2 + k}
    xpeer = {"seq": z * 2 + (x + 1) % 2}

    def cpeer(d):
        return {"ctx": (ctx + d) % 4}

    def zpeer(d):
        return {"seq": ((z + d) % 4) * 2 + x}

    def take(count, n=1):
        first = next(count)
        for _ in range(n - 1):
            next(count)
        return first

    def rtake(n=1):
        return take(rids, n)

    def stake(n=1):
        return take(sids, n)

    def rcopy(src, dst, dev, i, s):
        return pltpu.make_async_remote_copy(
            src_ref=src, dst_ref=dst, send_sem=ssem.at[s], recv_sem=rsem.at[i],
            device_id=dev, device_id_type=MESH)

    def wait_bytes(ref, sem):
        pltpu.make_async_copy(ref, ref, sem).wait()

    sends = []

    def sent(ref, i, cond=None):
        sends.append((ref, i, cond))

    def flush():
        for ref, i, cond in sends:
            if cond is None:
                wait_bytes(ref, ssem.at[i])
            else:
                @pl.when(cond)
                def _(ref=ref, i=i):
                    wait_bytes(ref, ssem.at[i])
        sends.clear()

    rows = lambda c: pl.ds(mul(c * R, R), R)
    srow = lambda s: pl.ds(s * 128 if isinstance(s, int) else mul(s * 128, 128), 128)

    barrier = pltpu.get_barrier_semaphore()
    for d in (1, 2, 3):
        pl.semaphore_signal(barrier, inc=1, device_id=cpeer(d), device_id_type=MESH)
        pl.semaphore_signal(barrier, inc=1, device_id=zpeer(d), device_id_type=MESH)
    pl.semaphore_signal(barrier, inc=1, device_id=xpeer, device_id_type=MESH)
    pl.semaphore_wait(barrier, 7)

    i_smc, s_smc = rtake(), stake()
    for d in (1, 2, 3):
        rcopy(small, smc.at[d], cpeer(d), i_smc, s_smc).start()
    sent(smc.at[pl.ds(1, 3)], s_smc)
    own32 = pl.ds(mul(seq * 128 + ctx * 32, 32), 32)

    def qkv_pieces(c):
        for j in range(6):
            yield (pl.ds(mul((j % 3) * D + (c + 4 * (j // 3)) * 128, 128), 128),
                   pl.ds(j * 128, 128))

    i_qa, s_qa = rtake(), stake()
    for d in (1, 2, 3):
        for a, b in qkv_pieces((ctx + d) % 4):
            rcopy(qkv_in.at[:, a], wqkv.at[own32, b], cpeer(d), i_qa, s_qa).start()
    sent(wqkv.at[pl.ds(0, 96), :], s_qa)
    l_q = next(lids)
    for a, b in qkv_pieces(ctx):
        pltpu.make_async_copy(qkv_in.at[:, a], wqkv.at[own32, b], lsem.at[l_q]).start()

    t = seq % 4
    out32 = pl.ds(mul((seq // 4) * 128 + ctx * 32, 32), 32)
    i_oa, s_oa = rtake(), stake()
    l_o = next(lids)

    @pl.when(ctx != t)
    def _():
        rcopy(out_in, wout.at[out32, :], {"ctx": t}, i_oa, s_oa).start()

    sent(wout.at[pl.ds(0, 32), :], s_oa, ctx != t)

    @pl.when(ctx == t)
    def _():
        pltpu.make_async_copy(out_in, wout.at[out32, :], lsem.at[l_o]).start()

    i_ua, s_ua = rtake(), stake()
    for d in (1, 2, 3):
        c2 = (ctx + d) % 4
        for s in range(8):
            rcopy(up_in.at[:, pl.ds(mul((s * 4 + c2) * 128, 128), 128)],
                  wup.at[own32, pl.ds(s * 128, 128)], cpeer(d), i_ua, s_ua).start()
    sent(wup.at[pl.ds(0, 96), :], s_ua)
    l_u = next(lids)
    for s in range(8):
        pltpu.make_async_copy(up_in.at[:, pl.ds(mul((s * 4 + ctx) * 128, 128), 128)],
                              wup.at[own32, pl.ds(s * 128, 128)], lsem.at[l_u]).start()

    wait_bytes(smc.at[pl.ds(1, 3)], rsem.at[i_smc])
    rowid = lax.broadcasted_iota(jnp.int32, (16, 128), 0)
    smb[seq] = small[...] + jnp.where(rowid < 8, smc[1] + smc[2] + smc[3], 0.0)

    def relay_start(block, i, s, src=None):
        own = block(seq) if src is None else src
        for cond, step, first, sz in ((z < 3, 1, i, s), (z > 0, -1, i + 4, s + 1)):
            @pl.when(cond)
            def _(step=step, first=first, sz=sz):
                rcopy(own, block(seq), {"seq": (z + step) * 2 + x}, first + 1, sz).start()

    def relay_x(block, i, s, src=None):
        own = block(seq) if src is None else src
        rcopy(own, block(seq), xpeer, i, s + 2).start()

    def relay_step(block, i, s, j):
        for has, on, step, first, sz in ((z >= j, z < 3, 1, i, s), (z + j <= 3, z > 0, -1, i + 4, s + 1)):
            zz = z - j * step

            @pl.when(has)
            def _(on=on, step=step, first=first, zz=zz, sz=sz):
                b = block(zz * 2 + x)
                wait_bytes(b, rsem.at[first + j])
                if j < 3:
                    @pl.when(on)
                    def _():
                        rcopy(b, b, {"seq": (z + step) * 2 + x}, first + j + 1, sz).start()
                rcopy(b, b, xpeer, i, s + 2).start()

    def relay_finish(w, i):
        wait_bytes(w.at[pl.ds(0, 512), :], rsem.at[i])

    def relay_sent(w, s):
        for n in (1, 2, 3):
            sent(w.at[pl.ds(0, n * 128), :], s, z == n - 1)
            sent(w.at[pl.ds(0, n * 128), :], s + 1, z == 4 - n)
        sent(w.at[pl.ds(0, 512), :], s + 2)

    i_sz, i_sx, s_sz, s_sx = rtake(3), rtake(), stake(), stake()
    for d in ORDER:
        rcopy(smb.at[seq], smb.at[seq], zpeer(d), i_sz + d - 1, s_sz).start()
    rcopy(smb.at[seq], smb.at[seq], xpeer, i_sx, s_sx).start()
    sent(smb.at[pl.ds(0, 3)], s_sz)
    sent(smb.at[pl.ds(0, 4)], s_sx)

    wait_bytes(wqkv.at[pl.ds(0, 96), :], rsem.at[i_qa])
    wait_bytes(wqkv.at[pl.ds(0, 32), :], lsem.at[l_q])
    qkv_block = lambda s: wqkv.at[srow(s), :]
    i_qr, s_qr = rtake(8), stake(3)
    relay_start(qkv_block, i_qr, s_qr)
    relay_sent(wqkv, s_qr)
    for d in ORDER:
        b = smb.at[((z - d + 4) % 4) * 2 + x]
        wait_bytes(b, rsem.at[i_sz + d - 1])
        rcopy(b, b, xpeer, i_sx, s_sx).start()
    relay_x(qkv_block, i_qr, s_qr)
    l_d = next(lids)
    down_block = lambda s: wdown.at[srow(s), :]
    i_dr, s_dr = rtake(8), stake(3)
    relay_x(down_block, i_dr, s_dr, src=down_in)
    relay_sent(wdown, s_dr)
    pltpu.make_async_copy(down_in, down_block(seq), lsem.at[l_d]).start()

    wait_bytes(smb.at[pl.ds(0, 4)], rsem.at[i_sx])
    for s in range(8):
        vec[:, s * 128 : (s + 1) * 128] = smb[s]

    length = length_ref[0]
    my = mul(ctx * R, R)

    def valid_rows(r0, n):
        pos = lax.broadcasted_iota(jnp.int32, (n, 1), 0) + (ctx * R + r0)
        return jnp.where(pos < length, 1.0, 0.0).astype(f32)

    CH = 2
    RC = R // CH

    def chunk(buf, c, ch):
        return buf.at[pl.ds(mul(c * R + ch * RC, RC), RC), :]

    def ag_start(buf, i, s, ch):
        own = chunk(buf, ctx, ch)
        rcopy(own, own, ypeer, i + 1 + ch, s + ch).start()
        rcopy(own, own, mate, i, s + ch).start()

    def ag_forward(buf, i, s, ch):
        b = chunk(buf, ((y + 1) % 2) * 2 + k, ch)
        wait_bytes(b, rsem.at[i + 1 + ch])
        rcopy(b, b, mate, i + 3, s + ch).start()

    def ag_wait(buf, i, which):
        wait_bytes(buf.at[pl.ds(0, R), :], rsem.at[i + which])

    def ag_bytes(buf):
        return buf.at[pl.ds(0, 3 * RC), :]

    i_n1, s_n1 = rtake(4), stake(2)
    for ch in range(CH):
        sent(ag_bytes(n1), s_n1 + ch)
    for ch in range(CH):
        def first(q, ch=ch):
            r0 = mul(ch * RC + q * 32, 32)
            zz, _ = layer_stats(tok[pl.ds(r0, 32), :].astype(f32))
            n1[pl.ds(mul(my + r0, 32), 32), :] = (zz * vec[0:1, :] + vec[1:2, :]).astype(bf16)

        loop(RC // 32, first)
        ag_start(n1, i_n1, s_n1, ch)


    def mask_rows(q):
        r0 = mul(q * 32, 32)
        g = cot[pl.ds(r0, 32), :].astype(f32) * valid_rows(r0, 32)
        gf[pl.ds(mul(my + r0, 32), 32), :] = g.astype(bf16)

    loop(R // 32, mask_rows)
    i_gf, s_gf = rtake(4), stake(2)
    for ch in range(CH):
        ag_start(gf, i_gf, s_gf, ch)
    for j in range(6):
        if j % 3 == 1:
            qbias[:, j * 128 : (j + 1) * 128] = jnp.zeros((8, 128), f32)
        else:
            r = 2 + j % 3 // 2
            b = vec[r : r + 1, pl.ds(mul((ctx + 4 * (j // 3)) * 128, 128), 128)]
            qbias[:, j * 128 : (j + 1) * 128] = jnp.broadcast_to(b, (8, 128))
    relay_step(qkv_block, i_qr, s_qr, 1)
    relay_step(qkv_block, i_qr, s_qr, 2)
    i_oz, i_ox, s_oz, s_ox = rtake(3), rtake(), stake(), stake()
    out_block = lambda zz: wout.at[pl.ds(mul((zz // 2) * 128, 128), 128), :]

    @pl.when(ctx == t)
    def _():
        wait_bytes(wout.at[pl.ds(0, 96), :], rsem.at[i_oa])
        wait_bytes(wout.at[pl.ds(0, 32), :], lsem.at[l_o])
        for d in (1, 2, 3):
            rcopy(out_block(z), out_block(z), zpeer(d), i_oz + d - 1, s_oz).start()
        rcopy(out_block(z), out_block(z), xpeer, i_ox, s_ox).start()

    sent(n1.at[pl.ds(0, 384), :], s_oz, ctx == t)
    sent(wout, s_ox, x == k)
    ag_forward(n1, i_n1, s_n1, 0)
    relay_step(qkv_block, i_qr, s_qr, 3)

    wait_bytes(wup.at[pl.ds(0, 96), :], rsem.at[i_ua])
    wait_bytes(wup.at[pl.ds(0, 32), :], lsem.at[l_u])
    up_block = lambda s: wup.at[srow(s), :]
    i_ur, s_ur = rtake(8), stake(3)
    relay_start(up_block, i_ur, s_ur)
    relay_sent(wup, s_ur)
    ag_forward(n1, i_n1, s_n1, 1)

    ag_wait(n1, i_n1, 0)
    relay_finish(wqkv, i_qr)
    mine = x == k
    for d in (1, 2, 3):
        zz = (z - d + 4) % 4

        @pl.when(jnp.logical_and(mine, zz % 2 == y))
        def _(d=d, zz=zz):
            wait_bytes(out_block(zz), rsem.at[i_oz + d - 1])
            rcopy(out_block(zz), out_block(zz), xpeer, i_ox, s_ox).start()

    relay_x(up_block, i_ur, s_ur)

    def project(it):
        blk = ((y + it // 2) % 2) * 2 + (k + it % 2) % 2

        @pl.when(it == 3)
        def _():
            ag_wait(n1, i_n1, 3)

        qkv[rows(blk), :] = (nn(n1[rows(blk), :], wqkv[...]) + qbias[0:1, :]).astype(bf16)

    loop(4, project)
    relay_step(up_block, i_ur, s_ur, 1)
    relay_start(down_block, i_dr, s_dr, src=down_in)

    def turn(i):
        c0 = pl.ds(mul(i * 128, 128), 128)
        vt[c0, :] = qkv[:, pl.ds(mul(i * 384 + 256, 128), 128)].T
        kt[c0, :] = qkv[:, pl.ds(mul(i * 384 + 128, 128), 128)].T

    loop(2, turn)

    lane = lax.broadcasted_iota(jnp.int32, (256, 128), 1)
    krow = lax.broadcasted_iota(jnp.int32, (256, 256), 0)
    qcol = lax.broadcasted_iota(jnp.int32, (256, 256), 1)

    def tri(kb, qb):
        return (qb * (qb + 1)) // 2 + kb

    def half(v, j):
        return jnp.where((lane // 64) == j, v, jnp.zeros_like(v))

    def pair_forward(i):
        for j in range(2):
            slope = jnp.exp2(jnp.full((1024, 128), -0.5, f32)
                             * (2 * ctx + 8 * i + j + 1).astype(f32)) * LOG2E
            b = slope * lax.broadcasted_iota(jnp.int32, (1024, 128), 0).astype(f32)
            for kb in range(4):
                own_b[j * 256 : (j + 1) * 256, kb * 128 : (kb + 1) * 128] = b[kb * 256 : (kb + 1) * 256]

        def queries(qb):
            q0 = pl.ds(mul(qb * 256, 256), 256)
            qblk = qkv[q0, pl.ds(mul(i * 384, 128), 128)]

            def scores(kb, best):
                k0 = pl.ds(mul(kb * 256, 256), 256)
                kblk = qkv[k0, pl.ds(mul(i * 384 + 128, 128), 128)]
                new = []
                for j in range(2):
                    b = own_b[j * 256 : (j + 1) * 256, pl.ds(mul(kb * 128, 128), 128)]
                    sc = nt(half(kblk, j), qblk) * (0.125 * LOG2E) + jnp.concatenate([b, b], axis=1)
                    sc = jnp.where(krow + kb * 256 <= qcol + qb * 256, sc, -1e30)
                    own_a[j * 256 : (j + 1) * 256, k0] = sc
                    new.append(jnp.maximum(best[j], jnp.max(sc.reshape(32, 8, 256), axis=0)))
                return tuple(new)

            low = jnp.full((8, 256), -3e38, f32)
            best = lax.fori_loop(0, qb + 1, scores, (low, low))
            top = [jnp.max(b, axis=0, keepdims=True) for b in best]

            def weigh(kb, carry):
                k0 = pl.ds(mul(kb * 256, 256), 256)
                new = []
                for j in range(2):
                    total, acc = carry[2 * j], carry[2 * j + 1]
                    p = jnp.exp2(own_a[j * 256 : (j + 1) * 256, k0] - top[j])
                    total = total + jnp.sum(p.reshape(32, 8, 256), axis=0)
                    p = p.astype(bf16)
                    ptri[2 * i + j, tri(kb, qb)] = p
                    v = vt[pl.ds(mul(i * 128 + j * 64, 64), 64), k0]
                    new += [total, acc + nn(v, p)]
                return tuple(new)

            zero = (jnp.zeros((8, 256), f32), jnp.zeros((64, 256), f32))
            out = lax.fori_loop(0, qb + 1, weigh, zero + zero)
            for j in range(2):
                inv = 1.0 / jnp.sum(out[2 * j], axis=0, keepdims=True)
                linv[2 * i + j, :, q0] = jnp.broadcast_to(inv, (8, 256))
                attt[pl.ds(mul(i * 128 + j * 64, 64), 64), q0] = (out[2 * j + 1] * inv).astype(bf16)

        loop(4, queries)

    pair_forward(0)
    for ch in range(CH):
        ag_forward(gf, i_gf, s_gf, ch)
    pair_forward(1)

    relay_step(up_block, i_ur, s_ur, 2)
    def rs_run(partial, sb, rb, own, i, s):
        def step(tt):
            g, ch, sub = tt // 4, tt % 2, (tt // 2) % 2
            blk = ((y + 1 - g) % 2) * 2 + (k + 1 - sub) % 2
            partial(blk, ch, tmp)

            @pl.when(jnp.logical_and(g == 0, sub == 0))
            def _():
                sb[0, ch] = tmp[...].astype(bf16)
                rcopy(sb.at[0, ch], rb.at[0, ch], mate, i + ch, s + ch).start()

            @pl.when(jnp.logical_and(g == 0, sub == 1))
            def _():
                wait_bytes(rb.at[0, ch], rsem.at[i + ch])
                sb[1, ch] = (tmp[...] + rb[0, ch].astype(f32)).astype(bf16)
                rcopy(sb.at[1, ch], rb.at[1, ch], ypeer, i + CH + ch, s + ch).start()

            @pl.when(jnp.logical_and(g == 1, sub == 0))
            def _():
                sb[2, ch] = tmp[...].astype(bf16)
                rcopy(sb.at[2, ch], rb.at[2, ch], mate, i + 2 * CH + ch, s + ch).start()

            @pl.when(jnp.logical_and(g == 1, sub == 1))
            def _():
                own[ch] = tmp[...]

        loop(4 * CH, step)

    def rs_wait(sb, rb, i, ch):
        wait_bytes(rb.at[2, ch], rsem.at[i + 2 * CH + ch])
        wait_bytes(rb.at[1, ch], rsem.at[i + CH + ch])

    def rs_sum(rb, own, ch, r):
        return own[ch, r, :] + rb[2, ch, r, :].astype(f32) + rb[1, ch, r, :].astype(f32)

    def rs_sent(sb, s):
        for ch in range(CH):
            wait_bytes(sb.at[:, ch], ssem.at[s + ch])

    @pl.when(x != k)
    def _():
        wait_bytes(wout, rsem.at[i_ox])

    def branch_part(blk, ch, dst):
        a = attt[:, pl.ds(mul(blk * R + ch * RC, RC), RC)]
        dst[...] = tn(a, wout[...])

    i_br, s_br = rtake(3 * CH), stake(CH)
    rs_run(branch_part, rs_s, rs_r, rs_own, i_br, s_br)
    relay_step(up_block, i_ur, s_ur, 3)
    relay_step(down_block, i_dr, s_dr, 1)

    i_n2, s_n2 = rtake(4), stake(2)
    stat[...] = jnp.zeros_like(stat)
    for ch in range(CH):
        rs_wait(rs_s, rs_r, i_br, ch)

        def second(q, ch=ch):
            r = pl.ds(mul(q * 32, 32), 32)
            r1 = pl.ds(mul(ch * RC + q * 32, 32), 32)
            branch = rs_sum(rs_r, rs_own, ch, r) + vec[4:5, :]
            resid = tok[r1, :].astype(f32) + branch
            res[r1, :] = resid
            zz, _ = layer_stats(resid)
            n2[pl.ds(mul(my + ch * RC + q * 32, 32), 32), :] = (
                zz * vec[5:6, :] + vec[6:7, :]).astype(bf16)
            v = valid_rows(ch * RC + q * 32, 32)
            stat[0:8, :] += jnp.sum((branch * branch * v).reshape(4, 8, D), axis=0)
            stat[8:16, :] += jnp.sum((resid * resid * v).reshape(4, 8, D), axis=0)

        loop(RC // 32, second)
        ag_start(n2, i_n2, s_n2, ch)

    relay_step(down_block, i_dr, s_dr, 2)
    relay_finish(wup, i_ur)

    def feed(it):
        blk = ((y + it // 2) % 2) * 2 + (k + it % 2) % 2

        @pl.when(it == 1)
        def _():
            ag_wait(n2, i_n2, 0)
            ag_forward(n2, i_n2, s_n2, 0)
            relay_step(down_block, i_dr, s_dr, 3)

        @pl.when(it == 2)
        def _():
            ag_forward(n2, i_n2, s_n2, 1)

        @pl.when(it == 3)
        def _():
            ag_wait(n2, i_n2, 3)

        def cols(n):
            c0 = pl.ds(mul(n * 512, 512), 512)
            pre = nn(n2[rows(blk), :], wup[:, c0]) + vec[8:9, c0]
            sq = pre * pre
            th = jnp.tanh(0.7978845608028654 * pre * (1.0 + 0.044715 * sq))
            a1 = 0.5 * (1.0 + th)
            act[rows(blk), c0] = (pre * a1).astype(bf16)
            der = a1 + 0.5 * pre * (1.0 - th * th) * (
                0.7978845608028654 * (1.0 + 0.134145 * sq))
            gpre[rows(blk), c0] = der.astype(bf16)

        loop(2, cols)

    loop(4, feed)

    def dw_half(a, b, c0, n, xx, hh):
        c1 = pl.ds(mul((hh * 2 + xx) * 128, 128), 128)
        c2 = pl.ds(mul(((3 - hh) * 2 + xx) * 128, 128), 128)
        return tn(jnp.concatenate([a[:, c1], a[:, c2]], axis=1), b[:, c0 : c0 + n])

    def dw_away(a, b, c0, n, xb, xr, i, s, parts):
        w = n // parts
        for hh in range(2):
            r = pl.ds(hh * 256, 256)
            xb[r, c0 : c0 + n] = dw_half(a, b, c0, n, (x + 1) % 2, hh).astype(bf16)
            for p in range(parts):
                c = pl.ds(c0 + p * w, w)
                rcopy(xb.at[r, c], xr.at[r, c], xpeer, i + hh * parts + p, s).start()
        sent(xb.at[pl.ds(0, 512), pl.ds(c0, n)], s)

    def dw_keep(a, b, c0, n, own):
        def keep(hh):
            own[pl.ds(mul(hh * 256, 256), 256), c0 : c0 + n] = dw_half(a, b, c0, n, x, hh)

        loop(2, keep)

    def dw_z(hh, c0, n, xr, own, zb, zr0, zc, zr, fin, i, iz, sz):
        wait_bytes(xr.at[pl.ds(0, 256), pl.ds(c0, n)], rsem.at[i])
        c = slice(c0, c0 + n)
        cz = slice(zc, zc + n)
        for part, zz in enumerate((hh, 3 - hh)):
            r = slice(hh * 256 + part * 128, hh * 256 + part * 128 + 128)
            ro = slice(zr0 + zz * 128, zr0 + zz * 128 + 128)
            dz = (zz - z + 4) % 4

            @pl.when(zz == z)
            def _(r=r):
                fin[:, c] = own[r, c] + xr[r, c].astype(f32)

            @pl.when(zz != z)
            def _(r=r, ro=ro, zz=zz, dz=dz):
                zb[ro, cz] = (own[r, c] + xr[r, c].astype(f32)).astype(bf16)
                rcopy(zb.at[ro, cz], zr.at[dz - 1, :, c], {"seq": zz * 2 + x}, iz, sz).start()

    def dw_end(c0, n, zr, fin, iz):
        c = slice(c0, c0 + n)
        wait_bytes(zr.at[:, :, pl.ds(c0, n)], rsem.at[iz])
        fin[:, c] += (zr[0, :, c].astype(f32) + zr[1, :, c].astype(f32)) + zr[2, :, c].astype(f32)

    ag_wait(gf, i_gf, 0)
    ag_wait(gf, i_gf, 3)
    i_dwx, i_dwz, s_dwx, s_dwz = rtake(4), rtake(2), stake(), stake(2)
    dw_away(act, gf, 0, D, xs_down, xr_down, i_dwx, s_dwx, 2)
    dw_keep(act, gf, 0, D, own_a)
    relay_finish(wdown, i_dr)
    wait_bytes(wdown.at[pl.ds(0, 128), :], lsem.at[l_d])
    gvec[...] = jnp.zeros_like(gvec)

    def grad_feed(it):
        r = pl.ds(mul(it * R, R), R)

        def cols(n):
            c0 = pl.ds(mul(n * 512, 512), 512)
            ga = nt(gf[r, :], wdown[c0, :])
            g = (ga * gpre[r, c0].astype(f32)).astype(bf16)
            gpre[r, c0] = g
            gvec[2, :, c0] += jnp.sum(g.astype(f32).reshape(R // 8, 8, 512), axis=0)

        loop(2, cols)

    loop(4, grad_feed)

    def down_z(hh, p):
        dw_z(hh, p * 512, 512, xr_down, own_a, dmix, p * 512, 0, zr_down, fin_down,
             i_dwx + hh * 2 + p, i_dwz + p, s_dwz + p)

    down_z(0, 0)

    rs_sent(rs_s, s_br)

    def gn2_part(blk, ch, dst):
        dst[...] = nt(gpre[pl.ds(mul(blk * R + ch * RC, RC), RC), :], wup[...])

    i_g2, s_g2 = rtake(3 * CH), stake(CH)
    rs_run(gn2_part, rs_s, rs_r, rs_own, i_g2, s_g2)

    down_z(0, 1)
    i_uwx, i_uwz, s_uwx, s_uwz = rtake(4), rtake(2), stake(), stake(2)
    dw_away(n2, gpre, 0, D, xs_up, xr_up, i_uwx, s_uwx, 2)
    dw_keep(n2, gpre, 0, D, own_b)

    def up_z(hh, p):
        dw_z(hh, p * 512, 512, xr_up, own_b, gpre, 0, p * 512, zr_up, fin_up,
             i_uwx + hh * 2 + p, i_uwz + p, s_uwz + p)

    for p in range(2):
        sent(gpre.at[pl.ds(0, 384), pl.ds(0, 512)], s_uwz + p)
    down_z(1, 0)

    i_gb, s_gb = rtake(4), stake(2)
    for ch in range(CH):
        sent(ag_bytes(gb), s_gb + ch)
    for ch in range(CH):
        rs_wait(rs_s, rs_r, i_g2, ch)

        def third(q, ch=ch):
            r = pl.ds(mul(q * 32, 32), 32)
            r1 = pl.ds(mul(ch * RC + q * 32, 32), 32)
            g2 = rs_sum(rs_r, rs_own, ch, r)
            zz, rstd = layer_stats(res[r1, :])
            gout = cot[r1, :].astype(f32) * valid_rows(ch * RC + q * 32, 32)
            gres = gout + layer_back(g2, vec[5:6, :], zz, rstd)
            st_grad[r1, :] = gres
            low = gres.astype(bf16)
            gb[pl.ds(mul(my + ch * RC + q * 32, 32), 32), :] = low
            fold = lambda v: jnp.sum(v.reshape(4, 8, D), axis=0)
            gvec[4] += fold(low.astype(f32))
            gvec[5] += fold(g2 * zz)
            gvec[6] += fold(g2)
            gvec[7] += fold(gout)

        loop(RC // 32, third)
        ag_start(gb, i_gb, s_gb, ch)

    down_z(1, 1)
    ag_forward(gb, i_gb, s_gb, 0)

    def ffn_part(blk, ch, dst):
        dst[...] = nn(act[pl.ds(mul(blk * R + ch * RC, RC), RC), :], wdown[...])

    i_ff, s_ff = rtake(3 * CH), stake(CH)
    rs_run(ffn_part, rt_s, rt_r, rt_own, i_ff, s_ff)
    up_z(0, 0)
    ag_forward(gb, i_gb, s_gb, 1)

    ag_wait(gb, i_gb, 0)
    ag_wait(gb, i_gb, 3)

    def att_grad(i):
        c0 = pl.ds(mul(i * 256, 256), 256)
        dot_[:, c0] = nt(wout[...], gb[c0, :]).astype(bf16)

    loop(4, att_grad)
    own_out[...] = nn(attt[...], gb[...])
    i_owx, i_owz, s_owx, s_owz = rtake(), rtake(), stake(), stake()
    for ch in range(CH):
        wait_bytes(ag_bytes(gf), ssem.at[s_gf + ch])
        wait_bytes(ag_bytes(n2), ssem.at[s_n2 + ch])
    xs_out = gf.at[pl.ds(512, 256), :]

    @pl.when(x != k)
    def _():
        gf[512:768, :] = own_out[...].astype(bf16)
        rcopy(xs_out, xr_out, xpeer, i_owx, s_owx).start()

    sent(xs_out, s_owx, x != k)
    sent(n2.at[pl.ds(0, 128), :], s_owz, jnp.logical_and(x == k, z % 2 == y))
    sent(n2.at[pl.ds(0, 256), :], s_owz, jnp.logical_and(x == k, z % 2 != y))

    lane2 = lax.broadcasted_iota(jnp.int32, (1024, 128), 1)

    def pair_backward(i):
        p0 = pl.ds(mul(i * 128, 128), 128)
        for j in range(2):
            r0 = pl.ds(mul(i * 128 + j * 64, 64), 64)
            li = linv[2 * i + j, 0:1, :]
            dd = dot_[r0, :].astype(f32) * li
            delta = jnp.sum(dd * attt[r0, :].astype(f32), axis=0, keepdims=True)
            linv[2 * i + j, :, :] = jnp.broadcast_to(delta, (8, 1024))
            dot_[r0, :] = dd.astype(bf16)
        do_[...] = dot_[p0, :].T
        acck[...] = jnp.zeros_like(acck)
        accv[...] = jnp.zeros_like(accv)

        def queries(qb):
            q0 = pl.ds(mul(qb * 256, 256), 256)
            qblk = qkv[q0, pl.ds(mul(i * 384, 128), 128)]
            doblk = do_[q0, :]
            dt = dot_[p0, q0]

            def keys(kb, carry):
                k0 = pl.ds(mul(kb * 256, 256), 256)
                vblk = qkv[k0, pl.ds(mul(i * 384 + 256, 128), 128)]
                new = []
                for j in range(2):
                    p = ptri[2 * i + j, tri(kb, qb)]
                    dp = nn(half(vblk, j), dt) - linv[2 * i + j, 0:1, q0]
                    ds = (p.astype(f32) * dp).astype(bf16)
                    accv[j, k0, :] += nn(p, doblk)
                    acck[j, k0, :] += nn(ds, qblk)
                    kk = kt[pl.ds(mul(i * 128 + j * 64, 64), 64), k0]
                    new.append(carry[j] + nn(kk, ds))
                return tuple(new)

            zero = jnp.zeros((64, 256), f32)
            dq = lax.fori_loop(0, qb + 1, keys, (zero, zero))
            dq = jnp.concatenate(dq, axis=0) * 0.125
            dmix[q0, pl.ds(mul(i * 384, 128), 128)] = dq.T.astype(bf16)

        loop(4, queries)
        dk = jnp.where(lane2 < 64, acck[0], acck[1]) * 0.125
        dv = jnp.where(lane2 < 64, accv[0], accv[1])
        dmix[:, pl.ds(mul(i * 384 + 128, 128), 128)] = dk.astype(bf16)
        dmix[:, pl.ds(mul(i * 384 + 256, 128), 128)] = dv.astype(bf16)

    up_z(0, 1)
    for p in range(2):
        wait_bytes(dmix.at[pl.ds(0, 384), pl.ds(0, 512)], ssem.at[s_dwz + p])
    pair_backward(0)
    i_qwx, i_qwz, s_qwx, s_qwz = (rtake(2), rtake(2)), rtake(2), stake(2), stake(2)
    up_z(1, 0)
    dw_away(n1, dmix, 0, 384, gf, xr_qkv, i_qwx[0], s_qwx, 1)
    pair_backward(1)

    rs_sent(rs_s, s_g2)

    def gn1_part(blk, ch, dst):
        dst[...] = nt(dmix[pl.ds(mul(blk * R + ch * RC, RC), RC), :], wqkv[...])

    i_g1, s_g1 = rtake(3 * CH), stake(CH)
    up_z(1, 1)
    rs_run(gn1_part, rs_s, rs_r, rs_own, i_g1, s_g1)
    dw_away(n1, dmix, 384, 384, gf, xr_qkv, i_qwx[1], s_qwx + 1, 1)
    dw_keep(n1, dmix, 0, 768, own_a)

    def qkv_z(h):
        for hh in range(2):
            dw_z(hh, h * 384, 384, xr_qkv, own_a, n2, 0, h * 384, zr_qkv, fin_qkv,
                 i_qwx[h] + hh, i_qwz + h, s_qwz + h)
        sent(n2.at[pl.ds(0, 384), pl.ds(0, 384)], s_qwz + h)

    for i in range(2):
        zi = y + 2 * i
        dz = (zi - z + 4) % 4

        @pl.when(x == k)
        def _(i=i, zi=zi, dz=dz):
            if i == 0:
                wait_bytes(xr_out, rsem.at[i_owx])
            half_rows = slice(i * 128, (i + 1) * 128)
            total = own_out[half_rows, :] + xr_out[half_rows, :].astype(f32)

            @pl.when(zi == z)
            def _():
                fin_out[...] = total

            @pl.when(zi != z)
            def _():
                n2[512 + i * 128 : 640 + i * 128, :] = total.astype(bf16)
                rcopy(n2.at[pl.ds(512 + i * 128, 128), :], zr_out.at[dz - 1], {"seq": zi * 2 + x}, i_owz, s_owz).start()

    qkv_z(0)
    for ch in range(CH):
        rs_wait(rs_s, rs_r, i_g1, ch)

        def fourth(q, ch=ch):
            r = pl.ds(mul(q * 32, 32), 32)
            r1 = pl.ds(mul(ch * RC + q * 32, 32), 32)
            g1 = rs_sum(rs_r, rs_own, ch, r)
            zz, rstd = layer_stats(tok[r1, :].astype(f32))
            st_grad[r1, :] += layer_back(g1, vec[0:1, :], zz, rstd)
            fold = lambda v: jnp.sum(v.reshape(4, 8, D), axis=0)
            gvec[0] += fold(g1 * zz)
            gvec[1] += fold(g1)

        loop(RC // 32, fourth)
    l_g = next(lids)
    pltpu.make_async_copy(st_grad, o_grad, lsem.at[l_g]).start()

    gmat[...] = jnp.zeros_like(gmat)
    for r, v in ((0, 0), (1, 1), (4, 4), (5, 5), (6, 6), (7, 7), (8, 2)):
        gmat[r : r + 1, :] = jnp.sum(gvec[v], axis=0, keepdims=True)
    for r, p in ((2, 0), (3, 256)):
        for i in range(2):
            v = dmix[:, i * 384 + p : i * 384 + p + 128].astype(f32)
            v = jnp.sum(jnp.sum(v.reshape(128, 8, 128), axis=0), axis=0, keepdims=True)
            gmat[r : r + 1, pl.ds(mul((ctx + 4 * i) * 128, 128), 128)] = v
    for s in range(8):
        sg[s] = gmat[:, s * 128 : (s + 1) * 128]
    i_sgx, i_sgz, i_sgc, s_sgx, s_sgz, s_sgc = rtake(), rtake(), rtake(), stake(), stake(), stake()
    for j in range(4):
        src = sg.at[j * 2 + (x + 1) % 2]
        rcopy(src, sgx.at[j], xpeer, i_sgx, s_sgx).start()
    sent(sgx, s_sgx)

    qkv_z(1)
    wait_bytes(sgx, rsem.at[i_sgx])
    for d in (1, 2, 3):
        zz = (z + d) % 4
        sgs[d - 1] = sg[zz * 2 + x] + sgx[zz]
        rcopy(sgs.at[d - 1], sgz.at[d - 1], zpeer(d), i_sgz, s_sgz).start()
    sent(sgs, s_sgz)

    for p in range(2):
        dw_end(p * 512, 512, zr_down, fin_down, i_dwz + p)
    l_dd = next(lids)
    pltpu.make_async_copy(fin_down, o_ddown, lsem.at[l_dd]).start()
    for p in range(2):
        dw_end(p * 512, 512, zr_up, fin_up, i_uwz + p)
    i_uf, i_qf, i_of, s_uf, s_qf, s_of = rtake(), rtake(2), rtake(), stake(), stake(2), stake()

    def up_piece(fin, c, s):
        return (fin.at[pl.ds(mul(c * 32, 32), 32), pl.ds(s * 128, 128)],
                o_dup.at[:, pl.ds(mul((s * 4 + ctx) * 128, 128), 128)])

    for d in (1, 2, 3):
        for s in range(8):
            a, b = up_piece(fin_up, (ctx + d) % 4, s)
            rcopy(a, b, cpeer(d), i_uf, s_uf).start()
    sent(fin_up.at[pl.ds(0, 96), :], s_uf)
    mine32 = pl.ds(mul(ctx * 32, 32), 32)
    l_up = next(lids)
    for s in range(8):
        a, b = up_piece(fin_up, ctx, s)
        pltpu.make_async_copy(a, b, lsem.at[l_up]).start()

    l_do = next(lids)

    @pl.when(ctx == t)
    def _():
        wait_bytes(zr_out, rsem.at[i_owz])
        fin_out[...] += (zr_out[0].astype(f32) + zr_out[1].astype(f32)) + zr_out[2].astype(f32)
        for d in (1, 2, 3):
            src = fin_out.at[pl.ds(mul(((ctx + d) % 4) * 32, 32), 32), :]
            rcopy(src, o_dout, cpeer(d), i_of, s_of).start()
        pltpu.make_async_copy(fin_out.at[mine32, :], o_dout, lsem.at[l_do]).start()

    sent(fin_out.at[pl.ds(0, 96), :], s_of, ctx == t)

    for ch in range(CH):
        rs_wait(rt_s, rt_r, i_ff, ch)

        def last(q, ch=ch):
            r = pl.ds(mul(q * 32, 32), 32)
            r1 = pl.ds(mul(ch * RC + q * 32, 32), 32)
            ffn = rs_sum(rt_r, rt_own, ch, r) + vec[7:8, :]
            v = valid_rows(ch * RC + q * 32, 32)
            st_out[r1, :] = (v * (res[r1, :] + ffn)).astype(bf16)
            stat[16:24, :] += jnp.sum((ffn * ffn * v).reshape(4, 8, D), axis=0)

        loop(RC // 32, last)
    l_t = next(lids)
    pltpu.make_async_copy(st_out, o_out, lsem.at[l_t]).start()

    wait_bytes(sgz, rsem.at[i_sgz])
    sgf[...] = sg[seq] + sgx[z] + (sgz[0] + sgz[1] + sgz[2])
    for j in range(3):
        v = jnp.sum(stat[j * 8 : (j + 1) * 8, :], axis=0, keepdims=True)
        sgf[9 + j : 10 + j, :] = jnp.broadcast_to(jnp.sum(v, axis=1, keepdims=True), (1, 128))
    for d in (1, 2, 3):
        rcopy(sgf, sgc.at[d], cpeer(d), i_sgc, s_sgc).start()
    sent(sgc.at[pl.ds(1, 3)], s_sgc)

    l_dq = []
    for h in range(2):
        dw_end(h * 384, 384, zr_qkv, fin_qkv, i_qwz + h)
        pieces = list(qkv_pieces(ctx))[3 * h : 3 * h + 3]
        for d in (1, 2, 3):
            c2 = (ctx + d) % 4
            for a, b in pieces:
                rcopy(fin_qkv.at[pl.ds(mul(c2 * 32, 32), 32), b], o_dqkv.at[:, a], cpeer(d), i_qf + h, s_qf + h).start()
        sent(fin_qkv.at[pl.ds(0, 96), pl.ds(0, 384)], s_qf + h)
        l_dq.append(next(lids))
        for a, b in pieces:
            pltpu.make_async_copy(fin_qkv.at[mine32, b], o_dqkv.at[:, a], lsem.at[l_dq[h]]).start()

    wait_bytes(sgc.at[pl.ds(1, 3)], rsem.at[i_sgc])
    o_small[...] = sgf[...] + jnp.where(rowid != 8, sgc[1] + sgc[2] + sgc[3], 0.0)

    @pl.when(ctx != t)
    def _():
        wait_bytes(fin_out.at[pl.ds(0, 32), :], rsem.at[i_of])

    @pl.when(ctx == t)
    def _():
        wait_bytes(fin_out.at[pl.ds(0, 32), :], lsem.at[l_do])

    wait_bytes(fin_up.at[pl.ds(0, 96), :], rsem.at[i_uf])
    for h in range(2):
        wait_bytes(fin_qkv.at[pl.ds(0, 96), pl.ds(0, 384)], rsem.at[i_qf + h])
    rs_sent(rs_s, s_g1)
    rs_sent(rt_s, s_ff)
    flush()
    for ref, i in ((st_grad, l_g), (st_out, l_t), (fin_down, l_dd), (fin_up.at[pl.ds(0, 32), :], l_up),
                   (fin_qkv.at[pl.ds(0, 32), pl.ds(0, 384)], l_dq[0]),
                   (fin_qkv.at[pl.ds(0, 32), pl.ds(0, 384)], l_dq[1])):
        wait_bytes(ref, lsem.at[i])
    assert next(rids) == NRECV and next(sids) == NSEND and next(lids) == NLOCAL


def finish_kernel(length_ref, sums, *refs):
    big, outs, vecs = refs[:6], refs[6:12], refs[12:20]
    o_ub, o_stats = refs[20:22]
    stage, s_in, s_out = refs[22:28], refs[28], refs[29]
    for i in range(6):
        pltpu.make_async_copy(big[i], stage[i], s_in.at[i]).start()
    ctx = lax.axis_index("ctx")
    mine = sums[0:8, 0:32]
    for c in range(1, 4):
        mine = jnp.where(ctx == c, sums[0:8, c * 32 : (c + 1) * 32], mine)
    for r in range(8):
        vecs[r][...] = mine[r, :]
    o_ub[...] = sums[8, :]
    lane = lax.broadcasted_iota(jnp.int32, (1, 128), 1)
    v = jnp.where(lane == 0, sums[9:10, :], jnp.where(lane == 1, sums[10:11, :], sums[11:12, :]))
    o_stats[...] = jnp.sqrt(v / (length_ref[0].astype(f32) * D))[:, 0:3]
    for i in range(6):
        pltpu.make_async_copy(big[i], stage[i], s_in.at[i]).wait()
        pltpu.make_async_copy(stage[i], outs[i], s_out.at[i]).start()
    for i in range(6):
        pltpu.make_async_copy(stage[i], outs[i], s_out.at[i]).wait()


def fast(mesh):
    def scratch():
        v = lambda dt, *shape: pltpu.VMEM(shape, dt)
        return [
            v(bf16, D, 768), v(bf16, 256, D), v(bf16, D, D), v(bf16, D, D),
            v(f32, 4, 16, 128), v(f32, 8, 16, 128), v(f32, 16, D),
            v(bf16, S, D), v(bf16, S, D), v(bf16, S, D), v(bf16, S, D), v(bf16, S, D), v(bf16, S, D),
            v(bf16, S, 768), v(bf16, 256, S), v(bf16, 256, S), v(bf16, 256, S),
            v(bf16, 256, S), v(bf16, S, 128), v(bf16, S, 768), v(f32, 4, 8, S),
            v(bf16, 4, 10, 256, 256), v(f32, 2, S, 128), v(f32, 2, S, 128),
            v(bf16, 3, 2, 128, D), v(bf16, 3, 2, 128, D), v(f32, 2, 128, D),
            v(bf16, 3, 2, 128, D), v(bf16, 3, 2, 128, D), v(f32, 2, 128, D),
            v(f32, 128, D), v(f32, R, D),
            v(bf16, 512, D), v(bf16, 512, D), v(bf16, 512, D), v(bf16, 512, D), v(bf16, 512, 768), v(bf16, 256, D),
            v(f32, 512, D), v(f32, 512, D), v(f32, 256, D),
            v(bf16, 3, 128, D), v(bf16, 3, 128, D), v(bf16, 3, 128, 768), v(bf16, 3, 128, D),
            v(f32, 128, D), v(f32, 128, 768), v(f32, 128, D),
            v(bf16, R, D), v(f32, R, D), v(f32, 128, D),
            v(f32, 8, 16, 128), v(f32, 4, 16, 128), v(f32, 3, 16, 128), v(f32, 3, 16, 128),
            v(f32, 16, 128), v(f32, 4, 16, 128), v(f32, 8, 8, D), v(f32, 16, D), v(f32, 24, D), v(f32, 8, 768),
            pltpu.SemaphoreType.DMA((NLOCAL,)),
            pltpu.SemaphoreType.DMA((NSEND,)),
            pltpu.SemaphoreType.DMA((NRECV,)),
        ]

    def on_device(tokens, lengths, cotangent, g1, b1, wq, qb, vb, wo, ob, g2, b2, wu, ub, wd, db):
        ctx = lax.axis_index("ctx")
        vectors = jnp.stack([g1, b1, qb, vb, ob, g2, b2, db]).astype(f32)
        place = (jnp.arange(128) // 32) == ctx
        small = jnp.concatenate([
            jnp.where(place[None], jnp.tile(vectors, (1, 4)), 0.0),
            ub.astype(f32)[None], jnp.zeros((7, 128), f32)])
        vm = pl.BlockSpec(memory_space=pltpu.VMEM)
        sds = jax.ShapeDtypeStruct
        out, grad, dqkv, dout, dup, ddown, sums = pl.pallas_call(
            block_kernel,
            out_shape=(sds((R, D), bf16), sds((R, D), f32), sds((32, 3 * D), f32), sds((32, D), f32),
                       sds((32, 4 * D), f32), sds((128, D), f32), sds((16, 128), f32)),
            in_specs=[pl.BlockSpec(memory_space=pltpu.SMEM)] + [vm] * 3 + [pl.BlockSpec(memory_space=pl.ANY)] * 4,
            out_specs=tuple([pl.BlockSpec(memory_space=pl.ANY)] * 6 + [vm]),
            scratch_shapes=scratch(),
            compiler_params=pltpu.CompilerParams(
                collective_id=0, has_side_effects=True, vmem_limit_bytes=LIMIT),
            name="block",
        )(lengths, tokens[0], cotangent[0], small, wq, wo, wu, wd)
        anyspec = pl.BlockSpec(memory_space=pl.ANY)
        big = (out, grad, dqkv, dout, dup, ddown)
        res = pl.pallas_call(
            finish_kernel,
            out_shape=tuple(sds(v.shape, v.dtype) for v in big)
            + tuple([sds((32,), f32)] * 8) + (sds((128,), f32), sds((1, 3), f32)),
            in_specs=[pl.BlockSpec(memory_space=pltpu.SMEM), vm] + [anyspec] * 6,
            out_specs=tuple([anyspec] * 6 + [vm] * 10),
            scratch_shapes=[pltpu.VMEM(v.shape, v.dtype) for v in big]
            + [pltpu.SemaphoreType.DMA((6,)), pltpu.SemaphoreType.DMA((6,))],
            compiler_params=pltpu.CompilerParams(vmem_limit_bytes=LIMIT),
            name="finish",
        )(lengths, sums, *big)
        out, grad, dqkv, dout, dup, ddown, g1, b1, qb, vb, ob, g2, b2, db, ub, stats = res
        return (out[None], grad[None], g1, b1, dqkv, qb, vb, dout, ob, g2, b2, dup, ub, ddown, db, stats)

    return on_device


HEADS = 16


epsilon = 1e-05


def normalize(inputs, gain, shift):
    average = jnp.mean(inputs, axis=-1, keepdims=True)
    centred = inputs - average
    variance = jnp.mean(centred * centred, axis=-1, keepdims=True)
    return centred * lax.rsqrt(variance + epsilon) * gain + shift


def gelu_tanh(inputs):
    return jax.nn.gelu(inputs, approximate=True)


def inner_rows(left, right):
    return lax.dot_general(
        left, right, (((0,), (0,)), ((), ())), preferred_element_type=jnp.float32
    )


def outer_cols(left, right):
    return lax.dot_general(
        left, right, (((1,), (1,)), ((), ())), preferred_element_type=jnp.float32
    )


def alibi_scores(query_block, key_block, query_pos, key_pos, slope_block):
    raw = jnp.einsum("qhd,khd->hqk", query_block, key_block, preferred_element_type=jnp.float32)
    offset = (key_pos[None, :] - query_pos[:, None]).astype(jnp.float32)
    scores = raw * query_block.shape[-1] ** (-0.5) + slope_block[:, None, None] * offset[None]
    allowed = key_pos[None, :] <= query_pos[:, None]
    return (scores, allowed)


def score_grads(
    query_block,
    key_block,
    value_block,
    grad_block,
    query_pos,
    key_pos,
    slope_block,
    log_block,
    delta_block,
):
    scores, allowed = alibi_scores(query_block, key_block, query_pos, key_pos, slope_block)
    probs = jnp.where(allowed[None], jnp.exp(scores - log_block[..., None]), 0.0)
    grad_probs = jnp.einsum(
        "qhd,khd->hqk", grad_block, value_block, preferred_element_type=jnp.float32
    )
    delta_block = jnp.sum(probs * grad_probs, axis=-1)
    grad_scores = (probs * (grad_probs - delta_block[..., None])).astype(jnp.bfloat16)
    return (probs, grad_scores, delta_block)


def on_device(
    tokens,
    lengths,
    cotangent,
    ln1_gain,
    ln1_bias,
    qkv_weight,
    query_bias,
    value_bias,
    out_weight,
    out_bias,
    ln2_gain,
    ln2_bias,
    up_weight,
    up_bias,
    down_weight,
    down_bias,
):
    shards = (
        ln1_gain,
        ln1_bias,
        qkv_weight,
        query_bias,
        value_bias,
        out_weight,
        out_bias,
        ln2_gain,
        ln2_bias,
        up_weight,
        up_bias,
        down_weight,
        down_bias,
    )
    row_count = tokens.shape[1]
    model_width = tokens.shape[2]
    head_count = HEADS
    head_width = model_width // head_count
    per_block = 2
    block_count = head_count // per_block
    slot_rows = row_count * lax.axis_size("ctx")
    positions = lax.axis_index("ctx") * row_count + jnp.arange(row_count, dtype=jnp.int32)
    length = lengths[0]
    valid_rows = (positions < length).astype(jnp.float32)[:, None]
    slopes = jnp.exp2(-8.0 * (jnp.arange(head_count, dtype=jnp.float32) + 1.0) / head_count)
    key_positions = jnp.arange(slot_rows, dtype=jnp.int32)
    scale = head_width ** (-0.5)
    full_weights = (
        lax.all_gather(shards[0], ("seq", "ctx"), axis=0, tiled=True),
        lax.all_gather(shards[1], ("seq", "ctx"), axis=0, tiled=True),
        lax.all_gather(shards[2], ("seq", "ctx"), axis=0, tiled=True),
        lax.all_gather(shards[3], ("seq", "ctx"), axis=0, tiled=True),
        lax.all_gather(shards[4], ("seq", "ctx"), axis=0, tiled=True),
        lax.all_gather(shards[5], ("seq", "ctx"), axis=0, tiled=True),
        lax.all_gather(shards[6], ("seq", "ctx"), axis=0, tiled=True),
        lax.all_gather(shards[7], ("seq", "ctx"), axis=0, tiled=True),
        lax.all_gather(shards[8], ("seq", "ctx"), axis=0, tiled=True),
        lax.all_gather(shards[9], ("seq", "ctx"), axis=0, tiled=True),
        lax.all_gather(shards[10], ("seq", "ctx"), axis=0, tiled=True),
        lax.all_gather(shards[11], ("seq", "ctx"), axis=0, tiled=True),
        lax.all_gather(shards[12], ("seq", "ctx"), axis=0, tiled=True),
    )
    (
        gain_one,
        shift_one,
        w_qkv,
        bias_query,
        bias_value,
        w_out,
        bias_out,
        gain_two,
        shift_two,
        w_up,
        bias_up,
        w_down,
        bias_down,
    ) = full_weights

    def pick(array, index):
        return lax.dynamic_slice_in_dim(array, index * per_block, per_block, 1)

    def pick_slopes(index):
        return lax.dynamic_slice_in_dim(slopes, index * per_block, per_block, 0)

    def to_blocks(array):
        return array.transpose(1, 0, 2, 3).reshape(array.shape[1], model_width)

    source = tokens[0].astype(jnp.float32)
    normed_one, back_one = jax.vjp(normalize, source, gain_one, shift_one)
    normed_low = normed_one.astype(jnp.bfloat16)
    mixed = jnp.dot(normed_low, w_qkv, preferred_element_type=jnp.float32)
    query = (mixed[:, :model_width] + bias_query).astype(jnp.bfloat16)
    keys = mixed[:, model_width : 2 * model_width].astype(jnp.bfloat16)
    values = (mixed[:, 2 * model_width :] + bias_value).astype(jnp.bfloat16)
    all_keys, all_values = (
        lax.all_gather(keys, "ctx", axis=0, tiled=True),
        lax.all_gather(values, "ctx", axis=0, tiled=True),
    )
    query_heads = query.reshape(row_count, head_count, head_width)
    key_heads = all_keys.reshape(slot_rows, head_count, head_width)
    value_heads = all_values.reshape(slot_rows, head_count, head_width)

    def forward_block(index):
        scores, allowed = alibi_scores(
            pick(query_heads, index),
            pick(key_heads, index),
            positions,
            key_positions,
            pick_slopes(index),
        )
        masked = jnp.where(allowed[None], scores, -1e30)
        highest = jnp.max(masked, axis=-1)
        total = jnp.sum(jnp.exp(masked - highest[..., None]), axis=-1)
        log_total = highest + jnp.log(total)
        probs = jnp.where(allowed[None], jnp.exp(scores - log_total[..., None]), 0.0)
        block_out = jnp.einsum(
            "hqk,khd->qhd",
            probs.astype(jnp.bfloat16),
            pick(value_heads, index),
            preferred_element_type=jnp.float32,
        )
        return (block_out, log_total)

    head_out, log_totals = lax.map(forward_block, jnp.arange(block_count))
    attended = to_blocks(head_out).astype(jnp.bfloat16)
    branch = jnp.dot(attended, w_out, preferred_element_type=jnp.float32) + bias_out
    resid = source + branch
    normed_two, back_two = jax.vjp(normalize, resid, gain_two, shift_two)
    normed_two_low = normed_two.astype(jnp.bfloat16)
    pre_act = jnp.dot(normed_two_low, w_up, preferred_element_type=jnp.float32) + bias_up
    activated, back_act = jax.vjp(gelu_tanh, pre_act)
    activated_low = activated.astype(jnp.bfloat16)
    ffn = jnp.dot(activated_low, w_down, preferred_element_type=jnp.float32) + bias_down
    output = (valid_rows * (resid + ffn)).astype(jnp.bfloat16)[None]
    squares = jnp.stack(
        [
            jnp.sum(valid_rows * branch * branch),
            jnp.sum(valid_rows * resid * resid),
            jnp.sum(valid_rows * ffn * ffn),
        ]
    )
    totals = lax.psum(squares, "ctx")
    stats = jnp.sqrt(totals / (length.astype(jnp.float32) * model_width))[None]
    w_qkv, w_out, w_up, w_down = (
        lax.all_gather(qkv_weight, ("seq", "ctx"), axis=0, tiled=True),
        lax.all_gather(out_weight, ("seq", "ctx"), axis=0, tiled=True),
        lax.all_gather(up_weight, ("seq", "ctx"), axis=0, tiled=True),
        lax.all_gather(down_weight, ("seq", "ctx"), axis=0, tiled=True),
    )
    grad_out = cotangent[0].astype(jnp.float32) * valid_rows
    grad_ffn = grad_out.astype(jnp.bfloat16)
    grad_down_w = inner_rows(activated_low, grad_ffn)
    grad_down_b = jnp.sum(grad_ffn.astype(jnp.float32), axis=0)
    grad_activated = outer_cols(grad_ffn, w_down)
    (grad_pre,) = back_act(grad_activated)
    grad_pre_low = grad_pre.astype(jnp.bfloat16)
    grad_up_w = inner_rows(normed_two_low, grad_pre_low)
    grad_up_b = jnp.sum(grad_pre_low.astype(jnp.float32), axis=0)
    grad_normed_two = outer_cols(grad_pre_low, w_up)
    grad_resid_norm, grad_gain_two, grad_shift_two = back_two(grad_normed_two)
    grad_resid = grad_out + grad_resid_norm
    grad_branch = grad_resid.astype(jnp.bfloat16)
    grad_out_w = inner_rows(attended, grad_branch)
    grad_out_b = jnp.sum(grad_branch.astype(jnp.float32), axis=0)
    grad_attended = outer_cols(grad_branch, w_out).astype(jnp.bfloat16)
    grad_heads = grad_attended.reshape(row_count, head_count, head_width)

    def backward_block(index):
        query_block = pick(query_heads, index)
        key_block = pick(key_heads, index)
        grad_block = pick(grad_heads, index)
        probs, grad_scores, delta_block = score_grads(
            query_block,
            key_block,
            pick(value_heads, index),
            grad_block,
            positions,
            key_positions,
            pick_slopes(index),
            log_totals[index],
            None,
        )
        grad_query_block = (
            jnp.einsum("hqk,khd->qhd", grad_scores, key_block, preferred_element_type=jnp.float32)
            * scale
        )
        grad_key_block = (
            jnp.einsum("hqk,qhd->khd", grad_scores, query_block, preferred_element_type=jnp.float32)
            * scale
        )
        grad_value_block = jnp.einsum(
            "hqk,qhd->khd",
            probs.astype(jnp.bfloat16),
            grad_block,
            preferred_element_type=jnp.float32,
        )
        return (grad_query_block, grad_key_block, grad_value_block)

    query_parts, key_parts, value_parts = lax.map(backward_block, jnp.arange(block_count))
    grad_query_all = to_blocks(query_parts)
    own_keys, own_values = (
        lax.psum_scatter(
            to_blocks(key_parts).astype(jnp.bfloat16), "ctx", scatter_dimension=0, tiled=True
        ).astype(jnp.float32),
        lax.psum_scatter(
            to_blocks(value_parts).astype(jnp.bfloat16), "ctx", scatter_dimension=0, tiled=True
        ).astype(jnp.float32),
    )
    grad_query_low = grad_query_all.astype(jnp.bfloat16)
    grad_key_low = own_keys.astype(jnp.bfloat16)
    grad_value_low = own_values.astype(jnp.bfloat16)
    grad_mixed = jnp.concatenate([grad_query_low, grad_key_low, grad_value_low], axis=1)
    grad_qkv_w = inner_rows(normed_low, grad_mixed)
    grad_query_bias = jnp.sum(grad_query_low.astype(jnp.float32), axis=0)
    grad_value_bias = jnp.sum(grad_value_low.astype(jnp.float32), axis=0)
    grad_normed_one = outer_cols(grad_mixed, w_qkv)
    grad_source_norm, grad_gain_one, grad_shift_one = back_one(grad_normed_one)
    grad_tokens = (grad_resid + grad_source_norm)[None]
    summed = (
        lax.psum_scatter(
            grad_gain_one.astype(jnp.float32), ("seq", "ctx"), scatter_dimension=0, tiled=True
        ),
        lax.psum_scatter(
            grad_shift_one.astype(jnp.float32), ("seq", "ctx"), scatter_dimension=0, tiled=True
        ),
        lax.psum_scatter(grad_qkv_w, ("seq", "ctx"), scatter_dimension=0, tiled=True),
        lax.psum_scatter(grad_query_bias, ("seq", "ctx"), scatter_dimension=0, tiled=True),
        lax.psum_scatter(grad_value_bias, ("seq", "ctx"), scatter_dimension=0, tiled=True),
        lax.psum_scatter(grad_out_w, ("seq", "ctx"), scatter_dimension=0, tiled=True),
        lax.psum_scatter(grad_out_b, ("seq", "ctx"), scatter_dimension=0, tiled=True),
        lax.psum_scatter(
            grad_gain_two.astype(jnp.float32), ("seq", "ctx"), scatter_dimension=0, tiled=True
        ),
        lax.psum_scatter(
            grad_shift_two.astype(jnp.float32), ("seq", "ctx"), scatter_dimension=0, tiled=True
        ),
        lax.psum_scatter(grad_up_w, ("seq", "ctx"), scatter_dimension=0, tiled=True),
        lax.psum_scatter(grad_up_b, ("seq", "ctx"), scatter_dimension=0, tiled=True),
        lax.psum_scatter(grad_down_w, ("seq", "ctx"), scatter_dimension=0, tiled=True),
        lax.psum_scatter(grad_down_b, ("seq", "ctx"), scatter_dimension=0, tiled=True),
    )
    return (output, grad_tokens) + tuple(summed) + (stats,)


def solution(mesh):
    small_slice = mesh.shape["seq"] == 8 and mesh.shape["ctx"] == 4
    placed = (
        P("seq", "ctx", None),
        P("seq"),
        P("seq", "ctx", None),
        P(("seq", "ctx")),
        P(("seq", "ctx")),
        P(("seq", "ctx"), None),
        P(("seq", "ctx")),
        P(("seq", "ctx")),
        P(("seq", "ctx"), None),
        P(("seq", "ctx")),
        P(("seq", "ctx")),
        P(("seq", "ctx")),
        P(("seq", "ctx"), None),
        P(("seq", "ctx")),
        P(("seq", "ctx"), None),
        P(("seq", "ctx")),
    )
    return jax.shard_map(
        fast(mesh) if small_slice else on_device,
        mesh=mesh,
        in_specs=placed,
        out_specs=(
            P("seq", "ctx", None),
            P("seq", "ctx", None),
            P(("seq", "ctx")),
            P(("seq", "ctx")),
            P(("seq", "ctx"), None),
            P(("seq", "ctx")),
            P(("seq", "ctx")),
            P(("seq", "ctx"), None),
            P(("seq", "ctx")),
            P(("seq", "ctx")),
            P(("seq", "ctx")),
            P(("seq", "ctx"), None),
            P(("seq", "ctx")),
            P(("seq", "ctx"), None),
            P(("seq", "ctx")),
            P("seq", None),
        ),
        check_vma=False,
    )
```

```python
import itertools

import jax
import jax.numpy as jnp
from jax import lax
from jax.experimental import pallas as pl
from jax.experimental.pallas import tpu as pltpu
from jax.sharding import PartitionSpec as P

MESH = pl.DeviceIdType.MESH
bf16, f32 = jnp.bfloat16, jnp.float32
LOG2E = 1.4426950408889634
D = 1024
R = 256
S = 1024
LIMIT = 66_000_000
NRECV, NSEND, NLOCAL = 103, 52, 11
ORDER = (2, 3, 1)


def nn(a, b):
    return lax.dot_general(a, b, (((1,), (0,)), ((), ())), preferred_element_type=f32)


def nt(a, b):
    return lax.dot_general(a, b, (((1,), (1,)), ((), ())), preferred_element_type=f32)


def tn(a, b):
    return lax.dot_general(a, b, (((0,), (0,)), ((), ())), preferred_element_type=f32)


def mul(v, m):
    return pl.multiple_of(v, m)


def loop(n, body, start=0):
    def step(i, carry):
        body(i)
        return carry

    lax.fori_loop(start, n, step, 0)


def layer_stats(v):
    mean = jnp.sum(v, axis=-1, keepdims=True) * (1.0 / D)
    cen = v - mean
    var = jnp.sum(cen * cen, axis=-1, keepdims=True) * (1.0 / D)
    rstd = lax.rsqrt(var + 1e-5)
    return cen * rstd, rstd


def layer_back(g2, gain, z, rstd):
    g = g2 * gain
    m1 = jnp.sum(g, axis=-1, keepdims=True) * (1.0 / D)
    m2 = jnp.sum(g * z, axis=-1, keepdims=True) * (1.0 / D)
    return rstd * (g - m1 - z * m2)


def block_kernel(
    length_ref, tok, cot, small, qkv_in, out_in, up_in, down_in,
    o_out, o_grad, o_dqkv, o_dout, o_dup, o_ddown, o_small,
    wqkv, wout, wup, wdown, smc, smb, vec,
    n1, n2, gf, gb, act, gpre, qkv, vt, kt, attt, dot_, do_, dmix, linv,
    ptri, acck, accv,
    rs_s, rs_r, rs_own, rt_s, rt_r, rt_own, tmp, res,
    xs_down, xs_up, xr_down, xr_up, xr_qkv, xr_out, own_a, own_b, own_out,
    zr_down, zr_up, zr_qkv, zr_out, fin_up, fin_qkv, fin_out,
    st_out, st_grad, fin_down, sg, sgx, sgs, sgz, sgf, sgc, gvec, gmat, stat, qbias,
    lsem, ssem, rsem,
):
    seq, ctx = lax.axis_index("seq"), lax.axis_index("ctx")
    z, x = seq // 2, seq % 2
    y, k = ctx // 2, ctx % 2
    rids, sids = itertools.count(), itertools.count()
    lids = itertools.count()

    mate = {"ctx": y * 2 + (k + 1) % 2}
    ypeer = {"ctx": ((y + 1) % 2) * 2 + k}
    xpeer = {"seq": z * 2 + (x + 1) % 2}

    def cpeer(d):
        return {"ctx": (ctx + d) % 4}

    def zpeer(d):
        return {"seq": ((z + d) % 4) * 2 + x}

    def take(count, n=1):
        first = next(count)
        for _ in range(n - 1):
            next(count)
        return first

    def rtake(n=1):
        return take(rids, n)

    def stake(n=1):
        return take(sids, n)

    def rcopy(src, dst, dev, i, s):
        return pltpu.make_async_remote_copy(
            src_ref=src, dst_ref=dst, send_sem=ssem.at[s], recv_sem=rsem.at[i],
            device_id=dev, device_id_type=MESH)

    def wait_bytes(ref, sem):
        pltpu.make_async_copy(ref, ref, sem).wait()

    sends = []

    def sent(ref, i, cond=None):
        sends.append((ref, i, cond))

    def flush():
        for ref, i, cond in sends:
            if cond is None:
                wait_bytes(ref, ssem.at[i])
            else:
                @pl.when(cond)
                def _(ref=ref, i=i):
                    wait_bytes(ref, ssem.at[i])
        sends.clear()

    rows = lambda c: pl.ds(mul(c * R, R), R)
    srow = lambda s: pl.ds(s * 128 if isinstance(s, int) else mul(s * 128, 128), 128)

    barrier = pltpu.get_barrier_semaphore()
    for d in (1, 2, 3):
        pl.semaphore_signal(barrier, inc=1, device_id=cpeer(d), device_id_type=MESH)
        pl.semaphore_signal(barrier, inc=1, device_id=zpeer(d), device_id_type=MESH)
    pl.semaphore_signal(barrier, inc=1, device_id=xpeer, device_id_type=MESH)
    pl.semaphore_wait(barrier, 7)

    i_smc, s_smc = rtake(), stake()
    for d in (1, 2, 3):
        rcopy(small, smc.at[d], cpeer(d), i_smc, s_smc).start()
    sent(smc.at[pl.ds(1, 3)], s_smc)
    own32 = pl.ds(mul(seq * 128 + ctx * 32, 32), 32)

    def qkv_pieces(c):
        for j in range(6):
            yield (pl.ds(mul((j % 3) * D + (c + 4 * (j // 3)) * 128, 128), 128),
                   pl.ds(j * 128, 128))

    i_qa, s_qa = rtake(), stake()
    for d in (1, 2, 3):
        for a, b in qkv_pieces((ctx + d) % 4):
            rcopy(qkv_in.at[:, a], wqkv.at[own32, b], cpeer(d), i_qa, s_qa).start()
    sent(wqkv.at[pl.ds(0, 96), :], s_qa)
    l_q = next(lids)
    for a, b in qkv_pieces(ctx):
        pltpu.make_async_copy(qkv_in.at[:, a], wqkv.at[own32, b], lsem.at[l_q]).start()

    t = seq % 4
    out32 = pl.ds(mul((seq // 4) * 128 + ctx * 32, 32), 32)
    i_oa, s_oa = rtake(), stake()
    l_o = next(lids)

    @pl.when(ctx != t)
    def _():
        rcopy(out_in, wout.at[out32, :], {"ctx": t}, i_oa, s_oa).start()

    sent(wout.at[pl.ds(0, 32), :], s_oa, ctx != t)

    @pl.when(ctx == t)
    def _():
        pltpu.make_async_copy(out_in, wout.at[out32, :], lsem.at[l_o]).start()

    i_ua, s_ua = rtake(), stake()
    for d in (1, 2, 3):
        c2 = (ctx + d) % 4
        for s in range(8):
            rcopy(up_in.at[:, pl.ds(mul((s * 4 + c2) * 128, 128), 128)],
                  wup.at[own32, pl.ds(s * 128, 128)], cpeer(d), i_ua, s_ua).start()
    sent(wup.at[pl.ds(0, 96), :], s_ua)
    l_u = next(lids)
    for s in range(8):
        pltpu.make_async_copy(up_in.at[:, pl.ds(mul((s * 4 + ctx) * 128, 128), 128)],
                              wup.at[own32, pl.ds(s * 128, 128)], lsem.at[l_u]).start()

    wait_bytes(smc.at[pl.ds(1, 3)], rsem.at[i_smc])
    rowid = lax.broadcasted_iota(jnp.int32, (16, 128), 0)
    smb[seq] = small[...] + jnp.where(rowid < 8, smc[1] + smc[2] + smc[3], 0.0)

    def relay_start(block, i, s, src=None):
        own = block(seq) if src is None else src
        for cond, step, first, sz in ((z < 3, 1, i, s), (z > 0, -1, i + 4, s + 1)):
            @pl.when(cond)
            def _(step=step, first=first, sz=sz):
                rcopy(own, block(seq), {"seq": (z + step) * 2 + x}, first + 1, sz).start()

    def relay_x(block, i, s, src=None):
        own = block(seq) if src is None else src
        rcopy(own, block(seq), xpeer, i, s + 2).start()

    def relay_step(block, i, s, j):
        for has, on, step, first, sz in ((z >= j, z < 3, 1, i, s), (z + j <= 3, z > 0, -1, i + 4, s + 1)):
            zz = z - j * step

            @pl.when(has)
            def _(on=on, step=step, first=first, zz=zz, sz=sz):
                b = block(zz * 2 + x)
                wait_bytes(b, rsem.at[first + j])
                if j < 3:
                    @pl.when(on)
                    def _():
                        rcopy(b, b, {"seq": (z + step) * 2 + x}, first + j + 1, sz).start()
                rcopy(b, b, xpeer, i, s + 2).start()

    def relay_finish(w, i):
        wait_bytes(w.at[pl.ds(0, 512), :], rsem.at[i])

    def relay_sent(w, s):
        for n in (1, 2, 3):
            sent(w.at[pl.ds(0, n * 128), :], s, z == n - 1)
            sent(w.at[pl.ds(0, n * 128), :], s + 1, z == 4 - n)
        sent(w.at[pl.ds(0, 512), :], s + 2)

    i_sz, i_sx, s_sz, s_sx = rtake(3), rtake(), stake(), stake()
    for d in ORDER:
        rcopy(smb.at[seq], smb.at[seq], zpeer(d), i_sz + d - 1, s_sz).start()
    rcopy(smb.at[seq], smb.at[seq], xpeer, i_sx, s_sx).start()
    sent(smb.at[pl.ds(0, 3)], s_sz)
    sent(smb.at[pl.ds(0, 4)], s_sx)

    wait_bytes(wqkv.at[pl.ds(0, 96), :], rsem.at[i_qa])
    wait_bytes(wqkv.at[pl.ds(0, 32), :], lsem.at[l_q])
    qkv_block = lambda s: wqkv.at[srow(s), :]
    i_qr, s_qr = rtake(8), stake(3)
    relay_start(qkv_block, i_qr, s_qr)
    relay_sent(wqkv, s_qr)
    for d in ORDER:
        b = smb.at[((z - d + 4) % 4) * 2 + x]
        wait_bytes(b, rsem.at[i_sz + d - 1])
        rcopy(b, b, xpeer, i_sx, s_sx).start()
    relay_x(qkv_block, i_qr, s_qr)
    l_d = next(lids)
    down_block = lambda s: wdown.at[srow(s), :]
    i_dr, s_dr = rtake(8), stake(3)
    relay_x(down_block, i_dr, s_dr, src=down_in)
    relay_sent(wdown, s_dr)
    pltpu.make_async_copy(down_in, down_block(seq), lsem.at[l_d]).start()

    wait_bytes(smb.at[pl.ds(0, 4)], rsem.at[i_sx])
    for s in range(8):
        vec[:, s * 128 : (s + 1) * 128] = smb[s]

    length = length_ref[0]
    my = mul(ctx * R, R)

    def valid_rows(r0, n):
        pos = lax.broadcasted_iota(jnp.int32, (n, 1), 0) + (ctx * R + r0)
        return jnp.where(pos < length, 1.0, 0.0).astype(f32)

    CH = 2
    RC = R // CH

    def chunk(buf, c, ch):
        return buf.at[pl.ds(mul(c * R + ch * RC, RC), RC), :]

    def ag_start(buf, i, s, ch):
        own = chunk(buf, ctx, ch)
        rcopy(own, own, ypeer, i + 1 + ch, s + ch).start()
        rcopy(own, own, mate, i, s + ch).start()

    def ag_forward(buf, i, s, ch):
        b = chunk(buf, ((y + 1) % 2) * 2 + k, ch)
        wait_bytes(b, rsem.at[i + 1 + ch])
        rcopy(b, b, mate, i + 3, s + ch).start()

    def ag_wait(buf, i, which):
        wait_bytes(buf.at[pl.ds(0, R), :], rsem.at[i + which])

    def ag_bytes(buf):
        return buf.at[pl.ds(0, 3 * RC), :]

    i_n1, s_n1 = rtake(4), stake(2)
    for ch in range(CH):
        sent(ag_bytes(n1), s_n1 + ch)
    for ch in range(CH):
        def first(q, ch=ch):
            r0 = mul(ch * RC + q * 32, 32)
            zz, _ = layer_stats(tok[pl.ds(r0, 32), :].astype(f32))
            n1[pl.ds(mul(my + r0, 32), 32), :] = (zz * vec[0:1, :] + vec[1:2, :]).astype(bf16)

        loop(RC // 32, first)
        ag_start(n1, i_n1, s_n1, ch)


    def mask_rows(q):
        r0 = mul(q * 32, 32)
        g = cot[pl.ds(r0, 32), :].astype(f32) * valid_rows(r0, 32)
        gf[pl.ds(mul(my + r0, 32), 32), :] = g.astype(bf16)

    loop(R // 32, mask_rows)
    i_gf, s_gf = rtake(4), stake(2)
    for ch in range(CH):
        ag_start(gf, i_gf, s_gf, ch)
    for j in range(6):
        if j % 3 == 1:
            qbias[:, j * 128 : (j + 1) * 128] = jnp.zeros((8, 128), f32)
        else:
            r = 2 + j % 3 // 2
            b = vec[r : r + 1, pl.ds(mul((ctx + 4 * (j // 3)) * 128, 128), 128)]
            qbias[:, j * 128 : (j + 1) * 128] = jnp.broadcast_to(b, (8, 128))
    relay_step(qkv_block, i_qr, s_qr, 1)
    relay_step(qkv_block, i_qr, s_qr, 2)
    i_oz, i_ox, s_oz, s_ox = rtake(3), rtake(), stake(), stake()
    out_block = lambda zz: wout.at[pl.ds(mul((zz // 2) * 128, 128), 128), :]

    @pl.when(ctx == t)
    def _():
        wait_bytes(wout.at[pl.ds(0, 96), :], rsem.at[i_oa])
        wait_bytes(wout.at[pl.ds(0, 32), :], lsem.at[l_o])
        for d in (1, 2, 3):
            rcopy(out_block(z), out_block(z), zpeer(d), i_oz + d - 1, s_oz).start()
        rcopy(out_block(z), out_block(z), xpeer, i_ox, s_ox).start()

    sent(n1.at[pl.ds(0, 384), :], s_oz, ctx == t)
    sent(wout, s_ox, x == k)
    ag_forward(n1, i_n1, s_n1, 0)
    relay_step(qkv_block, i_qr, s_qr, 3)

    wait_bytes(wup.at[pl.ds(0, 96), :], rsem.at[i_ua])
    wait_bytes(wup.at[pl.ds(0, 32), :], lsem.at[l_u])
    up_block = lambda s: wup.at[srow(s), :]
    i_ur, s_ur = rtake(8), stake(3)
    relay_start(up_block, i_ur, s_ur)
    relay_sent(wup, s_ur)
    ag_forward(n1, i_n1, s_n1, 1)

    ag_wait(n1, i_n1, 0)
    relay_finish(wqkv, i_qr)
    mine = x == k
    for d in (1, 2, 3):
        zz = (z - d + 4) % 4

        @pl.when(jnp.logical_and(mine, zz % 2 == y))
        def _(d=d, zz=zz):
            wait_bytes(out_block(zz), rsem.at[i_oz + d - 1])
            rcopy(out_block(zz), out_block(zz), xpeer, i_ox, s_ox).start()

    relay_x(up_block, i_ur, s_ur)

    def project(it):
        blk = ((y + it // 2) % 2) * 2 + (k + it % 2) % 2

        @pl.when(it == 3)
        def _():
            ag_wait(n1, i_n1, 3)

        qkv[rows(blk), :] = (nn(n1[rows(blk), :], wqkv[...]) + qbias[0:1, :]).astype(bf16)

    loop(4, project)
    relay_step(up_block, i_ur, s_ur, 1)
    relay_start(down_block, i_dr, s_dr, src=down_in)

    def turn(i):
        c0 = pl.ds(mul(i * 128, 128), 128)
        vt[c0, :] = qkv[:, pl.ds(mul(i * 384 + 256, 128), 128)].T
        kt[c0, :] = qkv[:, pl.ds(mul(i * 384 + 128, 128), 128)].T

    loop(2, turn)

    lane = lax.broadcasted_iota(jnp.int32, (256, 128), 1)
    krow = lax.broadcasted_iota(jnp.int32, (256, 256), 0)
    qcol = lax.broadcasted_iota(jnp.int32, (256, 256), 1)

    def tri(kb, qb):
        return (qb * (qb + 1)) // 2 + kb

    def half(v, j):
        return jnp.where((lane // 64) == j, v, jnp.zeros_like(v))

    def pair_forward(i):
        for j in range(2):
            slope = jnp.exp2(jnp.full((1024, 128), -0.5, f32)
                             * (2 * ctx + 8 * i + j + 1).astype(f32)) * LOG2E
            b = slope * lax.broadcasted_iota(jnp.int32, (1024, 128), 0).astype(f32)
            for kb in range(4):
                own_b[j * 256 : (j + 1) * 256, kb * 128 : (kb + 1) * 128] = b[kb * 256 : (kb + 1) * 256]

        def queries(qb):
            q0 = pl.ds(mul(qb * 256, 256), 256)
            qblk = qkv[q0, pl.ds(mul(i * 384, 128), 128)]

            def scores(kb, best, diagonal=False):
                k0 = pl.ds(mul(kb * 256, 256), 256)
                kblk = qkv[k0, pl.ds(mul(i * 384 + 128, 128), 128)]
                new = []
                for j in range(2):
                    b = own_b[j * 256 : (j + 1) * 256, pl.ds(mul(kb * 128, 128), 128)]
                    sc = nt(half(kblk, j), qblk) * (0.125 * LOG2E) + jnp.concatenate([b, b], axis=1)
                    if diagonal:
                        sc = jnp.where(krow <= qcol, sc, -1e30)
                    own_a[j * 256 : (j + 1) * 256, k0] = sc
                    new.append(jnp.maximum(best[j], jnp.max(sc.reshape(32, 8, 256), axis=0)))
                return tuple(new)

            low = jnp.full((8, 256), -3e38, f32)
            best = scores(qb, lax.fori_loop(0, qb, scores, (low, low)), diagonal=True)
            top = [jnp.max(b, axis=0, keepdims=True) for b in best]

            def weigh(kb, carry):
                k0 = pl.ds(mul(kb * 256, 256), 256)
                new = []
                for j in range(2):
                    total, acc = carry[2 * j], carry[2 * j + 1]
                    p = jnp.exp2(own_a[j * 256 : (j + 1) * 256, k0] - top[j])
                    total = total + jnp.sum(p.reshape(32, 8, 256), axis=0)
                    p = p.astype(bf16)
                    ptri[2 * i + j, tri(kb, qb)] = p
                    v = vt[pl.ds(mul(i * 128 + j * 64, 64), 64), k0]
                    new += [total, acc + nn(v, p)]
                return tuple(new)

            zero = (jnp.zeros((8, 256), f32), jnp.zeros((64, 256), f32))
            out = lax.fori_loop(0, qb + 1, weigh, zero + zero)
            for j in range(2):
                inv = 1.0 / jnp.sum(out[2 * j], axis=0, keepdims=True)
                linv[2 * i + j, :, q0] = jnp.broadcast_to(inv, (8, 256))
                attt[pl.ds(mul(i * 128 + j * 64, 64), 64), q0] = (out[2 * j + 1] * inv).astype(bf16)

        loop(4, queries)

    pair_forward(0)
    for ch in range(CH):
        ag_forward(gf, i_gf, s_gf, ch)
    pair_forward(1)

    relay_step(up_block, i_ur, s_ur, 2)
    def rs_run(partial, sb, rb, own, i, s):
        def step(tt):
            g, ch, sub = tt // 4, tt % 2, (tt // 2) % 2
            blk = ((y + 1 - g) % 2) * 2 + (k + 1 - sub) % 2
            partial(blk, ch, tmp)

            @pl.when(jnp.logical_and(g == 0, sub == 0))
            def _():
                sb[0, ch] = tmp[...].astype(bf16)
                rcopy(sb.at[0, ch], rb.at[0, ch], mate, i + ch, s + ch).start()

            @pl.when(jnp.logical_and(g == 0, sub == 1))
            def _():
                wait_bytes(rb.at[0, ch], rsem.at[i + ch])
                sb[1, ch] = (tmp[...] + rb[0, ch].astype(f32)).astype(bf16)
                rcopy(sb.at[1, ch], rb.at[1, ch], ypeer, i + CH + ch, s + ch).start()

            @pl.when(jnp.logical_and(g == 1, sub == 0))
            def _():
                sb[2, ch] = tmp[...].astype(bf16)
                rcopy(sb.at[2, ch], rb.at[2, ch], mate, i + 2 * CH + ch, s + ch).start()

            @pl.when(jnp.logical_and(g == 1, sub == 1))
            def _():
                own[ch] = tmp[...]

        loop(4 * CH, step)

    def rs_wait(sb, rb, i, ch):
        wait_bytes(rb.at[2, ch], rsem.at[i + 2 * CH + ch])
        wait_bytes(rb.at[1, ch], rsem.at[i + CH + ch])

    def rs_sum(rb, own, ch, r):
        return own[ch, r, :] + rb[2, ch, r, :].astype(f32) + rb[1, ch, r, :].astype(f32)

    def rs_sent(sb, s):
        for ch in range(CH):
            wait_bytes(sb.at[:, ch], ssem.at[s + ch])

    @pl.when(x != k)
    def _():
        wait_bytes(wout, rsem.at[i_ox])

    def branch_part(blk, ch, dst):
        a = attt[:, pl.ds(mul(blk * R + ch * RC, RC), RC)]
        dst[...] = tn(a, wout[...])

    i_br, s_br = rtake(3 * CH), stake(CH)
    rs_run(branch_part, rs_s, rs_r, rs_own, i_br, s_br)
    relay_step(up_block, i_ur, s_ur, 3)
    relay_step(down_block, i_dr, s_dr, 1)

    i_n2, s_n2 = rtake(4), stake(2)
    stat[...] = jnp.zeros_like(stat)
    for ch in range(CH):
        rs_wait(rs_s, rs_r, i_br, ch)

        def second(q, ch=ch):
            r = pl.ds(mul(q * 32, 32), 32)
            r1 = pl.ds(mul(ch * RC + q * 32, 32), 32)
            branch = rs_sum(rs_r, rs_own, ch, r) + vec[4:5, :]
            resid = tok[r1, :].astype(f32) + branch
            res[r1, :] = resid
            zz, _ = layer_stats(resid)
            n2[pl.ds(mul(my + ch * RC + q * 32, 32), 32), :] = (
                zz * vec[5:6, :] + vec[6:7, :]).astype(bf16)
            v = valid_rows(ch * RC + q * 32, 32)
            stat[0:8, :] += jnp.sum((branch * branch * v).reshape(4, 8, D), axis=0)
            stat[8:16, :] += jnp.sum((resid * resid * v).reshape(4, 8, D), axis=0)

        loop(RC // 32, second)
        ag_start(n2, i_n2, s_n2, ch)

    relay_step(down_block, i_dr, s_dr, 2)
    relay_finish(wup, i_ur)

    def feed(it):
        blk = ((y + it // 2) % 2) * 2 + (k + it % 2) % 2

        @pl.when(it == 1)
        def _():
            ag_wait(n2, i_n2, 0)
            ag_forward(n2, i_n2, s_n2, 0)
            relay_step(down_block, i_dr, s_dr, 3)

        @pl.when(it == 2)
        def _():
            ag_forward(n2, i_n2, s_n2, 1)

        @pl.when(it == 3)
        def _():
            ag_wait(n2, i_n2, 3)

        def cols(n):
            c0 = pl.ds(mul(n * 512, 512), 512)
            pre = nn(n2[rows(blk), :], wup[:, c0]) + vec[8:9, c0]
            sq = pre * pre
            th = jnp.tanh(0.7978845608028654 * pre * (1.0 + 0.044715 * sq))
            a1 = 0.5 * (1.0 + th)
            act[rows(blk), c0] = (pre * a1).astype(bf16)
            der = a1 + 0.5 * pre * (1.0 - th * th) * (
                0.7978845608028654 * (1.0 + 0.134145 * sq))
            gpre[rows(blk), c0] = der.astype(bf16)

        loop(2, cols)

    loop(4, feed)

    def dw_half(a, b, c0, n, xx, hh):
        c1 = pl.ds(mul((hh * 2 + xx) * 128, 128), 128)
        c2 = pl.ds(mul(((3 - hh) * 2 + xx) * 128, 128), 128)
        return tn(jnp.concatenate([a[:, c1], a[:, c2]], axis=1), b[:, c0 : c0 + n])

    def dw_away(a, b, c0, n, xb, xr, i, s, parts):
        w = n // parts
        for hh in range(2):
            r = pl.ds(hh * 256, 256)
            xb[r, c0 : c0 + n] = dw_half(a, b, c0, n, (x + 1) % 2, hh).astype(bf16)
            for p in range(parts):
                c = pl.ds(c0 + p * w, w)
                rcopy(xb.at[r, c], xr.at[r, c], xpeer, i + hh * parts + p, s).start()
        sent(xb.at[pl.ds(0, 512), pl.ds(c0, n)], s)

    def dw_keep(a, b, c0, n, own):
        def keep(hh):
            own[pl.ds(mul(hh * 256, 256), 256), c0 : c0 + n] = dw_half(a, b, c0, n, x, hh)

        loop(2, keep)

    def dw_z(hh, c0, n, xr, own, zb, zr0, zc, zr, fin, i, iz, sz):
        wait_bytes(xr.at[pl.ds(0, 256), pl.ds(c0, n)], rsem.at[i])
        c = slice(c0, c0 + n)
        cz = slice(zc, zc + n)
        for part, zz in enumerate((hh, 3 - hh)):
            r = slice(hh * 256 + part * 128, hh * 256 + part * 128 + 128)
            ro = slice(zr0 + zz * 128, zr0 + zz * 128 + 128)
            dz = (zz - z + 4) % 4

            @pl.when(zz == z)
            def _(r=r):
                fin[:, c] = own[r, c] + xr[r, c].astype(f32)

            @pl.when(zz != z)
            def _(r=r, ro=ro, zz=zz, dz=dz):
                zb[ro, cz] = (own[r, c] + xr[r, c].astype(f32)).astype(bf16)
                rcopy(zb.at[ro, cz], zr.at[dz - 1, :, c], {"seq": zz * 2 + x}, iz, sz).start()

    def dw_end(c0, n, zr, fin, iz):
        c = slice(c0, c0 + n)
        wait_bytes(zr.at[:, :, pl.ds(c0, n)], rsem.at[iz])
        fin[:, c] += (zr[0, :, c].astype(f32) + zr[1, :, c].astype(f32)) + zr[2, :, c].astype(f32)

    ag_wait(gf, i_gf, 0)
    ag_wait(gf, i_gf, 3)
    i_dwx, i_dwz, s_dwx, s_dwz = rtake(4), rtake(2), stake(), stake(2)
    dw_away(act, gf, 0, D, xs_down, xr_down, i_dwx, s_dwx, 2)
    dw_keep(act, gf, 0, D, own_a)
    relay_finish(wdown, i_dr)
    wait_bytes(wdown.at[pl.ds(0, 128), :], lsem.at[l_d])
    gvec[...] = jnp.zeros_like(gvec)

    def grad_feed(it):
        r = pl.ds(mul(it * R, R), R)

        def cols(n):
            c0 = pl.ds(mul(n * 512, 512), 512)
            ga = nt(gf[r, :], wdown[c0, :])
            g = (ga * gpre[r, c0].astype(f32)).astype(bf16)
            gpre[r, c0] = g
            gvec[2, :, c0] += jnp.sum(g.astype(f32).reshape(R // 8, 8, 512), axis=0)

        loop(2, cols)

    loop(4, grad_feed)

    def down_z(hh, p):
        dw_z(hh, p * 512, 512, xr_down, own_a, dmix, p * 512, 0, zr_down, fin_down,
             i_dwx + hh * 2 + p, i_dwz + p, s_dwz + p)

    down_z(0, 0)

    rs_sent(rs_s, s_br)

    def gn2_part(blk, ch, dst):
        dst[...] = nt(gpre[pl.ds(mul(blk * R + ch * RC, RC), RC), :], wup[...])

    i_g2, s_g2 = rtake(3 * CH), stake(CH)
    rs_run(gn2_part, rs_s, rs_r, rs_own, i_g2, s_g2)

    down_z(0, 1)
    i_uwx, i_uwz, s_uwx, s_uwz = rtake(4), rtake(2), stake(), stake(2)
    dw_away(n2, gpre, 0, D, xs_up, xr_up, i_uwx, s_uwx, 2)
    dw_keep(n2, gpre, 0, D, own_b)

    def up_z(hh, p):
        dw_z(hh, p * 512, 512, xr_up, own_b, gpre, 0, p * 512, zr_up, fin_up,
             i_uwx + hh * 2 + p, i_uwz + p, s_uwz + p)

    for p in range(2):
        sent(gpre.at[pl.ds(0, 384), pl.ds(0, 512)], s_uwz + p)
    down_z(1, 0)

    i_gb, s_gb = rtake(4), stake(2)
    for ch in range(CH):
        sent(ag_bytes(gb), s_gb + ch)
    for ch in range(CH):
        rs_wait(rs_s, rs_r, i_g2, ch)

        def third(q, ch=ch):
            r = pl.ds(mul(q * 32, 32), 32)
            r1 = pl.ds(mul(ch * RC + q * 32, 32), 32)
            g2 = rs_sum(rs_r, rs_own, ch, r)
            zz, rstd = layer_stats(res[r1, :])
            gout = cot[r1, :].astype(f32) * valid_rows(ch * RC + q * 32, 32)
            gres = gout + layer_back(g2, vec[5:6, :], zz, rstd)
            st_grad[r1, :] = gres
            low = gres.astype(bf16)
            gb[pl.ds(mul(my + ch * RC + q * 32, 32), 32), :] = low
            fold = lambda v: jnp.sum(v.reshape(4, 8, D), axis=0)
            gvec[4] += fold(low.astype(f32))
            gvec[5] += fold(g2 * zz)
            gvec[6] += fold(g2)
            gvec[7] += fold(gout)

        loop(RC // 32, third)
        ag_start(gb, i_gb, s_gb, ch)

    down_z(1, 1)
    ag_forward(gb, i_gb, s_gb, 0)

    def ffn_part(blk, ch, dst):
        dst[...] = nn(act[pl.ds(mul(blk * R + ch * RC, RC), RC), :], wdown[...])

    i_ff, s_ff = rtake(3 * CH), stake(CH)
    rs_run(ffn_part, rt_s, rt_r, rt_own, i_ff, s_ff)
    up_z(0, 0)
    ag_forward(gb, i_gb, s_gb, 1)

    ag_wait(gb, i_gb, 0)
    ag_wait(gb, i_gb, 3)

    def att_grad(i):
        c0 = pl.ds(mul(i * 256, 256), 256)
        dot_[:, c0] = nt(wout[...], gb[c0, :]).astype(bf16)

    loop(4, att_grad)
    own_out[...] = nn(attt[...], gb[...])
    i_owx, i_owz, s_owx, s_owz = rtake(), rtake(), stake(), stake()
    for ch in range(CH):
        wait_bytes(ag_bytes(gf), ssem.at[s_gf + ch])
        wait_bytes(ag_bytes(n2), ssem.at[s_n2 + ch])
    xs_out = gf.at[pl.ds(512, 256), :]

    @pl.when(x != k)
    def _():
        gf[512:768, :] = own_out[...].astype(bf16)
        rcopy(xs_out, xr_out, xpeer, i_owx, s_owx).start()

    sent(xs_out, s_owx, x != k)
    sent(n2.at[pl.ds(0, 128), :], s_owz, jnp.logical_and(x == k, z % 2 == y))
    sent(n2.at[pl.ds(0, 256), :], s_owz, jnp.logical_and(x == k, z % 2 != y))

    lane2 = lax.broadcasted_iota(jnp.int32, (1024, 128), 1)

    def pair_backward(i):
        p0 = pl.ds(mul(i * 128, 128), 128)
        for j in range(2):
            r0 = pl.ds(mul(i * 128 + j * 64, 64), 64)
            li = linv[2 * i + j, 0:1, :]
            dd = dot_[r0, :].astype(f32) * li
            delta = jnp.sum(dd * attt[r0, :].astype(f32), axis=0, keepdims=True)
            linv[2 * i + j, :, :] = jnp.broadcast_to(delta, (8, 1024))
            dot_[r0, :] = dd.astype(bf16)
        do_[...] = dot_[p0, :].T
        acck[...] = jnp.zeros_like(acck)
        accv[...] = jnp.zeros_like(accv)

        def queries(qb):
            q0 = pl.ds(mul(qb * 256, 256), 256)
            qblk = qkv[q0, pl.ds(mul(i * 384, 128), 128)]
            doblk = do_[q0, :]
            dt = dot_[p0, q0]

            def keys(kb, carry):
                k0 = pl.ds(mul(kb * 256, 256), 256)
                vblk = qkv[k0, pl.ds(mul(i * 384 + 256, 128), 128)]
                new = []
                for j in range(2):
                    p = ptri[2 * i + j, tri(kb, qb)]
                    dp = nn(half(vblk, j), dt) - linv[2 * i + j, 0:1, q0]
                    ds = (p.astype(f32) * dp).astype(bf16)
                    accv[j, k0, :] += nn(p, doblk)
                    acck[j, k0, :] += nn(ds, qblk)
                    kk = kt[pl.ds(mul(i * 128 + j * 64, 64), 64), k0]
                    new.append(carry[j] + nn(kk, ds))
                return tuple(new)

            zero = jnp.zeros((64, 256), f32)
            dq = lax.fori_loop(0, qb + 1, keys, (zero, zero))
            dq = jnp.concatenate(dq, axis=0) * 0.125
            dmix[q0, pl.ds(mul(i * 384, 128), 128)] = dq.T.astype(bf16)

        loop(4, queries)
        dk = jnp.where(lane2 < 64, acck[0], acck[1]) * 0.125
        dv = jnp.where(lane2 < 64, accv[0], accv[1])
        dmix[:, pl.ds(mul(i * 384 + 128, 128), 128)] = dk.astype(bf16)
        dmix[:, pl.ds(mul(i * 384 + 256, 128), 128)] = dv.astype(bf16)

    up_z(0, 1)
    for p in range(2):
        wait_bytes(dmix.at[pl.ds(0, 384), pl.ds(0, 512)], ssem.at[s_dwz + p])
    pair_backward(0)
    i_qwx, i_qwz, s_qwx, s_qwz = (rtake(2), rtake(2)), rtake(2), stake(2), stake(2)
    up_z(1, 0)
    dw_away(n1, dmix, 0, 384, gf, xr_qkv, i_qwx[0], s_qwx, 1)
    pair_backward(1)

    rs_sent(rs_s, s_g2)

    def gn1_part(blk, ch, dst):
        dst[...] = nt(dmix[pl.ds(mul(blk * R + ch * RC, RC), RC), :], wqkv[...])

    i_g1, s_g1 = rtake(3 * CH), stake(CH)
    up_z(1, 1)
    rs_run(gn1_part, rs_s, rs_r, rs_own, i_g1, s_g1)
    dw_away(n1, dmix, 384, 384, gf, xr_qkv, i_qwx[1], s_qwx + 1, 1)
    dw_keep(n1, dmix, 0, 768, own_a)

    def qkv_z(h):
        for hh in range(2):
            dw_z(hh, h * 384, 384, xr_qkv, own_a, n2, 0, h * 384, zr_qkv, fin_qkv,
                 i_qwx[h] + hh, i_qwz + h, s_qwz + h)
        sent(n2.at[pl.ds(0, 384), pl.ds(0, 384)], s_qwz + h)

    for i in range(2):
        zi = y + 2 * i
        dz = (zi - z + 4) % 4

        @pl.when(x == k)
        def _(i=i, zi=zi, dz=dz):
            if i == 0:
                wait_bytes(xr_out, rsem.at[i_owx])
            half_rows = slice(i * 128, (i + 1) * 128)
            total = own_out[half_rows, :] + xr_out[half_rows, :].astype(f32)

            @pl.when(zi == z)
            def _():
                fin_out[...] = total

            @pl.when(zi != z)
            def _():
                n2[512 + i * 128 : 640 + i * 128, :] = total.astype(bf16)
                rcopy(n2.at[pl.ds(512 + i * 128, 128), :], zr_out.at[dz - 1], {"seq": zi * 2 + x}, i_owz, s_owz).start()

    qkv_z(0)
    for ch in range(CH):
        rs_wait(rs_s, rs_r, i_g1, ch)

        def fourth(q, ch=ch):
            r = pl.ds(mul(q * 32, 32), 32)
            r1 = pl.ds(mul(ch * RC + q * 32, 32), 32)
            g1 = rs_sum(rs_r, rs_own, ch, r)
            zz, rstd = layer_stats(tok[r1, :].astype(f32))
            st_grad[r1, :] += layer_back(g1, vec[0:1, :], zz, rstd)
            fold = lambda v: jnp.sum(v.reshape(4, 8, D), axis=0)
            gvec[0] += fold(g1 * zz)
            gvec[1] += fold(g1)

        loop(RC // 32, fourth)
    l_g = next(lids)
    pltpu.make_async_copy(st_grad, o_grad, lsem.at[l_g]).start()

    gmat[...] = jnp.zeros_like(gmat)
    for r, v in ((0, 0), (1, 1), (4, 4), (5, 5), (6, 6), (7, 7), (8, 2)):
        gmat[r : r + 1, :] = jnp.sum(gvec[v], axis=0, keepdims=True)
    for r, p in ((2, 0), (3, 256)):
        for i in range(2):
            v = dmix[:, i * 384 + p : i * 384 + p + 128].astype(f32)
            v = jnp.sum(jnp.sum(v.reshape(128, 8, 128), axis=0), axis=0, keepdims=True)
            gmat[r : r + 1, pl.ds(mul((ctx + 4 * i) * 128, 128), 128)] = v
    for s in range(8):
        sg[s] = gmat[:, s * 128 : (s + 1) * 128]
    i_sgx, i_sgz, i_sgc, s_sgx, s_sgz, s_sgc = rtake(), rtake(), rtake(), stake(), stake(), stake()
    for j in range(4):
        src = sg.at[j * 2 + (x + 1) % 2]
        rcopy(src, sgx.at[j], xpeer, i_sgx, s_sgx).start()
    sent(sgx, s_sgx)

    qkv_z(1)
    wait_bytes(sgx, rsem.at[i_sgx])
    for d in (1, 2, 3):
        zz = (z + d) % 4
        sgs[d - 1] = sg[zz * 2 + x] + sgx[zz]
        rcopy(sgs.at[d - 1], sgz.at[d - 1], zpeer(d), i_sgz, s_sgz).start()
    sent(sgs, s_sgz)

    for p in range(2):
        dw_end(p * 512, 512, zr_down, fin_down, i_dwz + p)
    l_dd = next(lids)
    pltpu.make_async_copy(fin_down, o_ddown, lsem.at[l_dd]).start()
    for p in range(2):
        dw_end(p * 512, 512, zr_up, fin_up, i_uwz + p)
    i_uf, i_qf, i_of, s_uf, s_qf, s_of = rtake(), rtake(2), rtake(), stake(), stake(2), stake()

    def up_piece(fin, c, s):
        return (fin.at[pl.ds(mul(c * 32, 32), 32), pl.ds(s * 128, 128)],
                o_dup.at[:, pl.ds(mul((s * 4 + ctx) * 128, 128), 128)])

    for d in (1, 2, 3):
        for s in range(8):
            a, b = up_piece(fin_up, (ctx + d) % 4, s)
            rcopy(a, b, cpeer(d), i_uf, s_uf).start()
    sent(fin_up.at[pl.ds(0, 96), :], s_uf)
    mine32 = pl.ds(mul(ctx * 32, 32), 32)
    l_up = next(lids)
    for s in range(8):
        a, b = up_piece(fin_up, ctx, s)
        pltpu.make_async_copy(a, b, lsem.at[l_up]).start()

    l_do = next(lids)

    @pl.when(ctx == t)
    def _():
        wait_bytes(zr_out, rsem.at[i_owz])
        fin_out[...] += (zr_out[0].astype(f32) + zr_out[1].astype(f32)) + zr_out[2].astype(f32)
        for d in (1, 2, 3):
            src = fin_out.at[pl.ds(mul(((ctx + d) % 4) * 32, 32), 32), :]
            rcopy(src, o_dout, cpeer(d), i_of, s_of).start()
        pltpu.make_async_copy(fin_out.at[mine32, :], o_dout, lsem.at[l_do]).start()

    sent(fin_out.at[pl.ds(0, 96), :], s_of, ctx == t)

    for ch in range(CH):
        rs_wait(rt_s, rt_r, i_ff, ch)

        def last(q, ch=ch):
            r = pl.ds(mul(q * 32, 32), 32)
            r1 = pl.ds(mul(ch * RC + q * 32, 32), 32)
            ffn = rs_sum(rt_r, rt_own, ch, r) + vec[7:8, :]
            v = valid_rows(ch * RC + q * 32, 32)
            st_out[r1, :] = (v * (res[r1, :] + ffn)).astype(bf16)
            stat[16:24, :] += jnp.sum((ffn * ffn * v).reshape(4, 8, D), axis=0)

        loop(RC // 32, last)
    l_t = next(lids)
    pltpu.make_async_copy(st_out, o_out, lsem.at[l_t]).start()

    l_dq = []
    for h in range(2):
        dw_end(h * 384, 384, zr_qkv, fin_qkv, i_qwz + h)
        pieces = list(qkv_pieces(ctx))[3 * h : 3 * h + 3]
        for d in (1, 2, 3):
            c2 = (ctx + d) % 4
            for a, b in pieces:
                rcopy(fin_qkv.at[pl.ds(mul(c2 * 32, 32), 32), b], o_dqkv.at[:, a], cpeer(d), i_qf + h, s_qf + h).start()
        sent(fin_qkv.at[pl.ds(0, 96), pl.ds(0, 384)], s_qf + h)
        l_dq.append(next(lids))
        for a, b in pieces:
            pltpu.make_async_copy(fin_qkv.at[mine32, b], o_dqkv.at[:, a], lsem.at[l_dq[h]]).start()

    wait_bytes(sgz, rsem.at[i_sgz])
    sgf[...] = sg[seq] + sgx[z] + (sgz[0] + sgz[1] + sgz[2])
    for j in range(3):
        v = jnp.sum(stat[j * 8 : (j + 1) * 8, :], axis=0, keepdims=True)
        sgf[9 + j : 10 + j, :] = jnp.broadcast_to(jnp.sum(v, axis=1, keepdims=True), (1, 128))
    for d in (1, 2, 3):
        rcopy(sgf, sgc.at[d], cpeer(d), i_sgc, s_sgc).start()
    sent(sgc.at[pl.ds(1, 3)], s_sgc)

    wait_bytes(sgc.at[pl.ds(1, 3)], rsem.at[i_sgc])
    o_small[...] = sgf[...] + jnp.where(rowid != 8, sgc[1] + sgc[2] + sgc[3], 0.0)

    @pl.when(ctx != t)
    def _():
        wait_bytes(fin_out.at[pl.ds(0, 32), :], rsem.at[i_of])

    @pl.when(ctx == t)
    def _():
        wait_bytes(fin_out.at[pl.ds(0, 32), :], lsem.at[l_do])

    wait_bytes(fin_up.at[pl.ds(0, 96), :], rsem.at[i_uf])
    for h in range(2):
        wait_bytes(fin_qkv.at[pl.ds(0, 96), pl.ds(0, 384)], rsem.at[i_qf + h])
    rs_sent(rs_s, s_g1)
    rs_sent(rt_s, s_ff)
    flush()
    for ref, i in ((st_grad, l_g), (st_out, l_t), (fin_down, l_dd), (fin_up.at[pl.ds(0, 32), :], l_up),
                   (fin_qkv.at[pl.ds(0, 32), pl.ds(0, 384)], l_dq[0]),
                   (fin_qkv.at[pl.ds(0, 32), pl.ds(0, 384)], l_dq[1])):
        wait_bytes(ref, lsem.at[i])
    assert next(rids) == NRECV and next(sids) == NSEND and next(lids) == NLOCAL


def finish_kernel(length_ref, sums, *refs):
    big, outs, vecs = refs[:6], refs[6:12], refs[12:20]
    o_ub, o_stats = refs[20:22]
    stage, s_in, s_out = refs[22:28], refs[28], refs[29]
    for i in range(6):
        pltpu.make_async_copy(big[i], stage[i], s_in.at[i]).start()
    ctx = lax.axis_index("ctx")
    mine = sums[0:8, 0:32]
    for c in range(1, 4):
        mine = jnp.where(ctx == c, sums[0:8, c * 32 : (c + 1) * 32], mine)
    for r in range(8):
        vecs[r][...] = mine[r, :]
    o_ub[...] = sums[8, :]
    lane = lax.broadcasted_iota(jnp.int32, (1, 128), 1)
    v = jnp.where(lane == 0, sums[9:10, :], jnp.where(lane == 1, sums[10:11, :], sums[11:12, :]))
    o_stats[...] = jnp.sqrt(v / (length_ref[0].astype(f32) * D))[:, 0:3]
    for i in range(6):
        pltpu.make_async_copy(big[i], stage[i], s_in.at[i]).wait()
        pltpu.make_async_copy(stage[i], outs[i], s_out.at[i]).start()
    for i in range(6):
        pltpu.make_async_copy(stage[i], outs[i], s_out.at[i]).wait()


def fast(mesh):
    def scratch():
        v = lambda dt, *shape: pltpu.VMEM(shape, dt)
        return [
            v(bf16, D, 768), v(bf16, 256, D), v(bf16, D, D), v(bf16, D, D),
            v(f32, 4, 16, 128), v(f32, 8, 16, 128), v(f32, 16, D),
            v(bf16, S, D), v(bf16, S, D), v(bf16, S, D), v(bf16, S, D), v(bf16, S, D), v(bf16, S, D),
            v(bf16, S, 768), v(bf16, 256, S), v(bf16, 256, S), v(bf16, 256, S),
            v(bf16, 256, S), v(bf16, S, 128), v(bf16, S, 768), v(f32, 4, 8, S),
            v(bf16, 4, 10, 256, 256), v(f32, 2, S, 128), v(f32, 2, S, 128),
            v(bf16, 3, 2, 128, D), v(bf16, 3, 2, 128, D), v(f32, 2, 128, D),
            v(bf16, 3, 2, 128, D), v(bf16, 3, 2, 128, D), v(f32, 2, 128, D),
            v(f32, 128, D), v(f32, R, D),
            v(bf16, 512, D), v(bf16, 512, D), v(bf16, 512, D), v(bf16, 512, D), v(bf16, 512, 768), v(bf16, 256, D),
            v(f32, 512, D), v(f32, 512, D), v(f32, 256, D),
            v(bf16, 3, 128, D), v(bf16, 3, 128, D), v(bf16, 3, 128, 768), v(bf16, 3, 128, D),
            v(f32, 128, D), v(f32, 128, 768), v(f32, 128, D),
            v(bf16, R, D), v(f32, R, D), v(f32, 128, D),
            v(f32, 8, 16, 128), v(f32, 4, 16, 128), v(f32, 3, 16, 128), v(f32, 3, 16, 128),
            v(f32, 16, 128), v(f32, 4, 16, 128), v(f32, 8, 8, D), v(f32, 16, D), v(f32, 24, D), v(f32, 8, 768),
            pltpu.SemaphoreType.DMA((NLOCAL,)),
            pltpu.SemaphoreType.DMA((NSEND,)),
            pltpu.SemaphoreType.DMA((NRECV,)),
        ]

    def on_device(tokens, lengths, cotangent, g1, b1, wq, qb, vb, wo, ob, g2, b2, wu, ub, wd, db):
        ctx = lax.axis_index("ctx")
        vectors = jnp.stack([g1, b1, qb, vb, ob, g2, b2, db]).astype(f32)
        place = (jnp.arange(128) // 32) == ctx
        small = jnp.concatenate([
            jnp.where(place[None], jnp.tile(vectors, (1, 4)), 0.0),
            ub.astype(f32)[None], jnp.zeros((7, 128), f32)])
        vm = pl.BlockSpec(memory_space=pltpu.VMEM)
        sds = jax.ShapeDtypeStruct
        out, grad, dqkv, dout, dup, ddown, sums = pl.pallas_call(
            block_kernel,
            out_shape=(sds((R, D), bf16), sds((R, D), f32), sds((32, 3 * D), f32), sds((32, D), f32),
                       sds((32, 4 * D), f32), sds((128, D), f32), sds((16, 128), f32)),
            in_specs=[pl.BlockSpec(memory_space=pltpu.SMEM)] + [vm] * 3 + [pl.BlockSpec(memory_space=pl.ANY)] * 4,
            out_specs=tuple([pl.BlockSpec(memory_space=pl.ANY)] * 6 + [vm]),
            scratch_shapes=scratch(),
            compiler_params=pltpu.CompilerParams(
                collective_id=0, has_side_effects=True, vmem_limit_bytes=LIMIT),
            name="block",
        )(lengths, tokens[0], cotangent[0], small, wq, wo, wu, wd)
        anyspec = pl.BlockSpec(memory_space=pl.ANY)
        big = (out, grad, dqkv, dout, dup, ddown)
        res = pl.pallas_call(
            finish_kernel,
            out_shape=tuple(sds(v.shape, v.dtype) for v in big)
            + tuple([sds((32,), f32)] * 8) + (sds((128,), f32), sds((1, 3), f32)),
            in_specs=[pl.BlockSpec(memory_space=pltpu.SMEM), vm] + [anyspec] * 6,
            out_specs=tuple([anyspec] * 6 + [vm] * 10),
            scratch_shapes=[pltpu.VMEM(v.shape, v.dtype) for v in big]
            + [pltpu.SemaphoreType.DMA((6,)), pltpu.SemaphoreType.DMA((6,))],
            compiler_params=pltpu.CompilerParams(vmem_limit_bytes=LIMIT),
            name="finish",
        )(lengths, sums, *big)
        out, grad, dqkv, dout, dup, ddown, g1, b1, qb, vb, ob, g2, b2, db, ub, stats = res
        return (out[None], grad[None], g1, b1, dqkv, qb, vb, dout, ob, g2, b2, dup, ub, ddown, db, stats)

    return on_device


HEADS = 16


epsilon = 1e-05


def normalize(inputs, gain, shift):
    average = jnp.mean(inputs, axis=-1, keepdims=True)
    centred = inputs - average
    variance = jnp.mean(centred * centred, axis=-1, keepdims=True)
    return centred * lax.rsqrt(variance + epsilon) * gain + shift


def gelu_tanh(inputs):
    return jax.nn.gelu(inputs, approximate=True)


def inner_rows(left, right):
    return lax.dot_general(
        left, right, (((0,), (0,)), ((), ())), preferred_element_type=jnp.float32
    )


def outer_cols(left, right):
    return lax.dot_general(
        left, right, (((1,), (1,)), ((), ())), preferred_element_type=jnp.float32
    )


def alibi_scores(query_block, key_block, query_pos, key_pos, slope_block):
    raw = jnp.einsum("qhd,khd->hqk", query_block, key_block, preferred_element_type=jnp.float32)
    offset = (key_pos[None, :] - query_pos[:, None]).astype(jnp.float32)
    scores = raw * query_block.shape[-1] ** (-0.5) + slope_block[:, None, None] * offset[None]
    allowed = key_pos[None, :] <= query_pos[:, None]
    return (scores, allowed)


def score_grads(
    query_block,
    key_block,
    value_block,
    grad_block,
    query_pos,
    key_pos,
    slope_block,
    log_block,
    delta_block,
):
    scores, allowed = alibi_scores(query_block, key_block, query_pos, key_pos, slope_block)
    probs = jnp.where(allowed[None], jnp.exp(scores - log_block[..., None]), 0.0)
    grad_probs = jnp.einsum(
        "qhd,khd->hqk", grad_block, value_block, preferred_element_type=jnp.float32
    )
    delta_block = jnp.sum(probs * grad_probs, axis=-1)
    grad_scores = (probs * (grad_probs - delta_block[..., None])).astype(jnp.bfloat16)
    return (probs, grad_scores, delta_block)


def on_device(
    tokens,
    lengths,
    cotangent,
    ln1_gain,
    ln1_bias,
    qkv_weight,
    query_bias,
    value_bias,
    out_weight,
    out_bias,
    ln2_gain,
    ln2_bias,
    up_weight,
    up_bias,
    down_weight,
    down_bias,
):
    shards = (
        ln1_gain,
        ln1_bias,
        qkv_weight,
        query_bias,
        value_bias,
        out_weight,
        out_bias,
        ln2_gain,
        ln2_bias,
        up_weight,
        up_bias,
        down_weight,
        down_bias,
    )
    row_count = tokens.shape[1]
    model_width = tokens.shape[2]
    head_count = HEADS
    head_width = model_width // head_count
    per_block = 2
    block_count = head_count // per_block
    slot_rows = row_count * lax.axis_size("ctx")
    positions = lax.axis_index("ctx") * row_count + jnp.arange(row_count, dtype=jnp.int32)
    length = lengths[0]
    valid_rows = (positions < length).astype(jnp.float32)[:, None]
    slopes = jnp.exp2(-8.0 * (jnp.arange(head_count, dtype=jnp.float32) + 1.0) / head_count)
    key_positions = jnp.arange(slot_rows, dtype=jnp.int32)
    scale = head_width ** (-0.5)
    full_weights = (
        lax.all_gather(shards[0], ("seq", "ctx"), axis=0, tiled=True),
        lax.all_gather(shards[1], ("seq", "ctx"), axis=0, tiled=True),
        lax.all_gather(shards[2], ("seq", "ctx"), axis=0, tiled=True),
        lax.all_gather(shards[3], ("seq", "ctx"), axis=0, tiled=True),
        lax.all_gather(shards[4], ("seq", "ctx"), axis=0, tiled=True),
        lax.all_gather(shards[5], ("seq", "ctx"), axis=0, tiled=True),
        lax.all_gather(shards[6], ("seq", "ctx"), axis=0, tiled=True),
        lax.all_gather(shards[7], ("seq", "ctx"), axis=0, tiled=True),
        lax.all_gather(shards[8], ("seq", "ctx"), axis=0, tiled=True),
        lax.all_gather(shards[9], ("seq", "ctx"), axis=0, tiled=True),
        lax.all_gather(shards[10], ("seq", "ctx"), axis=0, tiled=True),
        lax.all_gather(shards[11], ("seq", "ctx"), axis=0, tiled=True),
        lax.all_gather(shards[12], ("seq", "ctx"), axis=0, tiled=True),
    )
    (
        gain_one,
        shift_one,
        w_qkv,
        bias_query,
        bias_value,
        w_out,
        bias_out,
        gain_two,
        shift_two,
        w_up,
        bias_up,
        w_down,
        bias_down,
    ) = full_weights

    def pick(array, index):
        return lax.dynamic_slice_in_dim(array, index * per_block, per_block, 1)

    def pick_slopes(index):
        return lax.dynamic_slice_in_dim(slopes, index * per_block, per_block, 0)

    def to_blocks(array):
        return array.transpose(1, 0, 2, 3).reshape(array.shape[1], model_width)

    source = tokens[0].astype(jnp.float32)
    normed_one, back_one = jax.vjp(normalize, source, gain_one, shift_one)
    normed_low = normed_one.astype(jnp.bfloat16)
    mixed = jnp.dot(normed_low, w_qkv, preferred_element_type=jnp.float32)
    query = (mixed[:, :model_width] + bias_query).astype(jnp.bfloat16)
    keys = mixed[:, model_width : 2 * model_width].astype(jnp.bfloat16)
    values = (mixed[:, 2 * model_width :] + bias_value).astype(jnp.bfloat16)
    all_keys, all_values = (
        lax.all_gather(keys, "ctx", axis=0, tiled=True),
        lax.all_gather(values, "ctx", axis=0, tiled=True),
    )
    query_heads = query.reshape(row_count, head_count, head_width)
    key_heads = all_keys.reshape(slot_rows, head_count, head_width)
    value_heads = all_values.reshape(slot_rows, head_count, head_width)

    def forward_block(index):
        scores, allowed = alibi_scores(
            pick(query_heads, index),
            pick(key_heads, index),
            positions,
            key_positions,
            pick_slopes(index),
        )
        masked = jnp.where(allowed[None], scores, -1e30)
        highest = jnp.max(masked, axis=-1)
        total = jnp.sum(jnp.exp(masked - highest[..., None]), axis=-1)
        log_total = highest + jnp.log(total)
        probs = jnp.where(allowed[None], jnp.exp(scores - log_total[..., None]), 0.0)
        block_out = jnp.einsum(
            "hqk,khd->qhd",
            probs.astype(jnp.bfloat16),
            pick(value_heads, index),
            preferred_element_type=jnp.float32,
        )
        return (block_out, log_total)

    head_out, log_totals = lax.map(forward_block, jnp.arange(block_count))
    attended = to_blocks(head_out).astype(jnp.bfloat16)
    branch = jnp.dot(attended, w_out, preferred_element_type=jnp.float32) + bias_out
    resid = source + branch
    normed_two, back_two = jax.vjp(normalize, resid, gain_two, shift_two)
    normed_two_low = normed_two.astype(jnp.bfloat16)
    pre_act = jnp.dot(normed_two_low, w_up, preferred_element_type=jnp.float32) + bias_up
    activated, back_act = jax.vjp(gelu_tanh, pre_act)
    activated_low = activated.astype(jnp.bfloat16)
    ffn = jnp.dot(activated_low, w_down, preferred_element_type=jnp.float32) + bias_down
    output = (valid_rows * (resid + ffn)).astype(jnp.bfloat16)[None]
    squares = jnp.stack(
        [
            jnp.sum(valid_rows * branch * branch),
            jnp.sum(valid_rows * resid * resid),
            jnp.sum(valid_rows * ffn * ffn),
        ]
    )
    totals = lax.psum(squares, "ctx")
    stats = jnp.sqrt(totals / (length.astype(jnp.float32) * model_width))[None]
    w_qkv, w_out, w_up, w_down = (
        lax.all_gather(qkv_weight, ("seq", "ctx"), axis=0, tiled=True),
        lax.all_gather(out_weight, ("seq", "ctx"), axis=0, tiled=True),
        lax.all_gather(up_weight, ("seq", "ctx"), axis=0, tiled=True),
        lax.all_gather(down_weight, ("seq", "ctx"), axis=0, tiled=True),
    )
    grad_out = cotangent[0].astype(jnp.float32) * valid_rows
    grad_ffn = grad_out.astype(jnp.bfloat16)
    grad_down_w = inner_rows(activated_low, grad_ffn)
    grad_down_b = jnp.sum(grad_ffn.astype(jnp.float32), axis=0)
    grad_activated = outer_cols(grad_ffn, w_down)
    (grad_pre,) = back_act(grad_activated)
    grad_pre_low = grad_pre.astype(jnp.bfloat16)
    grad_up_w = inner_rows(normed_two_low, grad_pre_low)
    grad_up_b = jnp.sum(grad_pre_low.astype(jnp.float32), axis=0)
    grad_normed_two = outer_cols(grad_pre_low, w_up)
    grad_resid_norm, grad_gain_two, grad_shift_two = back_two(grad_normed_two)
    grad_resid = grad_out + grad_resid_norm
    grad_branch = grad_resid.astype(jnp.bfloat16)
    grad_out_w = inner_rows(attended, grad_branch)
    grad_out_b = jnp.sum(grad_branch.astype(jnp.float32), axis=0)
    grad_attended = outer_cols(grad_branch, w_out).astype(jnp.bfloat16)
    grad_heads = grad_attended.reshape(row_count, head_count, head_width)

    def backward_block(index):
        query_block = pick(query_heads, index)
        key_block = pick(key_heads, index)
        grad_block = pick(grad_heads, index)
        probs, grad_scores, delta_block = score_grads(
            query_block,
            key_block,
            pick(value_heads, index),
            grad_block,
            positions,
            key_positions,
            pick_slopes(index),
            log_totals[index],
            None,
        )
        grad_query_block = (
            jnp.einsum("hqk,khd->qhd", grad_scores, key_block, preferred_element_type=jnp.float32)
            * scale
        )
        grad_key_block = (
            jnp.einsum("hqk,qhd->khd", grad_scores, query_block, preferred_element_type=jnp.float32)
            * scale
        )
        grad_value_block = jnp.einsum(
            "hqk,qhd->khd",
            probs.astype(jnp.bfloat16),
            grad_block,
            preferred_element_type=jnp.float32,
        )
        return (grad_query_block, grad_key_block, grad_value_block)

    query_parts, key_parts, value_parts = lax.map(backward_block, jnp.arange(block_count))
    grad_query_all = to_blocks(query_parts)
    own_keys, own_values = (
        lax.psum_scatter(
            to_blocks(key_parts).astype(jnp.bfloat16), "ctx", scatter_dimension=0, tiled=True
        ).astype(jnp.float32),
        lax.psum_scatter(
            to_blocks(value_parts).astype(jnp.bfloat16), "ctx", scatter_dimension=0, tiled=True
        ).astype(jnp.float32),
    )
    grad_query_low = grad_query_all.astype(jnp.bfloat16)
    grad_key_low = own_keys.astype(jnp.bfloat16)
    grad_value_low = own_values.astype(jnp.bfloat16)
    grad_mixed = jnp.concatenate([grad_query_low, grad_key_low, grad_value_low], axis=1)
    grad_qkv_w = inner_rows(normed_low, grad_mixed)
    grad_query_bias = jnp.sum(grad_query_low.astype(jnp.float32), axis=0)
    grad_value_bias = jnp.sum(grad_value_low.astype(jnp.float32), axis=0)
    grad_normed_one = outer_cols(grad_mixed, w_qkv)
    grad_source_norm, grad_gain_one, grad_shift_one = back_one(grad_normed_one)
    grad_tokens = (grad_resid + grad_source_norm)[None]
    summed = (
        lax.psum_scatter(
            grad_gain_one.astype(jnp.float32), ("seq", "ctx"), scatter_dimension=0, tiled=True
        ),
        lax.psum_scatter(
            grad_shift_one.astype(jnp.float32), ("seq", "ctx"), scatter_dimension=0, tiled=True
        ),
        lax.psum_scatter(grad_qkv_w, ("seq", "ctx"), scatter_dimension=0, tiled=True),
        lax.psum_scatter(grad_query_bias, ("seq", "ctx"), scatter_dimension=0, tiled=True),
        lax.psum_scatter(grad_value_bias, ("seq", "ctx"), scatter_dimension=0, tiled=True),
        lax.psum_scatter(grad_out_w, ("seq", "ctx"), scatter_dimension=0, tiled=True),
        lax.psum_scatter(grad_out_b, ("seq", "ctx"), scatter_dimension=0, tiled=True),
        lax.psum_scatter(
            grad_gain_two.astype(jnp.float32), ("seq", "ctx"), scatter_dimension=0, tiled=True
        ),
        lax.psum_scatter(
            grad_shift_two.astype(jnp.float32), ("seq", "ctx"), scatter_dimension=0, tiled=True
        ),
        lax.psum_scatter(grad_up_w, ("seq", "ctx"), scatter_dimension=0, tiled=True),
        lax.psum_scatter(grad_up_b, ("seq", "ctx"), scatter_dimension=0, tiled=True),
        lax.psum_scatter(grad_down_w, ("seq", "ctx"), scatter_dimension=0, tiled=True),
        lax.psum_scatter(grad_down_b, ("seq", "ctx"), scatter_dimension=0, tiled=True),
    )
    return (output, grad_tokens) + tuple(summed) + (stats,)


def solution(mesh):
    small_slice = mesh.shape["seq"] == 8 and mesh.shape["ctx"] == 4
    placed = (
        P("seq", "ctx", None),
        P("seq"),
        P("seq", "ctx", None),
        P(("seq", "ctx")),
        P(("seq", "ctx")),
        P(("seq", "ctx"), None),
        P(("seq", "ctx")),
        P(("seq", "ctx")),
        P(("seq", "ctx"), None),
        P(("seq", "ctx")),
        P(("seq", "ctx")),
        P(("seq", "ctx")),
        P(("seq", "ctx"), None),
        P(("seq", "ctx")),
        P(("seq", "ctx"), None),
        P(("seq", "ctx")),
    )
    return jax.shard_map(
        fast(mesh) if small_slice else on_device,
        mesh=mesh,
        in_specs=placed,
        out_specs=(
            P("seq", "ctx", None),
            P("seq", "ctx", None),
            P(("seq", "ctx")),
            P(("seq", "ctx")),
            P(("seq", "ctx"), None),
            P(("seq", "ctx")),
            P(("seq", "ctx")),
            P(("seq", "ctx"), None),
            P(("seq", "ctx")),
            P(("seq", "ctx")),
            P(("seq", "ctx")),
            P(("seq", "ctx"), None),
            P(("seq", "ctx")),
            P(("seq", "ctx"), None),
            P(("seq", "ctx")),
            P("seq", None),
        ),
        check_vma=False,
    )
```
